32 devices in a mesh: dp: 16 (over z, y, x), tensor: 2 (over core).
Axes of the slice: x: 2, y: 2, z: 4, core: 2. Of those that a mesh axis runs over, the one named last changes fastest.
Arguments:
- layer_input: bfloat16 [8192, 1536], P(('dp', 'tensor')), may hold values from -6 to 6
- segments: int32 [16, 512], P('dp'), may hold values from 0 to 5, never falling along the last dimension, each value on 1 to 256 neighbouring positions
- gain_attn: float32 [1536], replicated, may hold values from 0.5 to 1.5
- w_query: bfloat16 [1536, 1536], P('dp', 'tensor'), may hold values from -3.8273277 to 3.8273277, as said below
- w_key: bfloat16 [1536, 768], P('dp', 'tensor'), may hold values from -0.15625 to 0.15625
- w_value: bfloat16 [1536, 768], P('dp', 'tensor'), may hold values from -0.15625 to 0.15625
- w_out: bfloat16 [1536, 1536], P('tensor', 'dp'), may hold values from -0.875 to 0.875
- gain_ffn: float32 [1536], replicated, may hold values from 0.5 to 1.5
- w_gate: bfloat16 [1536, 4096], P('dp', 'tensor'), may hold values from -0.15625 to 0.15625
- w_up: bfloat16 [1536, 4096], P('dp', 'tensor'), may hold values from -0.15625 to 0.15625
- w_down: bfloat16 [4096, 1536], P('tensor', 'dp'), may hold values from -0.09375 to 0.09375
- cotangent: bfloat16 [8192, 1536], P(('dp', 'tensor')), may hold values from -6 to 6
Outputs:
- output: bfloat16 [8192, 1536], P(('dp', 'tensor'))
- grad_input: float32 [8192, 1536], P(('dp', 'tensor'))
- grad_gain_attn: float32 [1536], replicated
- grad_query: float32 [1536, 1536], P('dp', 'tensor')
- grad_key: float32 [1536, 768], P('dp', 'tensor')
- grad_value: float32 [1536, 768], P('dp', 'tensor')
- grad_out: float32 [1536, 1536], P('tensor', 'dp')
- grad_gain_ffn: float32 [1536], replicated
- grad_gate: float32 [1536, 4096], P('dp', 'tensor')
- grad_up: float32 [1536, 4096], P('dp', 'tensor')
- grad_down: float32 [4096, 1536], P('tensor', 'dp')
The draws below stay inside these ranges and needn't reach their ends.
Inputs may be any that keep to these rules, and one draw needn't show every extreme that they name: `segments`: along each sequence the numbers never fall; each document holds 1 to 256 tokens. `w_query`: entries lie within 150 / sqrt(1536) of zero; in some draws they reach that bound.
All inputs are finite; a program needn't handle non-finite values.
Results may differ from the reference program's by a relative error of at most 0.017.
The reference program's roundings to bfloat16 on the way count: a program that leaves them out, or rounds other values in their place, can miss the bound.
Values may be sent and summed in bfloat16 or wider, within the bound.
A program may use at most 192 MiB of HBM per device.

```python
import math
import jax
import jax.numpy as jnp
import numpy as np
from jax import lax

D = 1536
H = 16
KV = 8
HD = 96
FF = 4096
L = 512
DOCS = 6
SEQS = 16
TOKENS = 8192


def draw_w_query(key, part):
    values = jnp.clip(jax.random.normal(key, (D, H * HD), jnp.float32), -6.0, 6.0) * D ** (-0.5)
    return values.astype(jnp.bfloat16)


def strengthened(drawn, stream_key, source, target, shards_of, factor):
    owner, partner = [(jnp.arange(drawn.shape[axis_at]) // (drawn.shape[axis_at] // shards_of)).reshape([-1 if axis == axis_at else 1 for axis in range(drawn.ndim)]) for axis_at in (source, target)]
    chosen = jax.random.permutation(stream_key, shards_of)[partner]
    strong = (owner == chosen) | (owner == (partner + shards_of // 2) % shards_of)
    return jnp.where(strong, factor * drawn, drawn)


def level_of(own_key, shape, cuts, least, high):
    def one(position, parts):
        heights = jax.random.uniform(jax.random.fold_in(jax.random.fold_in(own_key, 6), position), (parts,), jnp.float32, least / len(cuts), high / len(cuts))
        return jnp.repeat(jnp.exp(heights), shape[position] // parts).reshape((-1,) + (1,) * (len(shape) - position - 1))

    level = one(*cuts[0])
    for cut in cuts[1:]:
        level = level * one(*cut)
    return level


def split_up(number_of, total, reach, slope):
    portions = [(1 << 20) // math.isqrt(standing ** slope) + 1 for standing in range(2, number_of + 1)]
    rest, given = total - reach - (number_of - 1), [1] * (number_of - 1)
    while rest > 0:
        candidates = [i for i in range(number_of - 1) if given[i] < reach]
        mass, budget = sum([portions[i] for i in candidates]), rest
        for i in candidates:
            addition = min(reach - given[i], max(1, budget * portions[i] // mass), rest)
            given[i] = given[i] + addition
            rest = rest - addition
    return np.array([reach] + given)


def uneven_parts(stream_key, number_of, total, bound, slope):
    if number_of == 2:
        one = jax.random.randint(stream_key, (), max(1, total - bound), min(bound, total - 1) + 1)
        return jnp.stack([one, total - one])
    sizes = jnp.asarray(split_up(number_of, total, bound, slope), jnp.int32)
    pairs = (number_of - 1) // 2
    donor, receiver = sizes[1:1 + 2 * pairs:2], sizes[2:2 + 2 * pairs:2]
    margin = jnp.minimum(donor - 1, bound - receiver)
    moved = jax.random.randint(jax.random.fold_in(stream_key, 1), (pairs,), 0, 1 << 20) % (margin + 1)
    sizes = sizes.at[1:1 + 2 * pairs:2].set(donor - moved).at[2:2 + 2 * pairs:2].set(receiver + moved)
    return sizes[jax.random.permutation(jax.random.fold_in(stream_key, 2), number_of)]


def noise(own_key, shape, spread, most, pieces=(), kind=jnp.bfloat16):
    values = spread * jax.random.normal(own_key, shape, jnp.float32)
    if pieces:
        values = values * level_of(own_key, shape, pieces, -0.22, 0.18)
    return jnp.clip(values, -most, most).astype(kind)


def noise_with(rng, dims, scale, limit, shards, heavy, kind=jnp.bfloat16):
    drawn = scale * jax.random.normal(rng, dims, jnp.float32)
    if shards:
        drawn = drawn * level_of(rng, dims, shards, -0.22, 0.18)
    return jnp.clip(strengthened(drawn, jax.random.fold_in(rng, 3), *heavy), -limit, limit).astype(kind)


def setup_inputs(seed: int = 0) -> dict:
    streams_of = jax.random.split(jax.random.key(seed), 13)
    layer_input = noise(streams_of[0], (TOKENS, D), 1.0, 6.0, ((0, 32),))
    segments = jax.vmap(lambda own: jnp.searchsorted(jnp.cumsum(uneven_parts(own, DOCS, L, L // 2, 2)), jnp.arange(L), side="right"))(jax.random.split(streams_of[1], SEQS)).reshape((SEQS, L)).astype(jnp.int32)
    gain_attn = jnp.clip(1.0 + 0.1 * jax.random.normal(streams_of[2], (D,), jnp.float32), 0.5, 1.5)
    w_query = draw_w_query(jax.random.fold_in(streams_of[12], 71), 0)
    w_key = noise(streams_of[4], (D, KV * HD), D ** -0.5, 0.15625, ((0, 16), (1, 2)))
    w_value = noise(streams_of[5], (D, KV * HD), D ** -0.5, 0.15625, ((0, 16), (1, 2)))
    w_out = noise(streams_of[6], (H * HD, D), (H * HD // 32) ** -0.5, 0.875, ((0, 2), (1, 16)))
    gain_ffn = jnp.clip(1.0 + 0.1 * jax.random.normal(streams_of[7], (D,), jnp.float32), 0.5, 1.5)
    w_gate = noise(streams_of[8], (D, FF), D ** -0.5, 0.15625, ((0, 16), (1, 2)))
    w_up = noise(streams_of[9], (D, FF), D ** -0.5, 0.15625, ((0, 16), (1, 2)))
    w_down = noise(streams_of[10], (FF, D), FF ** -0.5, 0.09375, ((0, 2), (1, 16)))
    cotangent = noise_with(streams_of[11], (TOKENS, D), 1.0, 6.0, ((0, 32),), (0, 1, 32, 2.75))
    return dict(layer_input=layer_input, segments=segments, gain_attn=gain_attn, w_query=w_query, w_key=w_key, w_value=w_value, w_out=w_out, gain_ffn=gain_ffn, w_gate=w_gate, w_up=w_up, w_down=w_down, cotangent=cotangent)


EPSILON = 1e-05
ROPE_BASE = 100000.0
MASKED = -1e+30

def as_bf16(values):
    return lax.optimization_barrier(values.astype(jnp.bfloat16))

def doc_positions(segment_row):
    total_len = segment_row.shape[0]
    indices = jnp.arange(total_len, dtype=jnp.int32)
    changes = jnp.concatenate([jnp.ones((1,), dtype=bool), segment_row[1:] != segment_row[:-1]])
    starts = jnp.where(changes, indices, jnp.zeros_like(indices))
    return indices - lax.cummax(starts, axis=0)

def rotary_tables(positions, head_width):
    half_width = head_width // 2
    frequency = jnp.exp(-math.log(ROPE_BASE) * 2.0 * jnp.arange(half_width, dtype=jnp.float32) / head_width)
    angles = positions.astype(jnp.float32)[:, None] * frequency[None, :]
    return (jnp.cos(angles), jnp.sin(angles))

def rotate(values, cosine, sine):
    half_width = values.shape[-1] // 2
    first_half = values[..., :half_width]
    second_half = values[..., half_width:]
    cos_rows = cosine[:, None, :]
    sin_rows = sine[:, None, :]
    return jnp.concatenate([first_half * cos_rows - second_half * sin_rows, second_half * cos_rows + first_half * sin_rows], axis=-1)

def rotate_back(grads, cosine, sine):
    half_width = grads.shape[-1] // 2
    first_half = grads[..., :half_width]
    second_half = grads[..., half_width:]
    cos_rows = cosine[:, None, :]
    sin_rows = sine[:, None, :]
    return jnp.concatenate([first_half * cos_rows + second_half * sin_rows, second_half * cos_rows - first_half * sin_rows], axis=-1)

def rms_forward(values, gain):
    recip = lax.rsqrt(lax.optimization_barrier(jnp.mean(values * values, axis=-1, keepdims=True)) + EPSILON)
    x_hat = values * recip
    return (x_hat, recip, x_hat * gain)

def rms_backward(grad_normed, x_hat, recip, gain):
    grad_hat = grad_normed * gain
    grad_gain = lax.optimization_barrier(jnp.sum(grad_normed * x_hat, axis=0))
    inner = lax.optimization_barrier(jnp.mean(grad_hat * x_hat, axis=-1, keepdims=True))
    return (recip * (grad_hat - x_hat * inner), grad_gain)

def allowed_mask(segment_row, first_row, block_rows):
    total_len = segment_row.shape[0]
    query_index = first_row + jnp.arange(block_rows, dtype=jnp.int32)
    key_index = jnp.arange(total_len, dtype=jnp.int32)
    query_segs = lax.dynamic_slice_in_dim(segment_row, first_row, block_rows, 0)
    return (key_index[None, :] <= query_index[:, None]) & (segment_row[None, :] == query_segs[:, None])

def attend(query_rot, key_rot, value_b, segment_row):
    total_len, heads, width = query_rot.shape
    groups = key_rot.shape[1]
    ratio = heads // groups
    block_rows = min(512, total_len)
    scale = 1.0 / math.sqrt(width)
    quads = query_rot.reshape(total_len, groups, ratio, width)
    key_f = key_rot.astype(jnp.float32)
    value_f = value_b.astype(jnp.float32)

    def one_block(first_row):
        query_blk = lax.dynamic_slice_in_dim(quads, first_row, block_rows, 0).astype(jnp.float32)
        scores = jnp.einsum('qkgd,tkd->kgqt', query_blk, key_f) * scale
        scores = jnp.where(allowed_mask(segment_row, first_row, block_rows)[None, None], scores, MASKED)
        top_score = lax.optimization_barrier(jnp.max(scores, axis=-1, keepdims=True))
        log_total = top_score + jnp.log(lax.optimization_barrier(jnp.sum(jnp.exp(scores - top_score), axis=-1, keepdims=True)))
        probs = jnp.exp(scores - log_total)
        probs_b = as_bf16(probs).astype(jnp.float32)
        mixed = jnp.einsum('kgqt,tkd->qkgd', probs_b, value_f)
        return (as_bf16(mixed.reshape(block_rows, heads * width)), log_total[..., 0])
    starts = jnp.arange(total_len // block_rows, dtype=jnp.int32) * block_rows
    outs, log_totals = lax.map(one_block, starts)
    return (outs.reshape(total_len, heads * width), log_totals)

def attend_back(query_rot, key_rot, value_b, segment_row, log_totals, grad_att):
    total_len, heads, width = query_rot.shape
    groups = key_rot.shape[1]
    ratio = heads // groups
    block_rows = min(512, total_len)
    scale = 1.0 / math.sqrt(width)
    quads = query_rot.reshape(total_len, groups, ratio, width)
    grad_quads = grad_att.reshape(total_len, groups, ratio, width)
    key_f = key_rot.astype(jnp.float32)
    value_f = value_b.astype(jnp.float32)

    def one_block(carry, inputs):
        grad_key, grad_value = carry
        first_row, log_total = inputs
        query_blk = lax.dynamic_slice_in_dim(quads, first_row, block_rows, 0).astype(jnp.float32)
        grad_blk = lax.dynamic_slice_in_dim(grad_quads, first_row, block_rows, 0).astype(jnp.float32)
        scores = jnp.einsum('qkgd,tkd->kgqt', query_blk, key_f) * scale
        scores = jnp.where(allowed_mask(segment_row, first_row, block_rows)[None, None], scores, MASKED)
        probs = jnp.exp(scores - log_total[..., None])
        probs_b = as_bf16(probs).astype(jnp.float32)
        grad_probs = jnp.einsum('qkgd,tkd->kgqt', grad_blk, value_f)
        delta = lax.optimization_barrier(jnp.sum(probs * grad_probs, axis=-1, keepdims=True))
        grad_scores = as_bf16(probs * (grad_probs - delta) * scale).astype(jnp.float32)
        grad_query = jnp.einsum('kgqt,tkd->qkgd', grad_scores, key_f)
        grad_key = grad_key + jnp.einsum('kgqt,qkgd->tkd', grad_scores, query_blk)
        grad_value = grad_value + jnp.einsum('kgqt,qkgd->tkd', probs_b, grad_blk)
        return ((grad_key, grad_value), grad_query)
    starts = jnp.arange(total_len // block_rows, dtype=jnp.int32) * block_rows
    zeros_kv = jnp.zeros((total_len, groups, width), jnp.float32)
    (grad_key, grad_value), grad_queries = lax.scan(one_block, (zeros_kv, zeros_kv), (starts, log_totals))
    return (grad_queries.reshape(total_len, heads, width), grad_key, grad_value)

def reference(layer_input, segments, gain_attn, w_query, w_key, w_value, w_out, gain_ffn, w_gate, w_up, w_down, cotangent):
    seq_count, total_len = segments.shape
    width = layer_input.shape[1]
    rows_all = layer_input.reshape(seq_count, total_len, width)
    cots_all = cotangent.reshape(seq_count, total_len, width)

    def one_sequence(carry, inputs):
        acc_g1, acc_query, acc_key, acc_value, acc_out, acc_g2, acc_gate, acc_up, acc_down = carry
        rows, segment_row, cot_rows = inputs
        cosine, sine = rotary_tables(doc_positions(segment_row), HD)
        x_float = rows.astype(jnp.float32)
        x_hat1, recip1, normed1 = rms_forward(x_float, gain_attn)
        normed1 = as_bf16(normed1)
        query = jnp.dot(normed1, w_query, preferred_element_type=jnp.float32).reshape(total_len, H, HD)
        keys = jnp.dot(normed1, w_key, preferred_element_type=jnp.float32).reshape(total_len, KV, HD)
        values = jnp.dot(normed1, w_value, preferred_element_type=jnp.float32).reshape(total_len, KV, HD)
        query_rot = as_bf16(rotate(query, cosine, sine))
        key_rot = as_bf16(rotate(keys, cosine, sine))
        value_b = as_bf16(values)
        attended, log_totals = attend(query_rot, key_rot, value_b, segment_row)
        resid = x_float + jnp.dot(attended, w_out, preferred_element_type=jnp.float32)
        x_hat2, recip2, normed2 = rms_forward(resid, gain_ffn)
        normed2 = as_bf16(normed2)
        gate = jnp.dot(normed2, w_gate, preferred_element_type=jnp.float32)
        up_part = jnp.dot(normed2, w_up, preferred_element_type=jnp.float32)
        sig_gate = jax.nn.sigmoid(gate)
        hidden = as_bf16(gate * sig_gate * up_part)
        result = (resid + jnp.dot(hidden, w_down, preferred_element_type=jnp.float32)).astype(jnp.bfloat16)
        grad_hidden = jnp.dot(cot_rows, w_down.T, preferred_element_type=jnp.float32)
        grad_gate = as_bf16(grad_hidden * up_part * sig_gate * (1.0 + gate * (1.0 - sig_gate)))
        grad_upp = as_bf16(grad_hidden * gate * sig_gate)
        grad_normed2 = jnp.dot(grad_gate, w_gate.T, preferred_element_type=jnp.float32) + jnp.dot(grad_upp, w_up.T, preferred_element_type=jnp.float32)
        grad_norm2, grad_g2 = rms_backward(grad_normed2, x_hat2, recip2, gain_ffn)
        grad_resid = cot_rows.astype(jnp.float32) + grad_norm2
        grad_resid_b = as_bf16(grad_resid)
        grad_att = as_bf16(jnp.dot(grad_resid_b, w_out.T, preferred_element_type=jnp.float32))
        grad_qrot, grad_krot, grad_val = attend_back(query_rot, key_rot, value_b, segment_row, log_totals, grad_att)
        grad_q = as_bf16(rotate_back(grad_qrot, cosine, sine)).reshape(total_len, H * HD)
        grad_k = as_bf16(rotate_back(grad_krot, cosine, sine)).reshape(total_len, KV * HD)
        grad_v = as_bf16(grad_val).reshape(total_len, KV * HD)
        grad_normed1 = jnp.dot(grad_q, w_query.T, preferred_element_type=jnp.float32) + jnp.dot(grad_k, w_key.T, preferred_element_type=jnp.float32) + jnp.dot(grad_v, w_value.T, preferred_element_type=jnp.float32)
        grad_norm1, grad_g1 = rms_backward(grad_normed1, x_hat1, recip1, gain_attn)
        grad_rows = grad_resid + grad_norm1
        new_carry = (acc_g1 + grad_g1, acc_query + jnp.dot(normed1.T, grad_q, preferred_element_type=jnp.float32), acc_key + jnp.dot(normed1.T, grad_k, preferred_element_type=jnp.float32), acc_value + jnp.dot(normed1.T, grad_v, preferred_element_type=jnp.float32), acc_out + jnp.dot(attended.T, grad_resid_b, preferred_element_type=jnp.float32), acc_g2 + grad_g2, acc_gate + jnp.dot(normed2.T, grad_gate, preferred_element_type=jnp.float32), acc_up + jnp.dot(normed2.T, grad_upp, preferred_element_type=jnp.float32), acc_down + jnp.dot(hidden.T, cot_rows, preferred_element_type=jnp.float32))
        return (new_carry, (result, grad_rows))
    init = (jnp.zeros((D,), jnp.float32), jnp.zeros((D, H * HD), jnp.float32), jnp.zeros((D, KV * HD), jnp.float32), jnp.zeros((D, KV * HD), jnp.float32), jnp.zeros((H * HD, D), jnp.float32), jnp.zeros((D,), jnp.float32), jnp.zeros((D, FF), jnp.float32), jnp.zeros((D, FF), jnp.float32), jnp.zeros((FF, D), jnp.float32))
    sums, (results, grad_rows) = lax.scan(one_sequence, init, (rows_all, segments, cots_all))
    grad_g1, grad_query, grad_key, grad_value, grad_out, grad_g2, grad_gate, grad_up, grad_down = sums
    return (results.reshape(layer_input.shape), grad_rows.reshape(layer_input.shape), grad_g1, grad_query, grad_key, grad_value, grad_out, grad_g2, grad_gate, grad_up, grad_down)
```

```python
import math

import jax
import jax.numpy as jnp
from jax import lax
from jax.sharding import Mesh
from jax.sharding import PartitionSpec as P

HD = 96


EPSILON = 1e-05
ROPE_BASE = 100000.0
MASKED = -1e30


def lead_product(left_arr, right_arr):
    return lax.dot_general(
        left_arr, right_arr, (((0,), (0,)), ((), ())), preferred_element_type=jnp.float32
    )


def tail_product(left_arr, right_arr):
    return lax.dot_general(
        left_arr, right_arr, (((1,), (1,)), ((), ())), preferred_element_type=jnp.float32
    )


def plain_product(left_arr, right_arr):
    return jnp.dot(left_arr, right_arr, preferred_element_type=jnp.float32)


def doc_positions(segment_row):
    total_len = segment_row.shape[0]
    indices = jnp.arange(total_len, dtype=jnp.int32)
    changes = jnp.concatenate([jnp.ones((1,), dtype=bool), segment_row[1:] != segment_row[:-1]])
    starts = jnp.where(changes, indices, jnp.zeros_like(indices))
    return indices - lax.cummax(starts, axis=0)


def rotary_tables(positions, head_width):
    half_width = head_width // 2
    frequency = jnp.exp(
        -math.log(ROPE_BASE) * 2.0 * jnp.arange(half_width, dtype=jnp.float32) / head_width
    )
    angles = positions.astype(jnp.float32)[:, None] * frequency[None, :]
    return (jnp.cos(angles), jnp.sin(angles))


def rotate(values, cosine, sine):
    half_width = values.shape[-1] // 2
    first_half = values[..., :half_width]
    second_half = values[..., half_width:]
    cos_rows = cosine[:, None, :]
    sin_rows = sine[:, None, :]
    return jnp.concatenate(
        [
            first_half * cos_rows - second_half * sin_rows,
            second_half * cos_rows + first_half * sin_rows,
        ],
        axis=-1,
    )


def rotate_back(grads, cosine, sine):
    half_width = grads.shape[-1] // 2
    first_half = grads[..., :half_width]
    second_half = grads[..., half_width:]
    cos_rows = cosine[:, None, :]
    sin_rows = sine[:, None, :]
    return jnp.concatenate(
        [
            first_half * cos_rows + second_half * sin_rows,
            second_half * cos_rows - first_half * sin_rows,
        ],
        axis=-1,
    )


def rms_forward(values, gain):
    recip = lax.rsqrt(jnp.mean(values * values, axis=-1, keepdims=True) + EPSILON)
    x_hat = values * recip
    return (x_hat, recip, (x_hat * gain).astype(jnp.bfloat16))


def rms_backward(grad_normed, x_hat, recip, gain):
    grad_hat = grad_normed * gain
    grad_gain = jnp.sum(grad_normed * x_hat, axis=0)
    inner = jnp.mean(grad_hat * x_hat, axis=-1, keepdims=True)
    return (recip * (grad_hat - x_hat * inner), grad_gain)


def allowed_mask(segment_row, first_row, block_rows):
    total_len = segment_row.shape[0]
    query_index = first_row + jnp.arange(block_rows, dtype=jnp.int32)
    key_index = jnp.arange(total_len, dtype=jnp.int32)
    return (key_index[None, :] <= query_index[:, None]) & (
        segment_row[None, :] == segment_row[:, None]
    )


def attend(inputs):
    query_rot, key_rot, value_b, segment_row = inputs
    total_len, heads, width = query_rot.shape
    groups = key_rot.shape[1]
    ratio = heads // groups
    block_rows = min(512, total_len)
    scale = 1.0 / math.sqrt(width)
    quads = query_rot.reshape(total_len, groups, ratio, width)

    def one_block(first_row):
        scores = (
            jnp.einsum("qkgd,tkd->kgqt", quads, key_rot, preferred_element_type=jnp.float32) * scale
        )
        scores = jnp.where(
            allowed_mask(segment_row, first_row, block_rows)[None, None], scores, MASKED
        )
        top_score = jnp.max(scores, axis=-1, keepdims=True)
        log_total = top_score + jnp.log(
            jnp.sum(jnp.exp(scores - top_score), axis=-1, keepdims=True)
        )
        probs_b = jnp.exp(scores - log_total).astype(jnp.bfloat16)
        mixed = jnp.einsum("kgqt,tkd->qkgd", probs_b, value_b, preferred_element_type=jnp.float32)
        return (mixed.reshape(block_rows, heads * width).astype(jnp.bfloat16), log_total[..., 0])

    starts = jnp.arange(total_len // block_rows, dtype=jnp.int32) * block_rows
    outs, log_totals = lax.map(one_block, starts)
    return (outs.reshape(total_len, heads * width), log_totals)


def attend_back(inputs):
    query_rot, key_rot, value_b, segment_row, log_totals, grad_att = inputs
    total_len, heads, width = query_rot.shape
    groups = key_rot.shape[1]
    ratio = heads // groups
    block_rows = min(512, total_len)
    scale = 1.0 / math.sqrt(width)
    quads = query_rot.reshape(total_len, groups, ratio, width)
    grad_quads = grad_att.reshape(total_len, groups, ratio, width)

    def one_block(carry, block_in):
        grad_key, grad_value = carry
        first_row, log_total = block_in
        scores = (
            jnp.einsum("qkgd,tkd->kgqt", quads, key_rot, preferred_element_type=jnp.float32) * scale
        )
        scores = jnp.where(
            allowed_mask(segment_row, first_row, block_rows)[None, None], scores, MASKED
        )
        probs = jnp.exp(scores - log_total[..., None])
        probs_b = probs.astype(jnp.bfloat16)
        grad_probs = jnp.einsum(
            "qkgd,tkd->kgqt", grad_quads, value_b, preferred_element_type=jnp.float32
        )
        delta = jnp.sum(probs * grad_probs, axis=-1, keepdims=True)
        grad_scores = (probs * (grad_probs - delta) * scale).astype(jnp.bfloat16)
        grad_query = jnp.einsum(
            "kgqt,tkd->qkgd", grad_scores, key_rot, preferred_element_type=jnp.float32
        )
        grad_key = grad_key + jnp.einsum(
            "kgqt,qkgd->tkd", grad_scores, quads, preferred_element_type=jnp.float32
        )
        grad_value = grad_value + jnp.einsum(
            "kgqt,qkgd->tkd", probs_b, grad_quads, preferred_element_type=jnp.float32
        )
        return ((grad_key, grad_value), grad_query)

    starts = jnp.arange(total_len // block_rows, dtype=jnp.int32) * block_rows
    zeros_kv = jnp.zeros((total_len, groups, width), jnp.float32)
    (grad_key, grad_value), grad_queries = lax.scan(
        one_block, (zeros_kv, zeros_kv), (starts, log_totals)
    )
    return (grad_queries.reshape(total_len, heads, width), grad_key, grad_value)


def shifted(value, axis, size, step):
    return lax.ppermute(value, axis, [(i, (i + step) % size) for i in range(size)])


def moved(value, axis, size, step):
    pairs = [(i, i + step) for i in range(size) if 0 <= i + step < size]
    return lax.ppermute(value, axis, pairs)


def crossed(value):
    return lax.ppermute(value, ("y", "x"), [(0, 3), (1, 2), (2, 1), (3, 0)])


def flipped(value, axis):
    return lax.ppermute(value, axis, [(0, 1), (1, 0)])


def placed(blocks, indices, total):
    out = jnp.zeros((total,) + blocks[0].shape, blocks[0].dtype)
    for block, index in zip(blocks, indices):
        out = lax.dynamic_update_index_in_dim(out, block, index, 0)
    return out


def pair_rows(value, it):
    rows = value.shape[0]
    out = placed([value, flipped(value, "t")], [it, 1 - it], 2)
    return out.reshape((2 * rows,) + value.shape[1:])


def plane_blocks(value):
    return [value, flipped(value, "x"), flipped(value, "y"), crossed(value)]


def plane_exchange(blocks):
    return [blocks[0], flipped(blocks[1], "x"), flipped(blocks[2], "y"), crossed(blocks[3])]


def picked(value, index):
    return lax.dynamic_index_in_dim(value, index, 0, keepdims=False)


def make_local(depth):
    def local(
        layer_input,
        segments,
        gain_attn,
        w_query,
        w_key,
        w_value,
        w_out,
        gain_ffn,
        w_gate,
        w_up,
        w_down,
        cotangent,
    ):
        bf16 = jnp.bfloat16
        iz, it = lax.axis_index("z"), lax.axis_index("t")
        ip = lax.axis_index("y") * 2 + lax.axis_index("x")
        seqs_here, total_len = segments.shape
        own_rows, width = layer_input.shape
        wrows = w_query.shape[0]
        qcols, kcols = w_query.shape[1], w_key.shape[1]
        fcols = w_gate.shape[1]
        fq = fcols // 4
        ffn_pack = jnp.stack(
            [w_gate.reshape(wrows, 4, fq), w_up.reshape(wrows, 4, fq), w_down.T.reshape(wrows, 4, fq)],
            axis=2,
        )
        ffn_pack = jnp.transpose(ffn_pack, (1, 0, 2, 3)).reshape(4, wrows, 3 * fq)
        sent = [picked(ffn_pack, ip ^ k) for k in range(4)]
        came = plane_exchange(sent)
        ffn_plane = placed(came, [ip ^ k for k in range(4)], 4)
        ffn_plane = ffn_plane.reshape(4 * wrows, 3 * fq)
        ffn_all = placed(
            [ffn_plane] + [shifted(ffn_plane, "z", depth, s) for s in range(1, depth)],
            [(iz - s) % depth for s in range(depth)],
            depth,
        ).reshape(width, 3 * fq)
        full_gate, full_up, full_down = (
            ffn_all[:, :fq],
            ffn_all[:, fq : 2 * fq],
            ffn_all[:, 2 * fq :],
        )
        attn_pack = jnp.concatenate([w_query, w_key, w_value, w_out.T], axis=1)
        attn_all = lax.all_gather(attn_pack, ("z", "y", "x"), axis=0, tiled=True)
        full_query = attn_all[:, :qcols]
        full_key = attn_all[:, qcols : qcols + kcols]
        full_value = attn_all[:, qcols + kcols : qcols + 2 * kcols]
        full_out = attn_all[:, qcols + 2 * kcols :]

        x_float = layer_input.astype(jnp.float32)
        x_hat1, recip1, normed1 = rms_forward(x_float, gain_attn)
        normed_seq = pair_rows(normed1, it)
        positions = jax.vmap(doc_positions)(segments).reshape(total_len)
        cosine, sine = rotary_tables(positions, HD)
        query = plain_product(normed_seq, full_query).reshape(total_len, -1, HD)
        keys = plain_product(normed_seq, full_key).reshape(total_len, -1, HD)
        values = plain_product(normed_seq, full_value).reshape(total_len, -1, HD)
        heads_here, groups_here = query.shape[1], keys.shape[1]
        query_rot = rotate(query, cosine, sine).astype(bf16)
        key_rot = rotate(keys, cosine, sine).astype(bf16)
        value_b = values.astype(bf16)
        attended, log_totals = attend((query_rot, key_rot, value_b, segments[0]))
        mixed = tail_product(attended, full_out).reshape(2, own_rows, width)
        resid = x_float + (picked(mixed, it) + flipped(picked(mixed, 1 - it), "t"))
        x_hat2, recip2, normed2 = rms_forward(resid, gain_ffn)

        def plane_rows(value):
            blocks = jnp.stack(plane_blocks(value))
            both = jnp.stack([blocks, flipped(blocks, "t")], axis=1)
            return both.reshape(8 * value.shape[0], value.shape[1])

        normed_ffn = plane_rows(normed2)
        cot_all = plane_rows(cotangent)
        gate = plain_product(normed_ffn, full_gate)
        up_part = plain_product(normed_ffn, full_up)
        sig_gate = jax.nn.sigmoid(gate)
        hidden = (gate * sig_gate * up_part).astype(bf16)
        grad_hidden = plain_product(cot_all, full_down)
        grad_gate_b = (grad_hidden * up_part * sig_gate * (1.0 + gate * (1.0 - sig_gate))).astype(bf16)
        grad_up_b = (grad_hidden * gate * sig_gate).astype(bf16)

        def plane_sum(partial, narrow):
            tiles = partial.reshape(4, 2, own_rows, width)
            mine = tiles[:, 0] + flipped(tiles[:, 1].astype(narrow), "t").astype(jnp.float32)
            back = plane_exchange([mine[0]] + [mine[k].astype(narrow) for k in range(1, 4)])
            return ((back[0] + back[1].astype(jnp.float32)) + back[2].astype(jnp.float32)) + back[3].astype(
                jnp.float32
            )

        grad_normed2 = plane_sum(
            tail_product(grad_gate_b, full_gate) + tail_product(grad_up_b, full_up), jnp.float32
        )
        result = (resid + plane_sum(tail_product(hidden, full_down), bf16)).astype(bf16)

        def z_sum(grads):
            cols = grads.shape[1]
            blocks = grads.reshape(depth, 4 * wrows, cols)
            total = picked(blocks, iz)
            for s in range(1, depth):
                piece = picked(blocks, (iz + s) % depth).astype(bf16)
                total = total + shifted(piece, "z", depth, s).astype(jnp.float32)
            return total.reshape(4, wrows, cols)

        def to_owner(sums):
            back = plane_exchange([picked(sums, ip ^ k) for k in range(4)])
            return placed(back, [ip ^ k for k in range(4)], 4)

        ffn_grads = jnp.concatenate(
            [
                lead_product(normed_ffn, grad_gate_b),
                lead_product(normed_ffn, grad_up_b),
                lead_product(cot_all, hidden),
            ],
            axis=1,
        )
        ffn_sums = to_owner(z_sum(ffn_grads))
        ffn_sums = jnp.transpose(ffn_sums.reshape(4, wrows, 3, fq), (2, 1, 0, 3)).reshape(3, wrows, fcols)

        grad_norm2, grad_g2 = rms_backward(grad_normed2, x_hat2, recip2, gain_ffn)
        grad_resid = cotangent.astype(jnp.float32) + grad_norm2
        grad_resid_b = grad_resid.astype(bf16)
        grad_resid_seq = pair_rows(grad_resid_b, it)
        grad_att = plain_product(grad_resid_seq, full_out).astype(bf16)
        grad_qrot, grad_krot, grad_val = attend_back(
            (query_rot, key_rot, value_b, segments[0], log_totals, grad_att)
        )
        grad_q = rotate_back(grad_qrot, cosine, sine).astype(bf16).reshape(total_len, qcols)
        grad_k = rotate_back(grad_krot, cosine, sine).astype(bf16).reshape(total_len, kcols)
        grad_v = grad_val.astype(bf16).reshape(total_len, kcols)
        dn1 = (
            tail_product(grad_q, full_query) + tail_product(grad_k, full_key) + tail_product(grad_v, full_value)
        ).reshape(2, own_rows, width)
        grad_normed1 = picked(dn1, it) + flipped(picked(dn1, 1 - it).astype(bf16), "t").astype(jnp.float32)
        grad_norm1, grad_g1 = rms_backward(grad_normed1, x_hat1, recip1, gain_attn)
        grad_rows = grad_resid + grad_norm1

        qq, kq = qcols // 4, kcols // 4
        tok = jnp.concatenate(
            [
                grad_q.reshape(total_len, 4, qq),
                grad_k.reshape(total_len, 4, kq),
                grad_v.reshape(total_len, 4, kq),
                attended.reshape(total_len, 4, qq),
            ],
            axis=2,
        )
        tok = jnp.transpose(tok, (1, 0, 2))
        tok_all = jnp.concatenate(plane_exchange([picked(tok, ip ^ k) for k in range(4)]), axis=0)

        def plane_seqs(value):
            blocks = jnp.stack(plane_blocks(value))
            both = placed([blocks, flipped(blocks, "t")], [it, 1 - it], 2)
            return jnp.transpose(both, (1, 0, 2, 3)).reshape(4 * total_len, width)

        normed_plane = plane_seqs(normed1)
        resid_plane = plane_seqs(grad_resid_b)
        cut = qq + 2 * kq
        attn_grads = jnp.concatenate(
            [lead_product(normed_plane, tok_all[:, :cut]), lead_product(resid_plane, tok_all[:, cut:])], axis=1
        )
        attn_sums = to_owner(z_sum(attn_grads))

        def columns(start, count):
            part = attn_sums[:, :, start : start + count]
            return jnp.transpose(part, (1, 0, 2)).reshape(wrows, 4 * count)

        total_g1, total_g2 = lax.psum((grad_g1, grad_g2), ("z", "y", "x", "t"))
        return (
            result,
            grad_rows,
            total_g1,
            columns(0, qq),
            columns(qq, kq),
            columns(qq + kq, kq),
            columns(cut, qq).T,
            total_g2,
            ffn_sums[0],
            ffn_sums[1],
            ffn_sums[2].T,
        )

    return local


def solution(mesh):
    ring = mesh.shape["dp"]
    fine = Mesh(mesh.devices.reshape(ring // 4, 2, 2, mesh.shape["tensor"]), ("z", "y", "x", "t"))
    dp, every = ("z", "y", "x"), ("z", "y", "x", "t")
    return jax.shard_map(
        make_local(ring // 4),
        mesh=fine,
        in_specs=(
            P(every, None),
            P(dp, None),
            P(),
            P(dp, "t"),
            P(dp, "t"),
            P(dp, "t"),
            P("t", dp),
            P(),
            P(dp, "t"),
            P(dp, "t"),
            P("t", dp),
            P(every, None),
        ),
        out_specs=(
            P(every, None),
            P(every, None),
            P(),
            P(dp, "t"),
            P(dp, "t"),
            P(dp, "t"),
            P("t", dp),
            P(),
            P(dp, "t"),
            P(dp, "t"),
            P("t", dp),
        ),
        check_vma=False,
    )
```

```python
import functools
import math

import jax
import jax.numpy as jnp
from jax import lax
from jax.experimental import pallas as pl
from jax.experimental.pallas import tpu as pltpu
from jax.sharding import Mesh
from jax.sharding import PartitionSpec as P

HD = 96


EPSILON = 1e-05
ROPE_BASE = 100000.0
MASKED = -1e30


def lead_product(left_arr, right_arr):
    return lax.dot_general(
        left_arr, right_arr, (((0,), (0,)), ((), ())), preferred_element_type=jnp.float32
    )


def tail_product(left_arr, right_arr):
    return lax.dot_general(
        left_arr, right_arr, (((1,), (1,)), ((), ())), preferred_element_type=jnp.float32
    )


def plain_product(left_arr, right_arr):
    return jnp.dot(left_arr, right_arr, preferred_element_type=jnp.float32)


def doc_positions(segment_row):
    total_len = segment_row.shape[0]
    indices = jnp.arange(total_len, dtype=jnp.int32)
    changes = jnp.concatenate([jnp.ones((1,), dtype=bool), segment_row[1:] != segment_row[:-1]])
    starts = jnp.where(changes, indices, jnp.zeros_like(indices))
    return indices - lax.cummax(starts, axis=0)


def rotary_tables(positions, head_width):
    half_width = head_width // 2
    frequency = jnp.exp(
        -math.log(ROPE_BASE) * 2.0 * jnp.arange(half_width, dtype=jnp.float32) / head_width
    )
    angles = positions.astype(jnp.float32)[:, None] * frequency[None, :]
    return (jnp.cos(angles), jnp.sin(angles))


def rotate(values, cosine, sine):
    half_width = values.shape[-1] // 2
    first_half = values[..., :half_width]
    second_half = values[..., half_width:]
    cos_rows = cosine[:, None, :]
    sin_rows = sine[:, None, :]
    return jnp.concatenate(
        [
            first_half * cos_rows - second_half * sin_rows,
            second_half * cos_rows + first_half * sin_rows,
        ],
        axis=-1,
    )


def rotate_back(grads, cosine, sine):
    half_width = grads.shape[-1] // 2
    first_half = grads[..., :half_width]
    second_half = grads[..., half_width:]
    cos_rows = cosine[:, None, :]
    sin_rows = sine[:, None, :]
    return jnp.concatenate(
        [
            first_half * cos_rows + second_half * sin_rows,
            second_half * cos_rows - first_half * sin_rows,
        ],
        axis=-1,
    )


def rms_forward(values, gain):
    recip = lax.rsqrt(jnp.mean(values * values, axis=-1, keepdims=True) + EPSILON)
    x_hat = values * recip
    return (x_hat, recip, (x_hat * gain).astype(jnp.bfloat16))


def rms_backward(grad_normed, x_hat, recip, gain):
    grad_hat = grad_normed * gain
    grad_gain = jnp.sum(grad_normed * x_hat, axis=0)
    inner = jnp.mean(grad_hat * x_hat, axis=-1, keepdims=True)
    return (recip * (grad_hat - x_hat * inner), grad_gain)


def allowed_mask(segment_row, first_row, block_rows):
    total_len = segment_row.shape[0]
    query_index = first_row + jnp.arange(block_rows, dtype=jnp.int32)
    key_index = jnp.arange(total_len, dtype=jnp.int32)
    return (key_index[None, :] <= query_index[:, None]) & (
        segment_row[None, :] == segment_row[:, None]
    )


def attend(inputs):
    query_rot, key_rot, value_b, segment_row = inputs
    total_len, heads, width = query_rot.shape
    groups = key_rot.shape[1]
    ratio = heads // groups
    block_rows = min(512, total_len)
    scale = 1.0 / math.sqrt(width)
    quads = query_rot.reshape(total_len, groups, ratio, width)

    def one_block(first_row):
        scores = (
            jnp.einsum("qkgd,tkd->kgqt", quads, key_rot, preferred_element_type=jnp.float32) * scale
        )
        scores = jnp.where(
            allowed_mask(segment_row, first_row, block_rows)[None, None], scores, MASKED
        )
        top_score = jnp.max(scores, axis=-1, keepdims=True)
        log_total = top_score + jnp.log(
            jnp.sum(jnp.exp(scores - top_score), axis=-1, keepdims=True)
        )
        probs_b = jnp.exp(scores - log_total).astype(jnp.bfloat16)
        mixed = jnp.einsum("kgqt,tkd->qkgd", probs_b, value_b, preferred_element_type=jnp.float32)
        return (mixed.reshape(block_rows, heads * width).astype(jnp.bfloat16), log_total[..., 0])

    starts = jnp.arange(total_len // block_rows, dtype=jnp.int32) * block_rows
    outs, log_totals = lax.map(one_block, starts)
    return (outs.reshape(total_len, heads * width), log_totals)


def attend_back(inputs):
    query_rot, key_rot, value_b, segment_row, log_totals, grad_att = inputs
    total_len, heads, width = query_rot.shape
    groups = key_rot.shape[1]
    ratio = heads // groups
    block_rows = min(512, total_len)
    scale = 1.0 / math.sqrt(width)
    quads = query_rot.reshape(total_len, groups, ratio, width)
    grad_quads = grad_att.reshape(total_len, groups, ratio, width)

    def one_block(carry, block_in):
        grad_key, grad_value = carry
        first_row, log_total = block_in
        scores = (
            jnp.einsum("qkgd,tkd->kgqt", quads, key_rot, preferred_element_type=jnp.float32) * scale
        )
        scores = jnp.where(
            allowed_mask(segment_row, first_row, block_rows)[None, None], scores, MASKED
        )
        probs = jnp.exp(scores - log_total[..., None])
        probs_b = probs.astype(jnp.bfloat16)
        grad_probs = jnp.einsum(
            "qkgd,tkd->kgqt", grad_quads, value_b, preferred_element_type=jnp.float32
        )
        delta = jnp.sum(probs * grad_probs, axis=-1, keepdims=True)
        grad_scores = (probs * (grad_probs - delta) * scale).astype(jnp.bfloat16)
        grad_query = jnp.einsum(
            "kgqt,tkd->qkgd", grad_scores, key_rot, preferred_element_type=jnp.float32
        )
        grad_key = grad_key + jnp.einsum(
            "kgqt,qkgd->tkd", grad_scores, quads, preferred_element_type=jnp.float32
        )
        grad_value = grad_value + jnp.einsum(
            "kgqt,qkgd->tkd", probs_b, grad_quads, preferred_element_type=jnp.float32
        )
        return ((grad_key, grad_value), grad_query)

    starts = jnp.arange(total_len // block_rows, dtype=jnp.int32) * block_rows
    zeros_kv = jnp.zeros((total_len, groups, width), jnp.float32)
    (grad_key, grad_value), grad_queries = lax.scan(
        one_block, (zeros_kv, zeros_kv), (starts, log_totals)
    )
    return (grad_queries.reshape(total_len, heads, width), grad_key, grad_value)


MESH = pl.DeviceIdType.MESH


def remote(src, dst, send_sem, recv_sem, where):
    return pltpu.make_async_remote_copy(
        src_ref=src, dst_ref=dst, send_sem=send_sem, recv_sem=recv_sem, device_id=where, device_id_type=MESH
    )


def greet(targets):
    barrier = pltpu.get_barrier_semaphore()
    for where in targets:
        pl.semaphore_signal(barrier, inc=1, device_id=where, device_id_type=MESH)
    pl.semaphore_wait(barrier, len(targets))


def gather_kernel(depth, a_ref, b_ref, f_ref, fa, fb, ff, zs, zr, ps, pr, fs, fr, vs, vr, local_sem):
    z, y, x = lax.axis_index("z"), lax.axis_index("y"), lax.axis_index("x")
    to_x, to_y, to_d = {"x": 1 - x}, {"y": 1 - y}, {"y": 1 - y, "x": 1 - x}
    me, mx, my = 2 * y + x, 2 * y + 1 - x, 2 - 2 * y + x
    md = 3 - me
    up, down = z + 1 < depth, z > 0
    ahead = (up, down)
    to_z = ({"z": z + 1}, {"z": z - 1})
    barrier = pltpu.get_barrier_semaphore()
    for where in (to_x, to_y, to_d):
        pl.semaphore_signal(barrier, inc=1, device_id=where, device_id_type=MESH)
    for side in range(2):

        @pl.when(ahead[side])
        def _(side=side):
            pl.semaphore_signal(barrier, inc=1, device_id=to_z[side], device_id_type=MESH)

    pl.semaphore_wait(barrier, 3 + jnp.minimum(z, 1) + jnp.minimum(depth - 1 - z, 1))

    def block(side, step):
        return z - step if side == 0 else z + step

    def present(side, step):
        return z >= step if side == 0 else z + step < depth

    def along(side, step):
        at = block(side, step)
        return [
            remote(
                own if step == 0 else full.at[at, me],
                full.at[at, me],
                zs.at[side, step, c],
                zr.at[side, step, c],
                to_z[side],
            )
            for c, (own, full) in enumerate(((a_ref, fa), (b_ref, fb)))
        ]

    def across(side, step):
        at = block(side, step)
        src_a = a_ref if step == 0 else fa.at[at, me]
        src_b = b_ref if step == 0 else fb.at[at, me]
        routes = ((src_a, fa, to_x), (src_b, fb, to_y), (src_b, fb, to_x), (src_a, fa, to_y))
        return [
            remote(src, full.at[at, me], ps.at[side, step, n], pr.at[side, step, n], where)
            for n, (src, full, where) in enumerate(routes)
        ]

    def relay(side, step):
        at = block(side, step)
        return [
            remote(fa.at[at, mx], fa.at[at, mx], ps.at[side, step, 4], pr.at[side, step, 4], to_y),
            remote(fb.at[at, my], fb.at[at, my], ps.at[side, step, 5], pr.at[side, step, 5], to_x),
        ]

    locals_ = [
        pltpu.make_async_copy(a_ref, fa.at[z, me], local_sem.at[0]),
        pltpu.make_async_copy(b_ref, fb.at[z, me], local_sem.at[1]),
        pltpu.make_async_copy(f_ref.at[me], ff.at[z, me], local_sem.at[2]),
    ]
    quarters = [
        remote(f_ref.at[slot], ff.at[z, me], fs.at[n], fr.at[n], where)
        for n, (slot, where) in enumerate(((mx, to_x), (my, to_y), (md, to_d)))
    ]
    whole = [remote(ff.at[z], ff.at[z], vs.at[n], vr.at[n], to_z[n]) for n in range(2)]
    for side in range(2):

        @pl.when(ahead[side])
        def _(side=side):
            for copy in along(side, 0):
                copy.start()

    for copy in across(0, 0) + locals_ + quarters:
        copy.start()

    def sides(step):
        return (0,) if step == 0 else (0, 1)

    def pass_on(step):
        for side in sides(step):

            @pl.when(present(side, step))
            def _(side=side):
                first, sent = across(side, step), relay(side, step)
                first[0].wait_recv()
                sent[0].start()
                first[1].wait_recv()
                sent[1].start()

    for step in range(1, depth):
        for side in (0, 1):

            @pl.when(present(side, step))
            def _(side=side):
                for copy in along(side, step - 1):
                    copy.wait_recv()
                if step < depth - 1:

                    @pl.when(ahead[side])
                    def _():
                        for copy in along(side, step):
                            copy.start()

                for copy in across(side, step):
                    copy.start()

        pass_on(step - 1)
    for copy in quarters:
        copy.wait_recv()
    locals_[2].wait()
    for side in range(2):

        @pl.when(ahead[side])
        def _(side=side):
            whole[side].start()

    pass_on(depth - 1)
    for step in range(depth):
        for side in sides(step):

            @pl.when(present(side, step))
            def _(side=side):
                first, sent = across(side, step), relay(side, step)
                for copy in (first[2], first[3], sent[0], sent[1]):
                    copy.wait_recv()
                for copy in first + sent:
                    copy.wait_send()

    for step in range(depth - 1):
        for side in range(2):

            @pl.when(present(side, step) & ahead[side])
            def _(side=side):
                for copy in along(side, step):
                    copy.wait_send()

    for side in range(2):

        @pl.when(ahead[side])
        def _(side=side):
            whole[side].wait_send()

        @pl.when(ahead[1 - side])
        def _(side=side):
            whole[side].wait_recv()

    for copy in quarters:
        copy.wait_send()
    locals_[0].wait()
    locals_[1].wait()


def gather_weights(depth, part_a, part_b, ffn):
    rows, cols = part_a.shape
    dma = pltpu.SemaphoreType.DMA
    vmem, any_ = pl.BlockSpec(memory_space=pltpu.VMEM), pl.BlockSpec(memory_space=pl.ANY)
    full = jax.ShapeDtypeStruct((depth, 4, rows, cols), jnp.bfloat16)
    return pl.pallas_call(
        functools.partial(gather_kernel, depth),
        out_shape=(full, full, jax.ShapeDtypeStruct((depth, 4) + ffn.shape[1:], jnp.bfloat16)),
        in_specs=[vmem] * 3,
        out_specs=(any_,) * 3,
        scratch_shapes=[
            dma((2, depth, 2)),
            dma((2, depth, 2)),
            dma((2, depth, 6)),
            dma((2, depth, 6)),
            dma((3,)),
            dma((3,)),
            dma((2,)),
            dma((2,)),
            dma((3,)),
        ],
        compiler_params=pltpu.CompilerParams(collective_id=0, has_side_effects=True),
        name="gather_weights",
    )(part_a, part_b, ffn)


def plane_kernel(v_ref, out, ss, rs, local_sem):
    y, x, t = lax.axis_index("y"), lax.axis_index("x"), lax.axis_index("t")
    to_x, to_y, to_t = {"x": 1 - x}, {"y": 1 - y}, {"t": 1 - t}
    half = v_ref.shape[0] // 2
    low, high = pl.ds(0, half), pl.ds(half, half)
    greet((to_x, to_y, to_t))
    mine = pltpu.make_async_copy(v_ref, out.at[0, 0], local_sem)
    routes = (
        (v_ref, out.at[1, 0], to_x),
        (v_ref, out.at[2, 0], to_y),
        (v_ref, out.at[0, 1], to_t),
        (out.at[1, 0, low], out.at[3, 0, low], to_y),
        (out.at[2, 0, high], out.at[3, 0, high], to_x),
        (out.at[1, 0], out.at[1, 1], to_t),
        (out.at[2, 0], out.at[2, 1], to_t),
        (out.at[3, 0], out.at[3, 1], to_t),
    )
    copies = [remote(src, dst, ss.at[n], rs.at[n], where) for n, (src, dst, where) in enumerate(routes)]
    for n in range(3):
        copies[n].start()
    mine.start()
    copies[0].wait_recv()
    copies[3].start()
    copies[5].start()
    copies[1].wait_recv()
    copies[4].start()
    copies[6].start()
    copies[3].wait_recv()
    copies[4].wait_recv()
    copies[7].start()
    for n in (2, 5, 6, 7):
        copies[n].wait_recv()
    for copy in copies:
        copy.wait_send()
    mine.wait()


def plane_gather(value, number):
    rows, cols = value.shape
    dma = pltpu.SemaphoreType.DMA
    out = pl.pallas_call(
        plane_kernel,
        out_shape=jax.ShapeDtypeStruct((4, 2, rows, cols), value.dtype),
        in_specs=[pl.BlockSpec(memory_space=pltpu.VMEM)],
        out_specs=pl.BlockSpec(memory_space=pl.ANY),
        scratch_shapes=[dma((8,)), dma((8,)), dma],
        compiler_params=pltpu.CompilerParams(collective_id=number, has_side_effects=True),
        name="plane_gather",
    )(value)
    return out.reshape(8 * rows, cols)


def plane_sum_kernel(count, *refs):
    lefts, rights = refs[:count], refs[count : 2 * count]
    out, send, keep, from_t, from_x, from_y, ts, tr, xs, xr, ys, yr = refs[2 * count :]
    y, x, t = lax.axis_index("y"), lax.axis_index("x"), lax.axis_index("t")
    to_x, to_y, to_t = {"x": 1 - x}, {"y": 1 - y}, {"t": 1 - t}
    rows = out.shape[0]
    half = rows // 2
    low, high = pl.ds(0, half), pl.ds(half, half)
    greet((to_x, to_y, to_t))
    piece = rows // 2

    def product(k, side, dst):
        @pl.loop(0, rows // piece)
        def _(i):
            at = pl.ds(pl.multiple_of(i * piece, piece), piece)
            total = tail_product(lefts[0][k, side, at], rights[0][...])
            for left, right in zip(lefts[1:], rights[1:]):
                total = total + tail_product(left[k, side, at], right[...])
            dst[k, at] = total

    over = [remote(send.at[k], from_t.at[k], ts.at[k], tr.at[k], to_t) for k in range(4)]
    by_x = [
        remote(keep.at[3, low], from_x.at[0], xs.at[0], xr.at[0], to_x),
        remote(keep.at[1, low], from_x.at[1], xs.at[1], xr.at[1], to_x),
        remote(keep.at[1, high], from_x.at[2], xs.at[2], xr.at[2], to_x),
    ]
    by_y = [
        remote(keep.at[3, high], from_y.at[0], ys.at[0], yr.at[0], to_y),
        remote(keep.at[2, high], from_y.at[1], ys.at[1], yr.at[1], to_y),
        remote(keep.at[2, low], from_y.at[2], ys.at[2], yr.at[2], to_y),
    ]

    def compute(k):
        product(k, 1, send)
        over[k].start()
        product(k, 0, keep)

    def merge(k):
        over[k].wait_recv()
        keep[k] = keep[k] + from_t[k]

    compute(3)
    compute(1)
    merge(3)
    by_x[0].start()
    by_y[0].start()
    compute(2)
    merge(1)
    by_x[1].start()
    compute(0)
    merge(2)
    by_y[1].start()
    merge(0)
    by_x[0].wait_recv()
    keep[2, low] = keep[2, low] + from_x[0]
    by_y[2].start()
    by_y[0].wait_recv()
    keep[1, high] = keep[1, high] + from_y[0]
    by_x[2].start()
    by_x[1].wait_recv()
    by_y[1].wait_recv()
    keep[0, low] = keep[0, low] + from_x[1]
    keep[0, high] = keep[0, high] + from_y[1]
    by_y[2].wait_recv()
    out[low] = keep[0, low] + from_y[2]
    by_x[2].wait_recv()
    out[high] = keep[0, high] + from_x[2]
    for copy in over + by_x + by_y:
        copy.wait_send()


def plane_product_sum(lefts, rights, rows, number):
    width = rights[0].shape[0]
    lefts = [left.reshape(4, 2, rows, left.shape[1]) for left in lefts]
    dma, f32 = pltpu.SemaphoreType.DMA, jnp.float32
    vmem = pl.BlockSpec(memory_space=pltpu.VMEM)
    return pl.pallas_call(
        functools.partial(plane_sum_kernel, len(lefts)),
        out_shape=jax.ShapeDtypeStruct((rows, width), f32),
        in_specs=[vmem] * (2 * len(lefts)),
        out_specs=vmem,
        scratch_shapes=[
            pltpu.VMEM((4, rows, width), f32),
            pltpu.VMEM((4, rows, width), f32),
            pltpu.VMEM((4, rows, width), f32),
            pltpu.VMEM((3, rows // 2, width), f32),
            pltpu.VMEM((3, rows // 2, width), f32),
            dma((4,)),
            dma((4,)),
            dma((3,)),
            dma((3,)),
            dma((3,)),
            dma((3,)),
        ],
        compiler_params=pltpu.CompilerParams(collective_id=number, has_side_effects=True),
        name="plane_product_sum",
    )(*lefts, *rights)


def weight_grad_kernel(pairs, rest, at_ref, *refs):
    count, rights = len(pairs), max(pairs) + 1
    lefts, right = refs[:count], refs[count : count + rights]
    own, others = refs[count + rights : count + rights + 2]
    turned = refs[count + rights + 2 :]
    step = pl.program_id(0)

    @pl.when(step == 0)
    def _():
        for left, dst in zip(lefts, turned):
            chunk = 256

            @pl.loop(0, left.shape[0] // chunk)
            def _(i):
                rows = pl.ds(pl.multiple_of(i * chunk, chunk), chunk)
                dst[:, rows] = left[rows, :].T

    def product(n):
        return jnp.dot(turned[n][...], right[pairs[n]][...], preferred_element_type=jnp.float32)

    def spans():
        start = 0
        for left in lefts:
            yield pl.ds(start, left.shape[1])
            start += left.shape[1]

    @pl.when(step == 0)
    def _():
        for n, span in enumerate(spans()):
            own[span, :] = product(n)

    @pl.when(step > 0)
    def _():
        for n, span in enumerate(spans()):
            others[0, span, :] = product(n).astype(jnp.bfloat16)


def weight_grads(depth, iz, lefts, rights, pairs):
    tokens, width = rights[0].shape
    block = width // depth
    cols = sum(left.shape[1] for left in lefts)
    if block % 128:
        full = jnp.concatenate([lead_product(left, rights[n]) for left, n in zip(lefts, pairs)], axis=0)
        full = jnp.transpose(full.reshape(cols, depth, block), (1, 0, 2))
        own = picked(full, iz)
        return own, jnp.stack([picked(full, (iz + s) % depth).astype(jnp.bfloat16) for s in range(1, depth)])
    whole = lambda left: pl.BlockSpec(left.shape, lambda s, at: (0, 0))
    grid_spec = pltpu.PrefetchScalarGridSpec(
        num_scalar_prefetch=1,
        grid=(depth,),
        in_specs=[whole(left) for left in lefts]
        + [pl.BlockSpec((tokens, block), lambda s, at: (0, lax.rem(at[0] + s, depth)))] * len(rights),
        out_specs=(
            pl.BlockSpec((cols, block), lambda s, at: (0, 0)),
            pl.BlockSpec((1, cols, block), lambda s, at: (jnp.maximum(s - 1, 0), 0, 0)),
        ),
        scratch_shapes=[pltpu.VMEM(left.shape[::-1], jnp.bfloat16) for left in lefts],
    )
    return pl.pallas_call(
        functools.partial(weight_grad_kernel, tuple(pairs), None),
        grid_spec=grid_spec,
        out_shape=(
            jax.ShapeDtypeStruct((cols, block), jnp.float32),
            jax.ShapeDtypeStruct((depth - 1, cols, block), jnp.bfloat16),
        ),
        cost_estimate=pl.CostEstimate(
            flops=2 * tokens * cols * width,
            bytes_accessed=2 * tokens * (width * len(rights) + cols) + 2 * cols * width,
            transcendentals=0,
        ),
        name="weight_grads",
    )(iz.reshape(1), *lefts, *rights)


def owner_kernel(depth, widths, with_gains, *refs):
    own, others = refs[0], refs[1:depth]
    refs = refs[depth:]
    gains = None
    if with_gains:
        gains, refs = refs[0], refs[1:]
    outs, refs = refs[: len(widths)], refs[len(widths) :]
    if with_gains:
        gain_out, refs = refs[0], refs[1:]
    total, ss, rs, local_sem = refs[:4]
    z, y, x, t = (lax.axis_index(name) for name in ("z", "y", "x", "t"))
    to = (None, {"x": 1 - x}, {"y": 1 - y}, {"y": 1 - y, "x": 1 - x})
    me = 2 * y + x
    place = (me, 2 * y + 1 - x, 2 - 2 * y + x, 3 - me)
    rows, cols = total.shape[1], total.shape[2]
    targets = list(to[1:])
    if with_gains:
        targets += [{"t": 1 - t}] + [{"z": lax.rem(z + s, depth)} for s in range(1, depth)]
    greet(targets)
    if with_gains:
        gsum, got, got_z, gs, gr = refs[4:]
        gsum[0] = gains[...]
        stages = [
            remote(gsum.at[n], got.at[n], gs.at[n], gr.at[n], where)
            for n, where in enumerate(({"t": 1 - t}, to[1], to[2]))
        ]
        stages[0].start()
    spans = [(0, cols)] if len(widths) == 1 else [(n * widths[0], widths[0]) for n in range(len(widths))]
    for start, count in spans:
        at = pl.ds(start, count)
        part = own[at, :]
        for other in others:
            part = part + other[at, :].astype(jnp.float32)
        part = part.T
        for k in range(4):
            total[k, :, at] = part[k * rows : (k + 1) * rows]
    copies = []
    if len(widths) == 1:
        pieces = [(lambda ref: ref, outs[0].at[me])]
    else:
        pieces, start = [], 0
        for n, span in enumerate(widths):
            pieces.append(
                (
                    lambda ref, start=start, span=span: ref.at[:, pl.ds(start, span)],
                    outs[n].at[:, pl.ds(pl.multiple_of(me * span, span), span)],
                )
            )
            start += span
    for k in range(1, 4):
        for n, (cut, dst) in enumerate(pieces):
            copies.append(remote(cut(total.at[place[k]]), dst, ss.at[k - 1, n], rs.at[k - 1, n], to[k]))
    here = [pltpu.make_async_copy(cut(total.at[me]), dst, local_sem.at[n]) for n, (cut, dst) in enumerate(pieces)]
    for copy in copies + here:
        copy.start()
    if with_gains:
        for n in range(3):
            stages[n].wait_recv()
            gsum[n + 1] = gsum[n] + got[n]
            if n < 2:
                stages[n + 1].start()
        spread = [
            remote(gsum.at[3], got_z.at[z], gs.at[2 + s], gr.at[2 + s], {"z": lax.rem(z + s, depth)})
            for s in range(1, depth)
        ]
        for copy in spread:
            copy.start()
        got_z[z] = gsum[3]
        for copy in spread:
            copy.wait_recv()
        answer = got_z[0]
        for n in range(1, depth):
            answer = answer + got_z[n]
        gain_out[...] = answer
        for copy in stages + spread:
            copy.wait_send()
    for copy in copies:
        copy.wait_recv()
    for copy in copies:
        copy.wait_send()
    for copy in here:
        copy.wait()


def to_owners(depth, own, others, rows, widths, number, gains=None):
    cols = own.shape[0]
    dma, f32 = pltpu.SemaphoreType.DMA, jnp.float32
    vmem, any_ = pl.BlockSpec(memory_space=pltpu.VMEM), pl.BlockSpec(memory_space=pl.ANY)
    parts = len(widths)
    if parts == 1:
        shapes = [jax.ShapeDtypeStruct((4, rows, cols), f32)]
    else:
        shapes = [jax.ShapeDtypeStruct((rows, 4 * span), f32) for span in widths]
    out_specs = [any_] * parts
    operands = [own, *others]
    scratch = [pltpu.VMEM((4, rows, cols), f32), dma((3, parts)), dma((3, parts)), dma((parts,))]
    if gains is not None:
        operands.append(gains)
        shapes.append(jax.ShapeDtypeStruct(gains.shape, f32))
        out_specs.append(vmem)
        scratch += [
            pltpu.VMEM((4,) + gains.shape, f32),
            pltpu.VMEM((3,) + gains.shape, f32),
            pltpu.VMEM((depth,) + gains.shape, f32),
            dma((2 + depth,)),
            dma((2 + depth,)),
        ]
    return pl.pallas_call(
        functools.partial(owner_kernel, depth, tuple(widths), gains is not None),
        out_shape=tuple(shapes),
        in_specs=[vmem] * len(operands),
        out_specs=tuple(out_specs),
        scratch_shapes=scratch,
        compiler_params=pltpu.CompilerParams(collective_id=number, has_side_effects=True),
        name="to_owners",
    )(*operands)


def shifted(value, axis, size, step):
    return lax.ppermute(value, axis, [(i, (i + step) % size) for i in range(size)])


def moved(value, axis, size, step):
    pairs = [(i, i + step) for i in range(size) if 0 <= i + step < size]
    return lax.ppermute(value, axis, pairs)


def crossed(value):
    return lax.ppermute(value, ("y", "x"), [(0, 3), (1, 2), (2, 1), (3, 0)])


def flipped(value, axis):
    return lax.ppermute(value, axis, [(0, 1), (1, 0)])


def placed(blocks, indices, total):
    out = jnp.zeros((total,) + blocks[0].shape, blocks[0].dtype)
    for block, index in zip(blocks, indices):
        out = lax.dynamic_update_index_in_dim(out, block, index, 0)
    return out


def pair_rows(value, it):
    rows = value.shape[0]
    out = placed([value, flipped(value, "t")], [it, 1 - it], 2)
    return out.reshape((2 * rows,) + value.shape[1:])


def plane_blocks(value):
    return [value, flipped(value, "x"), flipped(value, "y"), crossed(value)]


def plane_exchange(blocks):
    return [blocks[0], flipped(blocks[1], "x"), flipped(blocks[2], "y"), crossed(blocks[3])]


def picked(value, index):
    return lax.dynamic_index_in_dim(value, index, 0, keepdims=False)


def make_local(depth):
    def local(
        layer_input,
        segments,
        gain_attn,
        w_query,
        w_key,
        w_value,
        w_out,
        gain_ffn,
        w_gate,
        w_up,
        w_down,
        cotangent,
    ):
        bf16 = jnp.bfloat16
        iz, it = lax.axis_index("z"), lax.axis_index("t")
        ip = lax.axis_index("y") * 2 + lax.axis_index("x")
        seqs_here, total_len = segments.shape
        own_rows, width = layer_input.shape
        wrows = w_query.shape[0]
        qcols, kcols = w_query.shape[1], w_key.shape[1]
        fcols = w_gate.shape[1]
        fq = fcols // 4
        ffn_pack = jnp.stack(
            [w_gate.reshape(wrows, 4, fq), w_up.reshape(wrows, 4, fq), w_down.T.reshape(wrows, 4, fq)],
            axis=2,
        )
        ffn_pack = jnp.transpose(ffn_pack, (1, 0, 2, 3)).reshape(4, wrows, 3 * fq)
        part_a = jnp.concatenate([w_query, w_key], axis=1)
        part_b = jnp.concatenate([w_value, w_out.T], axis=1)
        full_a, full_b, ffn_all = gather_weights(depth, part_a, part_b, ffn_pack)
        above, below = picked(ffn_all, (iz + depth - 1) % depth), picked(ffn_all, (iz + 1) % depth)
        for s in range(2, depth):
            above, below = moved(above, "z", depth, 1), moved(below, "z", depth, -1)
            for block, there, slot in (
                (above, iz >= s, (iz + depth - s) % depth),
                (below, iz + s < depth, (iz + s) % depth),
            ):
                block = jnp.where(there, block, picked(ffn_all, slot))
                ffn_all = lax.dynamic_update_index_in_dim(ffn_all, block, slot, 0)
        ffn_all = ffn_all.reshape(width, 3 * fq)
        full_gate, full_up, full_down = (
            ffn_all[:, :fq],
            ffn_all[:, fq : 2 * fq],
            ffn_all[:, 2 * fq :],
        )
        cot_late, full_a = lax.optimization_barrier((cotangent, full_a))
        full_a, full_b = full_a.reshape(width, -1), full_b.reshape(width, -1)
        full_query, full_key = full_a[:, :qcols], full_a[:, qcols:]
        full_value, full_out = full_b[:, :kcols], full_b[:, kcols:]

        x_float = layer_input.astype(jnp.float32)
        x_hat1, recip1, normed1 = rms_forward(x_float, gain_attn)
        normed_seq = pair_rows(normed1, it)
        positions = jax.vmap(doc_positions)(segments).reshape(total_len)
        cosine, sine = rotary_tables(positions, HD)
        query = plain_product(normed_seq, full_query).reshape(total_len, -1, HD)
        keys = plain_product(normed_seq, full_key).reshape(total_len, -1, HD)
        values = plain_product(normed_seq, full_value).reshape(total_len, -1, HD)
        heads_here, groups_here = query.shape[1], keys.shape[1]
        query_rot = rotate(query, cosine, sine).astype(bf16)
        key_rot = rotate(keys, cosine, sine).astype(bf16)
        value_b = values.astype(bf16)
        attended, log_totals = attend((query_rot, key_rot, value_b, segments[0]))
        mixed = tail_product(attended, full_out).reshape(2, own_rows, width)
        resid = x_float + (picked(mixed, it) + flipped(picked(mixed, 1 - it), "t"))
        x_hat2, recip2, normed2 = rms_forward(resid, gain_ffn)

        def plane_rows(value):
            blocks = jnp.stack(plane_blocks(value))
            both = jnp.stack([blocks, flipped(blocks, "t")], axis=1)
            return both.reshape(8 * value.shape[0], value.shape[1])

        normed_ffn = plane_gather(normed2, 1)
        cot_all = plane_rows(cot_late)
        gate = plain_product(normed_ffn, full_gate)
        up_part = plain_product(normed_ffn, full_up)
        sig_gate = jax.nn.sigmoid(gate)
        hidden = (gate * sig_gate * up_part).astype(bf16)
        grad_hidden = plain_product(cot_all, full_down)
        grad_gate_b = (grad_hidden * up_part * sig_gate * (1.0 + gate * (1.0 - sig_gate))).astype(bf16)
        grad_up_b = (grad_hidden * gate * sig_gate).astype(bf16)

        def plane_sum(partial, narrow):
            tiles = partial.reshape(4, 2, own_rows, width)
            mine = tiles[:, 0] + flipped(tiles[:, 1].astype(narrow), "t").astype(jnp.float32)
            back = plane_exchange([mine[0]] + [mine[k].astype(narrow) for k in range(1, 4)])
            return ((back[0] + back[1].astype(jnp.float32)) + back[2].astype(jnp.float32)) + back[3].astype(
                jnp.float32
            )

        grad_normed2 = plane_product_sum([grad_gate_b, grad_up_b], [full_gate, full_up], own_rows, 2)
        result = (resid + plane_sum(tail_product(hidden, full_down), bf16)).astype(bf16)

        def z_sums(lefts, rights, pairs, widths, number, gains=None):
            own, others = weight_grads(depth, iz, lefts, rights, pairs)
            others = [shifted(others[s - 1], "z", depth, s) for s in range(1, depth)]
            return to_owners(depth, own, others, wrows, widths, number, gains)

        sum_gate, sum_up, sum_down = z_sums(
            [grad_gate_b, grad_up_b, hidden], [normed_ffn, cot_all], [0, 0, 1], [fq] * 3, 3
        )
        grad_norm2, grad_g2 = rms_backward(grad_normed2, x_hat2, recip2, gain_ffn)
        grad_resid = cotangent.astype(jnp.float32) + grad_norm2
        grad_resid_b = grad_resid.astype(bf16)
        grad_resid_seq = pair_rows(grad_resid_b, it)
        grad_att = plain_product(grad_resid_seq, full_out).astype(bf16)
        grad_qrot, grad_krot, grad_val = attend_back(
            (query_rot, key_rot, value_b, segments[0], log_totals, grad_att)
        )
        grad_q = rotate_back(grad_qrot, cosine, sine).astype(bf16).reshape(total_len, qcols)
        grad_k = rotate_back(grad_krot, cosine, sine).astype(bf16).reshape(total_len, kcols)
        grad_v = grad_val.astype(bf16).reshape(total_len, kcols)
        dn1 = (
            tail_product(grad_q, full_query) + tail_product(grad_k, full_key) + tail_product(grad_v, full_value)
        ).reshape(2, own_rows, width)
        grad_normed1 = picked(dn1, it) + flipped(picked(dn1, 1 - it).astype(bf16), "t").astype(jnp.float32)
        grad_norm1, grad_g1 = rms_backward(grad_normed1, x_hat1, recip1, gain_attn)
        grad_rows = grad_resid + grad_norm1

        qq, kq = qcols // 4, kcols // 4
        def column_quarters(parts):
            value = jnp.concatenate([part.reshape(total_len, 4, -1) for part in parts], axis=2)
            value = jnp.transpose(value, (1, 0, 2))
            return jnp.concatenate(plane_exchange([picked(value, ip ^ k) for k in range(4)]), axis=0)

        att_all = column_quarters([attended])
        tok_all = column_quarters([grad_q, grad_k, grad_v])

        def plane_seqs(value):
            blocks = jnp.stack(plane_blocks(value))
            both = placed([blocks, flipped(blocks, "t")], [it, 1 - it], 2)
            return jnp.transpose(both, (1, 0, 2, 3)).reshape(4 * total_len, width)

        cut = qq + 2 * kq
        normed_plane = plane_seqs(normed1)
        resid_plane = plane_seqs(grad_resid_b)
        cut = qq + 2 * kq
        gains = jnp.stack([grad_g1, grad_g2]).reshape(8, -1)
        attn_sums, gains = z_sums(
            [tok_all, att_all], [normed_plane, resid_plane], [0, 1], [cut + qq], 4, gains
        )
        total_g1, total_g2 = gains.reshape(2, width)

        def columns(start, count):
            part = attn_sums[:, :, start : start + count]
            return jnp.transpose(part, (1, 0, 2)).reshape(wrows, 4 * count)

        return (
            result,
            grad_rows,
            total_g1,
            columns(0, qq),
            columns(qq, kq),
            columns(qq + kq, kq),
            columns(cut, qq).T,
            total_g2,
            sum_gate,
            sum_up,
            sum_down.T,
        )

    return local


def solution(mesh):
    ring = mesh.shape["dp"]
    fine = Mesh(mesh.devices.reshape(ring // 4, 2, 2, mesh.shape["tensor"]), ("z", "y", "x", "t"))
    dp, every = ("z", "y", "x"), ("z", "y", "x", "t")
    return jax.shard_map(
        make_local(ring // 4),
        mesh=fine,
        in_specs=(
            P(every, None),
            P(dp, None),
            P(),
            P(dp, "t"),
            P(dp, "t"),
            P(dp, "t"),
            P("t", dp),
            P(),
            P(dp, "t"),
            P(dp, "t"),
            P("t", dp),
            P(every, None),
        ),
        out_specs=(
            P(every, None),
            P(every, None),
            P(),
            P(dp, "t"),
            P(dp, "t"),
            P(dp, "t"),
            P("t", dp),
            P(),
            P(dp, "t"),
            P(dp, "t"),
            P("t", dp),
        ),
        check_vma=False,
    )
```

```python
import functools
import math

import jax
import jax.numpy as jnp
from jax import lax
from jax.experimental import pallas as pl
from jax.experimental.pallas import tpu as pltpu
from jax.sharding import Mesh
from jax.sharding import PartitionSpec as P

HD = 96


EPSILON = 1e-05
ROPE_BASE = 100000.0
MASKED = -1e30


def lead_product(left_arr, right_arr):
    return lax.dot_general(
        left_arr, right_arr, (((0,), (0,)), ((), ())), preferred_element_type=jnp.float32
    )


def tail_product(left_arr, right_arr):
    return lax.dot_general(
        left_arr, right_arr, (((1,), (1,)), ((), ())), preferred_element_type=jnp.float32
    )


def plain_product(left_arr, right_arr):
    return jnp.dot(left_arr, right_arr, preferred_element_type=jnp.float32)


def doc_positions(segment_row):
    total_len = segment_row.shape[0]
    indices = jnp.arange(total_len, dtype=jnp.int32)
    changes = jnp.concatenate([jnp.ones((1,), dtype=bool), segment_row[1:] != segment_row[:-1]])
    starts = jnp.where(changes, indices, jnp.zeros_like(indices))
    return indices - lax.cummax(starts, axis=0)


def rotary_tables(positions, head_width):
    half_width = head_width // 2
    frequency = jnp.exp(
        -math.log(ROPE_BASE) * 2.0 * jnp.arange(half_width, dtype=jnp.float32) / head_width
    )
    angles = positions.astype(jnp.float32)[:, None] * frequency[None, :]
    return (jnp.cos(angles), jnp.sin(angles))


def rms_forward(values, gain):
    recip = lax.rsqrt(jnp.mean(values * values, axis=-1, keepdims=True) + EPSILON)
    x_hat = values * recip
    return (x_hat, recip, (x_hat * gain).astype(jnp.bfloat16))


def rms_backward(grad_normed, x_hat, recip, gain):
    grad_hat = grad_normed * gain
    grad_gain = jnp.sum(grad_normed * x_hat, axis=0)
    inner = jnp.mean(grad_hat * x_hat, axis=-1, keepdims=True)
    return (recip * (grad_hat - x_hat * inner), grad_gain)


MESH = pl.DeviceIdType.MESH


def remote(src, dst, send_sem, recv_sem, where):
    return pltpu.make_async_remote_copy(
        src_ref=src, dst_ref=dst, send_sem=send_sem, recv_sem=recv_sem, device_id=where, device_id_type=MESH
    )


def greet(targets):
    barrier = pltpu.get_barrier_semaphore()
    for where in targets:
        pl.semaphore_signal(barrier, inc=1, device_id=where, device_id_type=MESH)
    pl.semaphore_wait(barrier, len(targets))


def gather_kernel(
    depth, a_ref, b_ref, gate_ref, up_ref, down_ref, fa, fb, ff, zs, zr, ps, pr, fs, fr, vs, vr, local_sem
):
    z, y, x = lax.axis_index("z"), lax.axis_index("y"), lax.axis_index("x")
    to_x, to_y, to_d = {"x": 1 - x}, {"y": 1 - y}, {"y": 1 - y, "x": 1 - x}
    me, mx, my = 2 * y + x, 2 * y + 1 - x, 2 - 2 * y + x
    md = 3 - me
    up, down = z + 1 < depth, z > 0
    ahead = (up, down)
    to_z = ({"z": z + 1}, {"z": z - 1})
    barrier = pltpu.get_barrier_semaphore()
    for where in (to_x, to_y, to_d):
        pl.semaphore_signal(barrier, inc=1, device_id=where, device_id_type=MESH)
    for side in range(2):

        @pl.when(ahead[side])
        def _(side=side):
            pl.semaphore_signal(barrier, inc=1, device_id=to_z[side], device_id_type=MESH)

    pl.semaphore_wait(barrier, 3 + jnp.minimum(z, 1) + jnp.minimum(depth - 1 - z, 1))

    def block(side, step):
        return z - step if side == 0 else z + step

    def present(side, step):
        return z >= step if side == 0 else z + step < depth

    def along(side, step):
        at = block(side, step)
        return [
            remote(
                own if step == 0 else full.at[at, me],
                full.at[at, me],
                zs.at[side, step, c],
                zr.at[side, step, c],
                to_z[side],
            )
            for c, (own, full) in enumerate(((a_ref, fa), (b_ref, fb)))
        ]

    def across(side, step):
        at = block(side, step)
        src_a = a_ref if step == 0 else fa.at[at, me]
        src_b = b_ref if step == 0 else fb.at[at, me]
        routes = ((src_a, fa, to_x), (src_b, fb, to_y), (src_b, fb, to_x), (src_a, fa, to_y))
        return [
            remote(src, full.at[at, me], ps.at[side, step, n], pr.at[side, step, n], where)
            for n, (src, full, where) in enumerate(routes)
        ]

    def relay(side, step):
        at = block(side, step)
        return [
            remote(fa.at[at, mx], fa.at[at, mx], ps.at[side, step, 4], pr.at[side, step, 4], to_y),
            remote(fb.at[at, my], fb.at[at, my], ps.at[side, step, 5], pr.at[side, step, 5], to_x),
        ]

    span = gate_ref.shape[1] // 4
    sources = (gate_ref, up_ref, down_ref)

    def quarter(n, slot):
        return sources[n].at[:, pl.ds(pl.multiple_of(slot * span, span), span)]

    def spot(n):
        return ff.at[z, me, :, pl.ds(n * span, span)]

    locals_ = [
        pltpu.make_async_copy(a_ref, fa.at[z, me], local_sem.at[0]),
        pltpu.make_async_copy(b_ref, fb.at[z, me], local_sem.at[1]),
    ] + [pltpu.make_async_copy(quarter(n, me), spot(n), local_sem.at[2 + n]) for n in range(3)]
    quarters = [
        remote(quarter(n, slot), spot(n), fs.at[k, n], fr.at[k, n], where)
        for k, (slot, where) in enumerate(((mx, to_x), (my, to_y), (md, to_d)))
        for n in range(3)
    ]
    whole = [remote(ff.at[z], ff.at[z], vs.at[n], vr.at[n], to_z[n]) for n in range(2)]
    for side in range(2):

        @pl.when(ahead[side])
        def _(side=side):
            for copy in along(side, 0):
                copy.start()

    for copy in across(0, 0) + locals_ + quarters:
        copy.start()

    def sides(step):
        return (0,) if step == 0 else (0, 1)

    def pass_on(step):
        for side in sides(step):

            @pl.when(present(side, step))
            def _(side=side):
                first, sent = across(side, step), relay(side, step)
                first[0].wait_recv()
                sent[0].start()
                first[1].wait_recv()
                sent[1].start()

    for step in range(1, depth):
        for side in (0, 1):

            @pl.when(present(side, step))
            def _(side=side):
                for copy in along(side, step - 1):
                    copy.wait_recv()
                if step < depth - 1:

                    @pl.when(ahead[side])
                    def _():
                        for copy in along(side, step):
                            copy.start()

                for copy in across(side, step):
                    copy.start()

        pass_on(step - 1)
    for copy in quarters:
        copy.wait_recv()
    for copy in locals_[2:]:
        copy.wait()
    for side in range(2):

        @pl.when(ahead[side])
        def _(side=side):
            whole[side].start()

    pass_on(depth - 1)
    for step in range(depth):
        for side in sides(step):

            @pl.when(present(side, step))
            def _(side=side):
                first, sent = across(side, step), relay(side, step)
                for copy in (first[2], first[3], sent[0], sent[1]):
                    copy.wait_recv()
                for copy in first + sent:
                    copy.wait_send()

    for step in range(depth - 1):
        for side in range(2):

            @pl.when(present(side, step) & ahead[side])
            def _(side=side):
                for copy in along(side, step):
                    copy.wait_send()

    for side in range(2):

        @pl.when(ahead[side])
        def _(side=side):
            whole[side].wait_send()

        @pl.when(ahead[1 - side])
        def _(side=side):
            whole[side].wait_recv()

    for copy in quarters:
        copy.wait_send()
    locals_[0].wait()
    locals_[1].wait()


def gather_weights(depth, part_a, part_b, gate, up_part, down):
    rows, cols = part_a.shape
    dma = pltpu.SemaphoreType.DMA
    vmem, any_ = pl.BlockSpec(memory_space=pltpu.VMEM), pl.BlockSpec(memory_space=pl.ANY)
    full = jax.ShapeDtypeStruct((depth, 4, rows, cols), jnp.bfloat16)
    return pl.pallas_call(
        functools.partial(gather_kernel, depth),
        out_shape=(full, full, jax.ShapeDtypeStruct((depth, 4, rows, 3 * gate.shape[1] // 4), jnp.bfloat16)),
        in_specs=[vmem] * 5,
        out_specs=(any_,) * 3,
        scratch_shapes=[
            dma((2, depth, 2)),
            dma((2, depth, 2)),
            dma((2, depth, 6)),
            dma((2, depth, 6)),
            dma((3, 3)),
            dma((3, 3)),
            dma((2,)),
            dma((2,)),
            dma((5,)),
        ],
        compiler_params=pltpu.CompilerParams(collective_id=0, has_side_effects=True),
        name="gather_weights",
    )(part_a, part_b, gate, up_part, down)


def greet_line(depth, z, targets):
    barrier = pltpu.get_barrier_semaphore()
    for where in targets:
        pl.semaphore_signal(barrier, inc=1, device_id=where, device_id_type=MESH)
    for ahead, where in ((z + 1 < depth, {"z": z + 1}), (z > 0, {"z": z - 1})):

        @pl.when(ahead)
        def _(where=where):
            pl.semaphore_signal(barrier, inc=1, device_id=where, device_id_type=MESH)

    pl.semaphore_wait(barrier, len(targets) + jnp.minimum(z, 1) + jnp.minimum(depth - 1 - z, 1))


def line_step(depth, z, blocks, step, ss, rs):
    sides = (
        ((z >= step - 1) & (z + 1 < depth), z >= step, z - step + 1, {"z": z + 1}),
        ((z + step - 1 < depth) & (z > 0), z + step < depth, z + step - 1, {"z": z - 1}),
    )

    def copy(n):
        at, where = sides[n][2], sides[n][3]
        return remote(blocks.at[at], blocks.at[at], ss.at[n], rs.at[n], where)

    def start():
        for n in range(2):

            @pl.when(sides[n][0])
            def _(n=n):
                copy(n).start()

    def finish():
        for n in range(2):

            @pl.when(sides[n][1])
            def _(n=n):
                copy(n).wait_recv()

            @pl.when(sides[n][0])
            def _(n=n):
                copy(n).wait_send()

    return start, finish


def plane_phases(value, out, ss, rs, local_sem, sides=(0, 1)):
    y, x, t = lax.axis_index("y"), lax.axis_index("x"), lax.axis_index("t")
    to_x, to_y, to_t = {"x": 1 - x}, {"y": 1 - y}, {"t": 1 - t}
    half = value.shape[0] // 2
    low, high = pl.ds(0, half), pl.ds(half, half)
    relative = isinstance(sides[0], int)
    near = sides[0]
    far_side = sides[1] if relative else sides[0]
    mine = pltpu.make_async_copy(value, out.at[0, near], local_sem)
    routes = (
        (value, out.at[1, near], to_x),
        (value, out.at[2, near], to_y),
        (value, out.at[0, far_side], to_t),
        (out.at[1, near, low], out.at[3, near, low], to_y),
        (out.at[2, near, high], out.at[3, near, high], to_x),
        (out.at[1, near], out.at[1, far_side], to_t),
        (out.at[2, near], out.at[2, far_side], to_t),
        (out.at[3, near], out.at[3, far_side], to_t),
    )
    copies = [remote(src, dst, ss.at[n], rs.at[n], where) for n, (src, dst, where) in enumerate(routes)]

    def begin():
        for n in range(3):
            copies[n].start()
        mine.start()

    def relay():
        copies[0].wait_recv()
        copies[3].start()
        copies[5].start()
        copies[1].wait_recv()
        copies[4].start()
        copies[6].start()

    def end():
        copies[3].wait_recv()
        copies[4].wait_recv()
        copies[7].start()
        for n in (2, 5, 6, 7):
            copies[n].wait_recv()
        for copy in copies:
            copy.wait_send()
        mine.wait()

    return begin, relay, end


def plane_kernel(depth, value, blocks_in, out, blocks, ss, rs, zs, zr, local_sem):
    z, y, x, t = (lax.axis_index(name) for name in ("z", "y", "x", "t"))
    greet_line(depth, z, ({"x": 1 - x}, {"y": 1 - y}, {"t": 1 - t}))
    begin, relay, end = plane_phases(value, out, ss, rs, local_sem)
    begin()
    start, finish = line_step(depth, z, blocks, depth - 1, zs, zr)
    start()
    relay()
    end()
    finish()


def plane_gather(depth, value, blocks, number):
    rows, cols = value.shape
    dma = pltpu.SemaphoreType.DMA
    any_ = pl.BlockSpec(memory_space=pl.ANY)
    shape = jax.ShapeDtypeStruct
    out, blocks = pl.pallas_call(
        functools.partial(plane_kernel, depth),
        out_shape=(shape((4, 2, rows, cols), value.dtype), shape(blocks.shape, blocks.dtype)),
        in_specs=[pl.BlockSpec(memory_space=pltpu.VMEM), any_],
        out_specs=(any_, any_),
        input_output_aliases={1: 1},
        scratch_shapes=[dma((8,)), dma((8,)), dma((2,)), dma((2,)), dma],
        compiler_params=pltpu.CompilerParams(collective_id=number, has_side_effects=True),
        name="plane_gather",
    )(value, blocks)
    return out.reshape(8 * rows, cols), blocks


def ffn_kernel(depth, inner, *refs):
    iz, iy, ix, it = (lax.axis_index(name) for name in ("z", "y", "x", "t"))
    tokens, cots, weights, extra = refs[:4]
    refs = refs[4:]
    out, down_out, extra_out = refs[:3]
    refs = refs[3:]
    if inner:
        own, near, far = refs[:3]
        refs = refs[3:]
    turned = refs[0]
    send, keep, from_t, from_x, from_y, down_got = refs[1:7]
    ts, tr, xs, xr, ys, yr, gs, gr, ds_, dr, local_sem = refs[7:18]
    refs = refs[18:]
    to_x, to_y, to_t = {"x": 1 - ix}, {"y": 1 - iy}, {"t": 1 - it}
    rows, cols = tokens.shape[2], weights.shape[1] // 3
    gate_w, up_w, down_w = (weights.at[:, pl.ds(n * cols, cols)] for n in range(3))
    half = rows // 2
    low, high = pl.ds(0, half), pl.ds(half, half)
    targets = [to_x, to_y, to_t]
    if inner:
        piece_ref, fs, fr = refs
        reach = depth // 2
        targets.append({"z": lax.rem(iz + reach, depth)})
    greet(targets)
    begin, relay, end = plane_phases(extra, extra_out, gs, gr, local_sem, (it, 1 - it))
    begin()

    def tile(k, side, dst, at):
        value = tokens[k, side]
        gate = plain_product(value, gate_w[...])
        up_part = plain_product(value, up_w[...])
        grad_hidden = plain_product(cots[k, side], down_w[...])
        sig_gate = jax.nn.sigmoid(gate)
        gated = gate * sig_gate
        hidden = (gated * up_part).astype(jnp.bfloat16)
        grad_gate = (grad_hidden * up_part * sig_gate * (1.0 + gate * (1.0 - sig_gate))).astype(jnp.bfloat16)
        grad_up = (grad_hidden * gated).astype(jnp.bfloat16)
        lanes = pl.ds((2 * k + side) * rows, rows)
        turned[0, :, lanes] = grad_gate.T
        turned[1, :, lanes] = grad_up.T
        turned[2, :, lanes] = hidden.T
        dst[at] = tail_product(grad_gate, gate_w[...]) + tail_product(grad_up, up_w[...])

    slot = (1, 1, 0, 0)
    over = [remote(send.at[slot[k]], from_t.at[k], ts.at[k], tr.at[k], to_t) for k in range(4)]
    by_x = [
        remote(keep.at[k, part], from_x.at[n], xs.at[n], xr.at[n], to_x)
        for n, (k, part) in enumerate(((3, low), (1, low), (1, high)))
    ]
    by_y = [
        remote(keep.at[k, part], from_y.at[n], ys.at[n], yr.at[n], to_y)
        for n, (k, part) in enumerate(((3, high), (2, high), (2, low)))
    ]

    def compute(k):
        tile(k, 1, send, slot[k])
        over[k].start()
        tile(k, 0, keep, k)

    def merge(k):
        over[k].wait_recv()
        keep[k] = keep[k] + from_t[k]

    compute(3)
    compute(1)
    merge(3)
    by_x[0].start()
    by_y[0].start()
    over[3].wait_send()
    compute(2)
    merge(1)
    by_x[1].start()
    over[1].wait_send()
    compute(0)
    merge(2)
    by_y[1].start()
    merge(0)

    def second_stage():
        by_x[0].wait_recv()
        keep[2, low] = keep[2, low] + from_x[0]
        by_y[2].start()
        by_y[0].wait_recv()
        keep[1, high] = keep[1, high] + from_y[0]
        by_x[2].start()

    if inner:
        block = tokens.shape[3] // depth
        count = 8 * rows

        def piece(step, store):
            at = lax.rem(iz + step, depth)
            lanes = pl.ds(pl.multiple_of(at * block, block), block)
            right = tokens[:, :, :, lanes].reshape(count, block)

            @pl.loop(0, 2)
            def _(n):
                store(pl.multiple_of(n * cols, cols), plain_product(turned[n], right))

            store(2 * cols, plain_product(turned[2], cots[:, :, :, lanes].reshape(count, block)))

        def to_ref(ref, index=None):
            def store(start, value):
                if index is None:
                    ref[pl.ds(start, cols)] = value.astype(ref.dtype)
                else:
                    ref[index, pl.ds(start, cols)] = value.astype(ref.dtype)

            return store

        piece(reach, to_ref(piece_ref))
        flight = remote(piece_ref, far, fs, fr, {"z": lax.rem(iz + reach, depth)})
        flight.start()
        relay()
        second_stage()

        @pl.loop(0, depth - 2)
        def _(n):
            piece(n + 1 + lax.div(n + 1, reach), to_ref(near, n))

        piece(0, to_ref(own))
    else:
        relay()
        second_stage()

    def down_copy(k):
        return remote(down_out.at[k], down_got.at[k], ds_.at[k], dr.at[k], to_t)

    def down_part(k, side):
        lanes = pl.ds(pl.multiple_of((2 * k + side) * rows, rows), rows)
        return tail_product(turned[2, :, lanes].T, down_w[...])

    @pl.loop(0, 4)
    def _(k):
        down_out[k] = down_part(k, 1).astype(jnp.bfloat16)
        down_copy(k).start()

    @pl.loop(0, 4)
    def _(k):
        part = down_part(k, 0)
        down_copy(k).wait()
        down_out[k] = (part + down_got[k].astype(jnp.float32)).astype(jnp.bfloat16)

    by_x[1].wait_recv()
    by_y[1].wait_recv()
    keep[0, low] = keep[0, low] + from_x[1]
    keep[0, high] = keep[0, high] + from_y[1]
    by_y[2].wait_recv()
    out[low] = keep[0, low] + from_y[2]
    by_x[2].wait_recv()
    out[high] = keep[0, high] + from_x[2]
    for copy in [over[2], over[0]] + by_x + by_y:
        copy.wait_send()
    end()
    if inner:
        flight.wait_recv()
        flight.wait_send()


def feed_forward(depth, tokens, cots, weights, extra, number):
    rows, model = extra.shape
    cols = weights.shape[1] // 3
    block = model // depth
    inner = block % 128 == 0
    bf16, f32, dma = jnp.bfloat16, jnp.float32, pltpu.SemaphoreType.DMA
    shape = jax.ShapeDtypeStruct
    vmem, any_ = pl.BlockSpec(memory_space=pltpu.VMEM), pl.BlockSpec(memory_space=pl.ANY)
    shapes = [shape((rows, model), f32), shape((4, rows, model), bf16), shape((4, 2, rows, model), bf16)]
    out_specs = [vmem, vmem, any_]
    turned = pltpu.VMEM((3, cols, 8 * rows), bf16)
    scratch = []
    if inner:
        shapes += [
            shape((3 * cols, block), f32),
            shape((depth - 2, 3 * cols, block), bf16),
            shape((3 * cols, block), bf16),
        ]
        out_specs += [vmem, vmem, any_]
        scratch.append(turned)
    else:
        shapes.append(shape((3, cols, 8 * rows), bf16))
        out_specs.append(vmem)
    scratch += [
        pltpu.VMEM((2, rows, model), f32),
        pltpu.VMEM((4, rows, model), f32),
        pltpu.VMEM((4, rows, model), f32),
        pltpu.VMEM((3, rows // 2, model), f32),
        pltpu.VMEM((3, rows // 2, model), f32),
        pltpu.VMEM((4, rows, model), bf16),
        dma((4,)),
        dma((4,)),
        dma((3,)),
        dma((3,)),
        dma((3,)),
        dma((3,)),
        dma((8,)),
        dma((8,)),
        dma((4,)),
        dma((4,)),
        dma,
    ]
    if inner:
        scratch += [pltpu.VMEM((3 * cols, block), bf16), dma, dma]
    return pl.pallas_call(
        functools.partial(ffn_kernel, depth, inner),
        out_shape=tuple(shapes),
        in_specs=[vmem] * 4,
        out_specs=tuple(out_specs),
        scratch_shapes=scratch,
        compiler_params=pltpu.CompilerParams(
            collective_id=number, has_side_effects=True, vmem_limit_bytes=66 * 10**6
        ),
        name="feed_forward",
    )(tokens.reshape(4, 2, rows, model), cots, weights, extra)


def weight_grad_kernel(pairs, at_ref, *refs):
    count, rights = len(pairs), max(pairs) + 1
    lefts, right = refs[:count], refs[count : count + rights]
    own, others = refs[count + rights :]
    step = pl.program_id(0)

    def product(n):
        return plain_product(lefts[n][...], right[pairs[n]][...])

    def spans():
        start = 0
        for left in lefts:
            yield pl.ds(start, left.shape[0])
            start += left.shape[0]

    @pl.when(step == 0)
    def _():
        for n, span in enumerate(spans()):
            own[span, :] = product(n)

    @pl.when(step > 0)
    def _():
        for n, span in enumerate(spans()):
            others[0, span, :] = product(n).astype(jnp.bfloat16)


def weight_grads(depth, iz, lefts, rights, pairs):
    tokens, width = rights[0].shape
    block = width // depth
    cols = sum(left.shape[0] for left in lefts)
    if block % 128:
        full = jnp.concatenate([plain_product(left, rights[n]) for left, n in zip(lefts, pairs)], axis=0)
        full = jnp.transpose(full.reshape(cols, depth, block), (1, 0, 2))
        own = picked(full, iz)
        return own, jnp.stack([picked(full, (iz + s) % depth).astype(jnp.bfloat16) for s in range(1, depth)])
    whole = lambda left: pl.BlockSpec(left.shape, lambda s, at: (0, 0))
    grid_spec = pltpu.PrefetchScalarGridSpec(
        num_scalar_prefetch=1,
        grid=(depth,),
        in_specs=[whole(left) for left in lefts]
        + [pl.BlockSpec((tokens, block), lambda s, at: (0, lax.rem(at[0] + s, depth)))] * len(rights),
        out_specs=(
            pl.BlockSpec((cols, block), lambda s, at: (0, 0)),
            pl.BlockSpec((1, cols, block), lambda s, at: (jnp.maximum(s - 1, 0), 0, 0)),
        ),
    )
    return pl.pallas_call(
        functools.partial(weight_grad_kernel, tuple(pairs)),
        grid_spec=grid_spec,
        out_shape=(
            jax.ShapeDtypeStruct((cols, block), jnp.float32),
            jax.ShapeDtypeStruct((depth - 1, cols, block), jnp.bfloat16),
        ),
        cost_estimate=pl.CostEstimate(
            flops=2 * tokens * cols * width,
            bytes_accessed=2 * tokens * (width * len(rights) + cols) + 2 * cols * width,
            transcendentals=0,
        ),
        name="weight_grads",
    )(iz.reshape(1), *lefts, *rights)


def owner_kernel(depth, widths, with_gains, *refs):
    own, others = refs[0], refs[1:depth]
    refs = refs[depth:]
    gains = None
    if with_gains:
        gains, refs = refs[0], refs[1:]
    outs, refs = refs[: len(widths)], refs[len(widths) :]
    if with_gains:
        gain_out, refs = refs[0], refs[1:]
    total, ss, rs, local_sem = refs[:4]
    z, y, x, t = (lax.axis_index(name) for name in ("z", "y", "x", "t"))
    to = (None, {"x": 1 - x}, {"y": 1 - y}, {"y": 1 - y, "x": 1 - x})
    me = 2 * y + x
    place = (me, 2 * y + 1 - x, 2 - 2 * y + x, 3 - me)
    rows, cols = total.shape[1], total.shape[2]
    targets = list(to[1:])
    if with_gains:
        targets += [{"t": 1 - t}] + [{"z": lax.rem(z + s, depth)} for s in range(1, depth)]
    greet(targets)
    if with_gains:
        gsum, got, got_z, gs, gr = refs[4:]
        gsum[0] = gains[...]
        stages = [
            remote(gsum.at[n], got.at[n], gs.at[n], gr.at[n], where)
            for n, where in enumerate(({"t": 1 - t}, to[1], to[2]))
        ]
        stages[0].start()
    spans = [(0, cols)] if len(widths) == 1 else [(n * widths[0], widths[0]) for n in range(len(widths))]
    for start, count in spans:
        at = pl.ds(start, count)
        part = own[at, :]
        for other in others:
            part = part + other[at, :].astype(jnp.float32)
        part = part.T
        for k in range(4):
            total[k, :, at] = part[k * rows : (k + 1) * rows]
    copies = []
    if len(widths) == 1:
        pieces = [(lambda ref: ref, outs[0].at[me])]
    else:
        pieces, start = [], 0
        for n, span in enumerate(widths):
            pieces.append(
                (
                    lambda ref, start=start, span=span: ref.at[:, pl.ds(start, span)],
                    outs[n].at[:, pl.ds(pl.multiple_of(me * span, span), span)],
                )
            )
            start += span
    for k in range(1, 4):
        for n, (cut, dst) in enumerate(pieces):
            copies.append(remote(cut(total.at[place[k]]), dst, ss.at[k - 1, n], rs.at[k - 1, n], to[k]))
    here = [pltpu.make_async_copy(cut(total.at[me]), dst, local_sem.at[n]) for n, (cut, dst) in enumerate(pieces)]
    for copy in copies + here:
        copy.start()
    if with_gains:
        for n in range(3):
            stages[n].wait_recv()
            gsum[n + 1] = gsum[n] + got[n]
            if n < 2:
                stages[n + 1].start()
        spread = [
            remote(gsum.at[3], got_z.at[z], gs.at[2 + s], gr.at[2 + s], {"z": lax.rem(z + s, depth)})
            for s in range(1, depth)
        ]
        for copy in spread:
            copy.start()
        got_z[z] = gsum[3]
        for copy in spread:
            copy.wait_recv()
        answer = got_z[0]
        for n in range(1, depth):
            answer = answer + got_z[n]
        gain_out[...] = answer
        for copy in stages + spread:
            copy.wait_send()
    for copy in copies:
        copy.wait_recv()
    for copy in copies:
        copy.wait_send()
    for copy in here:
        copy.wait()


def to_owners(depth, own, others, rows, widths, number, gains=None):
    cols = own.shape[0]
    dma, f32 = pltpu.SemaphoreType.DMA, jnp.float32
    vmem, any_ = pl.BlockSpec(memory_space=pltpu.VMEM), pl.BlockSpec(memory_space=pl.ANY)
    parts = len(widths)
    if parts == 1:
        shapes = [jax.ShapeDtypeStruct((4, rows, cols), f32)]
    else:
        shapes = [jax.ShapeDtypeStruct((rows, 4 * span), f32) for span in widths]
    out_specs = [any_] * parts
    operands = [own, *others]
    scratch = [pltpu.VMEM((4, rows, cols), f32), dma((3, parts)), dma((3, parts)), dma((parts,))]
    if gains is not None:
        operands.append(gains)
        shapes.append(jax.ShapeDtypeStruct(gains.shape, f32))
        out_specs.append(vmem)
        scratch += [
            pltpu.VMEM((4,) + gains.shape, f32),
            pltpu.VMEM((3,) + gains.shape, f32),
            pltpu.VMEM((depth,) + gains.shape, f32),
            dma((2 + depth,)),
            dma((2 + depth,)),
        ]
    return pl.pallas_call(
        functools.partial(owner_kernel, depth, tuple(widths), gains is not None),
        out_shape=tuple(shapes),
        in_specs=[vmem] * len(operands),
        out_specs=tuple(out_specs),
        scratch_shapes=scratch,
        compiler_params=pltpu.CompilerParams(collective_id=number, has_side_effects=True),
        name="to_owners",
    )(*operands)


def score_bias(seg_row, seg_col, bias):
    total = bias.shape[0]
    keys = lax.broadcasted_iota(jnp.int32, (total, total), 0)
    queries = lax.broadcasted_iota(jnp.int32, (total, total), 1)
    bias[...] = jnp.where((keys <= queries) & (seg_col[...] == seg_row[...]), 0.0, MASKED)


def attend_kernel(
    depth, own, other, fa, fb, cos_ref, sin_ref, seg_row, seg_col, x_ref, gain, cot, blocks_in,
    qt, kt, vt, at, lse, resid, normed, cot_all, blocks,
    raw, bias, mixed, arrived, send_sem, recv_sem, ss, rs, zs, zr, local_sem,
):
    z, y, x, t = (lax.axis_index(name) for name in ("z", "y", "x", "t"))
    heads, width, total = qt.shape
    groups = kt.shape[0]
    half = total // 2
    kcols = groups * width
    qcols = heads * width
    scale = 1.0 / math.sqrt(width)
    to_t = {"t": 1 - t}
    mine, theirs = (pl.ds(pl.multiple_of(p * half, half), half) for p in (t, 1 - t))
    greet_line(depth, z, ({"x": 1 - x}, {"y": 1 - y}, to_t))
    begin, relay, end = plane_phases(cot, cot_all, ss, rs, local_sem)
    begin()
    steps = [
        line_step(depth, z, blocks, step, zs.at[step - 2], zr.at[step - 2]) for step in range(2, depth - 1)
    ]
    if steps:
        steps[0][0]()
    score_bias(seg_row, seg_col, bias)
    for rows, lanes in ((own, mine), (other, theirs)):
        value = rows[...]
        for start in range(0, qcols + kcols, kcols):
            raw[pl.ds(start, kcols), lanes] = plain_product(value, fa[:, start : start + kcols]).T
        raw[pl.ds(qcols + kcols, kcols), lanes] = plain_product(value, fb[:, :kcols]).T
    cosine, sine = cos_ref[...], sin_ref[...]
    for n in range(heads + groups):
        first = raw[n * width : n * width + width // 2]
        second = raw[n * width + width // 2 : (n + 1) * width]
        dst, index = (qt, n) if n < heads else (kt, n - heads)
        dst[index, : width // 2] = (first * cosine - second * sine).astype(jnp.bfloat16)
        dst[index, width // 2 :] = (second * cosine + first * sine).astype(jnp.bfloat16)
    for n in range(groups):
        start = qcols + kcols + n * width
        vt[n] = raw[start : start + width].astype(jnp.bfloat16)

    @pl.loop(0, groups)
    def _(g):
        key = kt[g].T
        for r in range(heads // groups):
            h = g * (heads // groups) + r
            for j in range(2):
                seen, lanes = (j + 1) * half, pl.ds(j * half, half)
                scores = plain_product(key[:seen], qt[h, :, lanes]) * scale + bias[:seen, lanes]
                top = jnp.max(scores, axis=0, keepdims=True)
                logs = top + jnp.log(jnp.sum(jnp.exp(scores - top), axis=0, keepdims=True))
                lse[h, :, lanes] = logs
                probs = jnp.exp(scores - logs).astype(jnp.bfloat16)
                at[h, :, lanes] = plain_product(vt[g, :, :seen], probs).astype(jnp.bfloat16)

    relay()

    def project(lanes):
        rows = at[:, :, lanes].reshape(qcols, half).T
        return tail_product(rows, fb[:, kcols:])

    mixed[...] = project(theirs)
    copy = remote(mixed, arrived, send_sem, recv_sem, to_t)
    copy.start()
    part = x_ref[...].astype(jnp.float32) + project(mine)
    copy.wait_recv()
    part = part + arrived[...]
    resid[...] = part
    recip = lax.rsqrt(jnp.mean(part * part, axis=-1, keepdims=True) + EPSILON)
    normed[...] = (part * recip * gain[...]).astype(jnp.bfloat16)
    copy.wait_send()
    for n, (_, finish) in enumerate(steps):
        finish()
        if n + 1 < len(steps):
            steps[n + 1][0]()
    end()


def attention_forward(depth, own, other, fa, fb, cosine, sine, segments, x, gain, cot, blocks, heads, groups, number):
    rows, model = own.shape
    total, width = 2 * rows, 2 * cosine.shape[0]
    bf16, f32, dma = jnp.bfloat16, jnp.float32, pltpu.SemaphoreType.DMA
    shape = jax.ShapeDtypeStruct
    vmem = pl.BlockSpec(memory_space=pltpu.VMEM)
    any_ = pl.BlockSpec(memory_space=pl.ANY)
    hops = max(depth - 3, 1)
    return pl.pallas_call(
        functools.partial(attend_kernel, depth),
        out_shape=(
            shape((heads, width, total), bf16),
            shape((groups, width, total), bf16),
            shape((groups, width, total), bf16),
            shape((heads, width, total), bf16),
            shape((heads, 1, total), f32),
            shape((rows, model), f32),
            shape((rows, model), bf16),
            shape((4, 2, rows, model), bf16),
            shape(blocks.shape, bf16),
        ),
        in_specs=[vmem] * 11 + [any_],
        out_specs=(vmem,) * 7 + (any_, any_),
        input_output_aliases={11: 8},
        scratch_shapes=[
            pltpu.VMEM(((heads + 2 * groups) * width, total), f32),
            pltpu.VMEM((total, total), f32),
            pltpu.VMEM((rows, model), f32),
            pltpu.VMEM((rows, model), f32),
            dma,
            dma,
            dma((8,)),
            dma((8,)),
            dma((hops, 2)),
            dma((hops, 2)),
            dma,
        ],
        compiler_params=pltpu.CompilerParams(collective_id=number, has_side_effects=True),
        name="attention_forward",
    )(own, other, fa, fb, cosine, sine, segments, segments.reshape(total, 1), x, gain.reshape(1, model), cot, blocks)


def back_heads(fb, cos_ref, sin_ref, qt, kt, vt, lse, tok, own, other, bias, dat, dkv, turned, swap, mine, theirs):
    heads, width, total = qt.shape
    groups = kt.shape[0]
    ratio = heads // groups
    half = total // 2
    kcols = groups * width
    scale = 1.0 / math.sqrt(width)

    def incoming(rows, lanes):
        value = plain_product(rows[...], fb[:, kcols:]).astype(jnp.bfloat16)
        dat[:, :, lanes] = value.T.reshape(heads, width, half)

    incoming(own, mine)
    swap.wait_recv()
    incoming(other, theirs)
    cosine, sine = cos_ref[...], sin_ref[...]

    def unturned(grad):
        first, second = grad[: width // 2], grad[width // 2 :]
        return jnp.concatenate(
            [first * cosine + second * sine, second * cosine - first * sine], axis=0
        ).astype(jnp.bfloat16)

    @pl.loop(0, groups)
    def _(g):
        key, value = kt[g].T, vt[g].T
        dkv[...] = jnp.zeros_like(dkv)
        for r in range(ratio):
            h = g * ratio + r
            parts = []
            for j in range(2):
                seen, lanes = (j + 1) * half, pl.ds(j * half, half)
                query, grad = qt[h, :, lanes], dat[h, :, lanes]
                scores = plain_product(key[:seen], query) * scale + bias[:seen, lanes]
                probs = jnp.exp(scores - lse[h, :, lanes])
                grad_probs = plain_product(value[:seen], grad)
                delta = jnp.sum(probs * grad_probs, axis=0, keepdims=True)
                grad_scores = (probs * (grad_probs - delta) * scale).astype(jnp.bfloat16)
                parts.append(plain_product(kt[g, :, :seen], grad_scores))
                dkv[0, :, :seen] += tail_product(query, grad_scores)
                dkv[1, :, :seen] += tail_product(grad, probs.astype(jnp.bfloat16))
            grad_query = unturned(jnp.concatenate(parts, axis=1))
            turned[h] = grad_query
            tok[g, r * width : (r + 1) * width] = grad_query
        grad_key = unturned(dkv[0])
        turned[heads + g] = grad_key
        tok[g, ratio * width : (ratio + 1) * width] = grad_key
        grad_value = dkv[1].astype(jnp.bfloat16)
        turned[heads + groups + g] = grad_value
        tok[g, (ratio + 1) * width :] = grad_value


def attend_back_kernel(
    own, fa, fb, cos_ref, sin_ref, seg_row, seg_col, qt, kt, vt, lse, tok, result,
    other, bias, dat, dkv, turned, sent, arrived, send_sem, recv_sem,
):
    t = lax.axis_index("t")
    heads, width, total = qt.shape
    groups = kt.shape[0]
    half = total // 2
    kcols, qcols = groups * width, heads * width
    to_t = {"t": 1 - t}
    mine, theirs = (pl.ds(pl.multiple_of(p * half, half), half) for p in (t, 1 - t))
    greet((to_t,))
    swap = remote(own, other, send_sem.at[0], recv_sem.at[0], to_t)
    swap.start()
    score_bias(seg_row, seg_col, bias)
    back_heads(fb, cos_ref, sin_ref, qt, kt, vt, lse, tok, own, other, bias, dat, dkv, turned, swap, mine, theirs)

    def project(lanes):
        first = turned[: heads + groups, :, lanes].reshape(qcols + kcols, half).T
        second = turned[heads + groups :, :, lanes].reshape(kcols, half).T
        return tail_product(first, fa[...]) + tail_product(second, fb[:, :kcols])

    sent[...] = project(theirs).astype(jnp.bfloat16)
    back = remote(sent, arrived, send_sem.at[1], recv_sem.at[1], to_t)
    back.start()
    part = project(mine)
    back.wait_recv()
    result[...] = part + arrived[...].astype(jnp.float32)
    swap.wait_send()
    back.wait_send()


def attention_backward(own, fa, fb, cosine, sine, segments, qt, kt, vt, lse, number):
    rows, model = own.shape
    heads, width, total = qt.shape
    groups = kt.shape[0]
    bf16, f32, dma = jnp.bfloat16, jnp.float32, pltpu.SemaphoreType.DMA
    shape = jax.ShapeDtypeStruct
    vmem = pl.BlockSpec(memory_space=pltpu.VMEM)
    return pl.pallas_call(
        attend_back_kernel,
        out_shape=(
            shape((groups, (heads // groups + 2) * width, total), bf16),
            shape((rows, model), f32),
        ),
        in_specs=[vmem] * 11,
        out_specs=(vmem,) * 2,
        scratch_shapes=[
            pltpu.VMEM((rows, model), bf16),
            pltpu.VMEM((total, total), f32),
            pltpu.VMEM((heads, width, total), bf16),
            pltpu.VMEM((2, width, total), f32),
            pltpu.VMEM((heads + 2 * groups, width, total), bf16),
            pltpu.VMEM((rows, model), bf16),
            pltpu.VMEM((rows, model), bf16),
            dma((2,)),
            dma((2,)),
        ],
        compiler_params=pltpu.CompilerParams(collective_id=number, has_side_effects=True),
        name="attention_backward",
    )(own, fa, fb, cosine, sine, segments, segments.reshape(total, 1), qt, kt, vt, lse)


def finish_kernel(
    depth, dn2, resid, cot, x_ref, gain1, gain2, fa, fb, cos_ref, sin_ref, seg_row, seg_col, qt, kt, vt, lse, at,
    normed_plane, f_own, f_near, f_far, mine, result, grad_rows, gate_out, up_out, down_out, attn_out, gain_out,
    resid_plane, bias, dat, dkv, turned, tok, dh, dhb, other, tok_all, att_all, sent, arrived, a_own, a_piece, a_got,
    f_got, total_f, total_a, tile, got_tile, right_n, right_r, gsum, g_got, g_z, fs, fr, os_, or_, ks, kr, ms, mr,
    ws, wr, ps, pr, as_, ar, us, ur, vs, vr, gs, gr, swap_s, swap_r, local_sem, load_sem,
):
    z, y, x, t = (lax.axis_index(name) for name in ("z", "y", "x", "t"))
    to_t, to_z = {"t": 1 - t}, [{"z": lax.rem(z + s, depth)} for s in range(depth)]
    to = (None, {"x": 1 - x}, {"y": 1 - y}, {"y": 1 - y, "x": 1 - x})
    me = 2 * y + x
    place = (me, 2 * y + 1 - x, 2 - 2 * y + x, 3 - me)
    heads, width, total = qt.shape
    groups = kt.shape[0]
    ratio = heads // groups
    half = total // 2
    kcols, qcols = groups * width, heads * width
    cut = (ratio + 2) * width
    bf16 = jnp.bfloat16
    reach = depth // 2
    steps = [s for s in range(1, depth) if s != reach]
    mine_lanes, their_lanes = (pl.ds(pl.multiple_of(p * half, half), half) for p in (t, 1 - t))
    greet([to_t, *to[1:], *to_z[1:]])
    f_sends = [remote(f_near.at[n], f_got.at[n], fs.at[n], fr.at[n], to_z[s]) for n, s in enumerate(steps)]
    for copy in f_sends:
        copy.start()
    o_sends = [
        remote(at.at[pl.ds(ratio * place[k], ratio)], att_all.at[:, :, pl.ds(k * total, total)], os_.at[k - 1], or_.at[k - 1], to[k])
        for k in range(1, 4)
    ]
    for copy in o_sends:
        copy.start()
    own_tile = pltpu.make_async_copy(mine.at[0], tile, local_sem.at[0])
    own_tile.start()
    grad_gain = []
    rows = dh.shape[0]
    for part in (pl.ds(0, rows // 2), pl.ds(rows // 2, rows // 2)):
        h, grad = resid[part], dn2[part]
        recip = lax.rsqrt(jnp.mean(h * h, axis=-1, keepdims=True) + EPSILON)
        hat = h * recip
        grad_gain.append(jnp.sum(grad * hat, axis=0, keepdims=True))
        grad_hat = grad * gain2[...]
        inner = jnp.mean(grad_hat * hat, axis=-1, keepdims=True)
        value = cot[part].astype(jnp.float32) + recip * (grad_hat - hat * inner)
        dh[part] = value
        dhb[part] = value.astype(bf16)
    gsum[0, 1:2] = grad_gain[0] + grad_gain[1]
    swap = remote(dhb, other, swap_s.at[0], swap_r.at[0], to_t)
    swap.start()
    begin, relay, end = plane_phases(dhb, resid_plane, ps, pr, local_sem.at[1], (t, 1 - t))
    begin()
    att_all[:, :, :total] = at[pl.ds(ratio * me, ratio)]
    score_bias(seg_row, seg_col, bias)
    back_heads(fb, cos_ref, sin_ref, qt, kt, vt, lse, tok, dhb, other, bias, dat, dkv, turned, swap, mine_lanes, their_lanes)
    relay()
    k_sends = [
        remote(tok.at[place[k]], tok_all.at[:, pl.ds(k * total, total)], ks.at[k - 1], kr.at[k - 1], to[k])
        for k in range(1, 4)
    ]
    m_sends = [remote(mine.at[k], got_tile.at[k - 1], ms.at[k - 1], mr.at[k - 1], to[k]) for k in range(1, 4)]
    for copy in k_sends + m_sends:
        copy.start()
    tok_all[:, :total] = tok[me]

    def project(lanes):
        first = turned[: heads + groups, :, lanes].reshape(qcols + kcols, half).T
        second = turned[heads + groups :, :, lanes].reshape(kcols, half).T
        return tail_product(first, fa[...]) + tail_product(second, fb[:, :kcols])

    sent[...] = project(their_lanes).astype(bf16)
    back = remote(sent, arrived, swap_s.at[1], swap_r.at[1], to_t)
    back.start()
    grad_rows[...] = project(mine_lanes)
    back.wait_recv()
    grad_gain = []
    for part in (pl.ds(0, rows // 2), pl.ds(rows // 2, rows // 2)):
        h, grad = x_ref[part].astype(jnp.float32), grad_rows[part] + arrived[part].astype(jnp.float32)
        recip = lax.rsqrt(jnp.mean(h * h, axis=-1, keepdims=True) + EPSILON)
        hat = h * recip
        grad_gain.append(jnp.sum(grad * hat, axis=0, keepdims=True))
        grad_hat = grad * gain1[...]
        inner = jnp.mean(grad_hat * hat, axis=-1, keepdims=True)
        grad_rows[part] = dh[part] + recip * (grad_hat - hat * inner)
    gsum[0, 0:1] = grad_gain[0] + grad_gain[1]
    stages = [remote(gsum.at[n], g_got.at[n], gs.at[n], gr.at[n], where) for n, where in enumerate((to_t, to[1], to[2]))]
    stages[0].start()
    end()
    block = right_n.shape[4]
    order = [reach, *steps, 0]

    def loads(i):
        lanes = pl.ds(pl.multiple_of(lax.rem(z + order[i], depth) * block, 128), block)
        slot = i % 2
        return [
            pltpu.make_async_copy(src.at[:, :, :, lanes], dst.at[slot], load_sem.at[slot, n])
            for n, (src, dst) in enumerate(((normed_plane, right_n), (resid_plane, right_r)))
        ]

    for copy in loads(0):
        copy.start()
    for copy in k_sends + o_sends:
        copy.wait_recv()
    a_sends = []
    for i, s in enumerate(order):
        if i + 1 < depth:
            for copy in loads(i + 1):
                copy.start()
        for copy in loads(i):
            copy.wait()
        first = plain_product(tok_all[...], right_n[i % 2].reshape(4 * total, block))
        second = plain_product(att_all[...].reshape(ratio * width, 4 * total), right_r[i % 2].reshape(4 * total, block))
        if s:
            a_piece[s - 1, :cut] = first.astype(bf16)
            a_piece[s - 1, cut:] = second.astype(bf16)
            copy = remote(a_piece.at[s - 1], a_got.at[s - 1], as_.at[s - 1], ar.at[s - 1], to_z[s])
            copy.start()
            a_sends.append(copy)
        else:
            a_own[:cut] = first
            a_own[cut:] = second
    for n in range(3):
        stages[n].wait_recv()
        gsum[n + 1] = gsum[n] + g_got[n]
        if n < 2:
            stages[n + 1].start()
    spread = [remote(gsum.at[3], g_z.at[z], gs.at[2 + s], gr.at[2 + s], to_z[s]) for s in range(1, depth)]
    for copy in spread:
        copy.start()
    g_z[z] = gsum[3]
    for copy in f_sends:
        copy.wait_recv()
    wrows = total_f.shape[1]
    span = total_f.shape[2] // 3
    outs = (gate_out, up_out, down_out)
    u_sends, here = [], []
    for n in range(3):
        lanes = pl.ds(n * span, span)
        value = f_own[lanes] + f_far[lanes].astype(jnp.float32)
        for m in range(len(steps)):
            value = value + f_got[m, lanes].astype(jnp.float32)
        value = value.T
        for k in range(4):
            total_f[k, :, lanes] = value[k * wrows : (k + 1) * wrows]
        dst = outs[n].at[:, pl.ds(pl.multiple_of(me * span, span), span)]
        for k in range(1, 4):
            u_sends.append(remote(total_f.at[place[k], :, lanes], dst, us.at[k - 1, n], ur.at[k - 1, n], to[k]))
            u_sends[-1].start()
        here.append(pltpu.make_async_copy(total_f.at[me, :, lanes], dst, local_sem.at[2 + n]))
        here[-1].start()
    for copy in a_sends:
        copy.wait_recv()
    value = a_own[...]
    for m in range(depth - 1):
        value = value + a_got[m].astype(jnp.float32)
    value = value.T
    for k in range(4):
        total_a[k] = value[k * wrows : (k + 1) * wrows]
    v_sends = [remote(total_a.at[place[k]], attn_out.at[me], vs.at[k - 1], vr.at[k - 1], to[k]) for k in range(1, 4)]
    here.append(pltpu.make_async_copy(total_a.at[me], attn_out.at[me], local_sem.at[5]))
    for copy in v_sends + here[-1:]:
        copy.start()
    for copy in spread:
        copy.wait_recv()
    answer = g_z[0]
    for n in range(1, depth):
        answer = answer + g_z[n]
    gain_out[...] = answer
    own_tile.wait()
    for copy in m_sends:
        copy.wait_recv()
    value = resid[...] + tile[...].astype(jnp.float32)
    for k in range(3):
        value = value + got_tile[k].astype(jnp.float32)
    result[...] = value.astype(bf16)
    for copy in u_sends + v_sends:
        copy.wait_recv()
    for copy in f_sends + o_sends + k_sends + m_sends + a_sends + stages + spread + u_sends + v_sends + [swap, back]:
        copy.wait_send()
    for copy in here:
        copy.wait()


def finish(
    depth, dn2, resid, cot, x, gain1, gain2, fa, fb, cosine, sine, segments, qt, kt, vt, lse, at, normed_plane, f_own,
    f_near, f_far, mine, wrows, number,
):
    rows, model = dn2.shape
    heads, width, total = qt.shape
    groups = kt.shape[0]
    ratio = heads // groups
    fcols, block = f_own.shape
    acols = (2 * ratio + 2) * width
    bf16, f32, dma = jnp.bfloat16, jnp.float32, pltpu.SemaphoreType.DMA
    shape = jax.ShapeDtypeStruct
    vmem, any_ = pl.BlockSpec(memory_space=pltpu.VMEM), pl.BlockSpec(memory_space=pl.ANY)
    grads = shape((wrows, 4 * fcols // 3), f32)
    scratch = [
        ((total, total), f32),
        ((heads, width, total), bf16),
        ((2, width, total), f32),
        ((heads + 2 * groups, width, total), bf16),
        ((groups, (ratio + 2) * width, total), bf16),
        ((rows, model), f32),
        ((rows, model), bf16),
        ((rows, model), bf16),
        (((ratio + 2) * width, 4 * total), bf16),
        ((ratio, width, 4 * total), bf16),
        ((rows, model), bf16),
        ((rows, model), bf16),
        ((acols, block), f32),
        ((depth - 1, acols, block), bf16),
        ((depth - 1, acols, block), bf16),
        ((depth - 2, fcols, block), bf16),
        ((4, wrows, fcols), f32),
        ((4, wrows, acols), f32),
        ((rows, model), bf16),
        ((3, rows, model), bf16),
        ((2, 4, 2, rows, block), bf16),
        ((2, 4, 2, rows, block), bf16),
        ((4, 2, model), f32),
        ((3, 2, model), f32),
        ((depth, 2, model), f32),
    ]
    sems = [
        (depth - 2,), (depth - 2,), (3,), (3,), (3,), (3,), (3,), (3,), (3,), (3,), (8,), (8,), (depth - 1,),
        (depth - 1,), (3, 3), (3, 3), (3,), (3,), (2 + depth,), (2 + depth,), (2,), (2,), (6,), (2, 2),
    ]
    return pl.pallas_call(
        functools.partial(finish_kernel, depth),
        out_shape=(
            shape((rows, model), bf16),
            shape((rows, model), f32),
            grads,
            grads,
            grads,
            shape((4, wrows, acols), f32),
            shape((2, model), f32),
            shape((4, 2, rows, model), bf16),
        ),
        in_specs=[vmem] * 17 + [any_, vmem, any_, vmem, any_],
        out_specs=(vmem, vmem, any_, any_, any_, any_, vmem, any_),
        scratch_shapes=[pltpu.VMEM(*item) for item in scratch] + [dma(item) for item in sems],
        compiler_params=pltpu.CompilerParams(
            collective_id=number, has_side_effects=True, vmem_limit_bytes=66 * 10**6
        ),
        name="finish",
    )(
        dn2, resid, cot, x, gain1.reshape(1, model), gain2.reshape(1, model), fa, fb, cosine, sine, segments,
        segments.reshape(total, 1), qt, kt, vt, lse, at, normed_plane, f_own, f_near, f_far, mine,
    )


def shifted(value, axis, size, step):
    return lax.ppermute(value, axis, [(i, (i + step) % size) for i in range(size)])


def moved(value, axis, size, step):
    pairs = [(i, i + step) for i in range(size) if 0 <= i + step < size]
    return lax.ppermute(value, axis, pairs)


def crossed(value):
    return lax.ppermute(value, ("y", "x"), [(0, 3), (1, 2), (2, 1), (3, 0)])


def flipped(value, axis):
    return lax.ppermute(value, axis, [(0, 1), (1, 0)])


def placed(blocks, indices, total):
    out = jnp.zeros((total,) + blocks[0].shape, blocks[0].dtype)
    for block, index in zip(blocks, indices):
        out = lax.dynamic_update_index_in_dim(out, block, index, 0)
    return out


def pair_rows(value, it):
    rows = value.shape[0]
    out = placed([value, flipped(value, "t")], [it, 1 - it], 2)
    return out.reshape((2 * rows,) + value.shape[1:])


def plane_blocks(value):
    return [value, flipped(value, "x"), flipped(value, "y"), crossed(value)]


def plane_exchange(blocks):
    return [blocks[0], flipped(blocks[1], "x"), flipped(blocks[2], "y"), crossed(blocks[3])]


def picked(value, index):
    return lax.dynamic_index_in_dim(value, index, 0, keepdims=False)


def make_local(depth):
    def local(
        layer_input,
        segments,
        gain_attn,
        w_query,
        w_key,
        w_value,
        w_out,
        gain_ffn,
        w_gate,
        w_up,
        w_down,
        cotangent,
    ):
        bf16 = jnp.bfloat16
        iz, it = lax.axis_index("z"), lax.axis_index("t")
        ip = lax.axis_index("y") * 2 + lax.axis_index("x")
        seqs_here, total_len = segments.shape
        own_rows, width = layer_input.shape
        wrows = w_query.shape[0]
        qcols, kcols = w_query.shape[1], w_key.shape[1]
        fcols = w_gate.shape[1]
        fq = fcols // 4
        part_a = jnp.concatenate([w_query, w_key], axis=1)
        part_b = jnp.concatenate([w_value, w_out.T], axis=1)
        full_a, full_b, ffn_all = gather_weights(
            depth, part_a, part_b, w_gate, w_up, w_down.T
        )
        full_a, full_b = full_a.reshape(width, -1), full_b.reshape(width, -1)
        heads_here, groups_here = qcols // HD, kcols // HD
        x_float = layer_input.astype(jnp.float32)
        x_hat1, recip1, normed1 = rms_forward(x_float, gain_attn)
        positions = doc_positions(segments[0])
        cosine, sine = (table.T for table in rotary_tables(positions, HD))
        query_t, key_t, value_t, attended_t, log_totals, resid, normed2, cot_all, ffn_all = attention_forward(
            depth,
            normed1,
            flipped(normed1, "t"),
            full_a,
            full_b,
            cosine,
            sine,
            segments,
            layer_input,
            gain_ffn,
            cotangent,
            ffn_all,
            heads_here,
            groups_here,
            5,
        )

        normed_ffn, ffn_all = plane_gather(depth, normed2, ffn_all, 1)
        ffn_all = ffn_all.reshape(width, 3 * fq)
        grad_normed2, down_sums, normed_plane, *ffn_grads = feed_forward(
            depth, normed_ffn, cot_all, ffn_all, normed1, 2
        )
        qq, kq = qcols // 4, kcols // 4
        cut = qq + 2 * kq

        def columns(sums, start, count):
            part = sums[:, :, start : start + count]
            return jnp.transpose(part, (1, 0, 2)).reshape(wrows, 4 * count)

        def attention_sums(sums):
            return [columns(sums, *item) for item in ((0, qq), (qq, kq), (qq + kq, kq), (cut, qq))]

        if len(ffn_grads) == 3:
            own, near, far = ffn_grads
            result, grad_rows, sum_gate, sum_up, sum_down, attn_sums, gains, _ = finish(
                depth, grad_normed2, resid, cotangent, layer_input, gain_attn, gain_ffn, full_a, full_b, cosine, sine,
                segments, query_t, key_t, value_t, log_totals, attended_t, normed_plane, own, near, far, down_sums,
                wrows, 7,
            )
            sum_query, sum_key, sum_value, sum_out = attention_sums(attn_sums)
            return (
                result, grad_rows, gains[0], sum_query, sum_key, sum_value, sum_out.T, gains[1], sum_gate, sum_up,
                sum_down.T,
            )

        normed_plane = normed_plane.reshape(4 * total_len, width)
        down_sums = down_sums.astype(jnp.float32)
        result = down_sums[0]
        for block in plane_exchange([down_sums[k].astype(bf16) for k in range(4)])[1:]:
            result = result + block.astype(jnp.float32)
        result = (resid + result).astype(bf16)
        turned = ffn_grads[0]
        ffn_own, near = weight_grads(
            depth,
            iz,
            [turned[0], turned[1], turned[2]],
            [normed_ffn, cot_all.reshape(8 * own_rows, width)],
            [0, 0, 1],
        )
        ffn_others = [shifted(near[s - 1], "z", depth, s) for s in range(1, depth)]
        x_hat2, recip2, _ = rms_forward(resid, gain_ffn)

        grad_norm2, grad_g2 = rms_backward(grad_normed2, x_hat2, recip2, gain_ffn)
        grad_resid = cotangent.astype(jnp.float32) + grad_norm2
        grad_resid_b = grad_resid.astype(bf16)
        tok, grad_normed1 = attention_backward(
            grad_resid_b, full_a, full_b, cosine, sine, segments, query_t, key_t, value_t, log_totals, 6
        )
        grad_norm1, grad_g1 = rms_backward(grad_normed1, x_hat1, recip1, gain_attn)
        grad_rows = grad_resid + grad_norm1

        def column_quarters(value):
            return jnp.concatenate(plane_exchange([picked(value, ip ^ k) for k in range(4)]), axis=1)

        att_all = column_quarters(attended_t.reshape(4, qq, total_len))
        tok_all = column_quarters(tok)

        blocks = jnp.stack(plane_blocks(grad_resid_b))
        both = placed([blocks, flipped(blocks, "t")], [it, 1 - it], 2)
        resid_plane = jnp.transpose(both, (1, 0, 2, 3)).reshape(4 * total_len, width)
        gains = jnp.stack([grad_g1, grad_g2]).reshape(8, -1)
        own, near = weight_grads(depth, iz, [tok_all, att_all], [normed_plane, resid_plane], [0, 1])
        others = [shifted(near[s - 1], "z", depth, s) for s in range(1, depth)]
        ffn_own, own = lax.optimization_barrier((ffn_own, own))
        sum_gate, sum_up, sum_down = to_owners(depth, ffn_own, ffn_others, wrows, [fq] * 3, 3)
        attn_sums, gains = to_owners(depth, own, others, wrows, [cut + qq], 4, gains)
        total_g1, total_g2 = gains.reshape(2, width)

        sum_query, sum_key, sum_value, sum_out = attention_sums(attn_sums)
        return (
            result,
            grad_rows,
            total_g1,
            sum_query,
            sum_key,
            sum_value,
            sum_out.T,
            total_g2,
            sum_gate,
            sum_up,
            sum_down.T,
        )

    return local


def solution(mesh):
    ring = mesh.shape["dp"]
    fine = Mesh(mesh.devices.reshape(ring // 4, 2, 2, mesh.shape["tensor"]), ("z", "y", "x", "t"))
    dp, every = ("z", "y", "x"), ("z", "y", "x", "t")
    return jax.shard_map(
        make_local(ring // 4),
        mesh=fine,
        in_specs=(
            P(every, None),
            P(dp, None),
            P(),
            P(dp, "t"),
            P(dp, "t"),
            P(dp, "t"),
            P("t", dp),
            P(),
            P(dp, "t"),
            P(dp, "t"),
            P("t", dp),
            P(every, None),
        ),
        out_specs=(
            P(every, None),
            P(every, None),
            P(),
            P(dp, "t"),
            P(dp, "t"),
            P(dp, "t"),
            P("t", dp),
            P(),
            P(dp, "t"),
            P(dp, "t"),
            P("t", dp),
        ),
        check_vma=False,
    )
```

```python
import functools
import math

import jax
import jax.numpy as jnp
from jax import lax
from jax.experimental import pallas as pl
from jax.experimental.pallas import tpu as pltpu
from jax.sharding import Mesh
from jax.sharding import PartitionSpec as P

HD = 96


EPSILON = 1e-05
ROPE_BASE = 100000.0
MASKED = -1e30


def lead_product(left_arr, right_arr):
    return lax.dot_general(
        left_arr, right_arr, (((0,), (0,)), ((), ())), preferred_element_type=jnp.float32
    )


def tail_product(left_arr, right_arr):
    return lax.dot_general(
        left_arr, right_arr, (((1,), (1,)), ((), ())), preferred_element_type=jnp.float32
    )


def plain_product(left_arr, right_arr):
    return jnp.dot(left_arr, right_arr, preferred_element_type=jnp.float32)


def doc_positions(segment_row):
    total_len = segment_row.shape[0]
    indices = jnp.arange(total_len, dtype=jnp.int32)
    changes = jnp.concatenate([jnp.ones((1,), dtype=bool), segment_row[1:] != segment_row[:-1]])
    starts = jnp.where(changes, indices, jnp.zeros_like(indices))
    return indices - lax.cummax(starts, axis=0)


def rotary_tables(positions, head_width):
    half_width = head_width // 2
    frequency = jnp.exp(
        -math.log(ROPE_BASE) * 2.0 * jnp.arange(half_width, dtype=jnp.float32) / head_width
    )
    angles = positions.astype(jnp.float32)[:, None] * frequency[None, :]
    return (jnp.cos(angles), jnp.sin(angles))


def rms_forward(values, gain):
    recip = lax.rsqrt(jnp.mean(values * values, axis=-1, keepdims=True) + EPSILON)
    x_hat = values * recip
    return (x_hat, recip, (x_hat * gain).astype(jnp.bfloat16))


def rms_backward(grad_normed, x_hat, recip, gain):
    grad_hat = grad_normed * gain
    grad_gain = jnp.sum(grad_normed * x_hat, axis=0)
    inner = jnp.mean(grad_hat * x_hat, axis=-1, keepdims=True)
    return (recip * (grad_hat - x_hat * inner), grad_gain)


MESH = pl.DeviceIdType.MESH


def remote(src, dst, send_sem, recv_sem, where):
    return pltpu.make_async_remote_copy(
        src_ref=src, dst_ref=dst, send_sem=send_sem, recv_sem=recv_sem, device_id=where, device_id_type=MESH
    )


def greet(targets):
    barrier = pltpu.get_barrier_semaphore()
    for where in targets:
        pl.semaphore_signal(barrier, inc=1, device_id=where, device_id_type=MESH)
    pl.semaphore_wait(barrier, len(targets))


def gather_kernel(
    depth, a_ref, b_ref, gate_ref, up_ref, down_ref, fa, fb, ff, zs, zr, ps, pr, fs, fr, vs, vr, local_sem
):
    z, y, x = lax.axis_index("z"), lax.axis_index("y"), lax.axis_index("x")
    to_x, to_y, to_d = {"x": 1 - x}, {"y": 1 - y}, {"y": 1 - y, "x": 1 - x}
    me, mx, my = 2 * y + x, 2 * y + 1 - x, 2 - 2 * y + x
    md = 3 - me
    up, down = z + 1 < depth, z > 0
    ahead = (up, down)
    to_z = ({"z": z + 1}, {"z": z - 1})
    barrier = pltpu.get_barrier_semaphore()
    for where in (to_x, to_y, to_d):
        pl.semaphore_signal(barrier, inc=1, device_id=where, device_id_type=MESH)
    for side in range(2):

        @pl.when(ahead[side])
        def _(side=side):
            pl.semaphore_signal(barrier, inc=1, device_id=to_z[side], device_id_type=MESH)

    pl.semaphore_wait(barrier, 3 + jnp.minimum(z, 1) + jnp.minimum(depth - 1 - z, 1))

    def block(side, step):
        return z - step if side == 0 else z + step

    def present(side, step):
        return z >= step if side == 0 else z + step < depth

    def along(side, step):
        at = block(side, step)
        return [
            remote(
                own if step == 0 else full.at[at, me],
                full.at[at, me],
                zs.at[side, step, c],
                zr.at[side, step, c],
                to_z[side],
            )
            for c, (own, full) in enumerate(((a_ref, fa), (b_ref, fb)))
        ]

    def across(side, step):
        at = block(side, step)
        src_a = a_ref if step == 0 else fa.at[at, me]
        src_b = b_ref if step == 0 else fb.at[at, me]
        routes = ((src_a, fa, to_x), (src_b, fb, to_y), (src_b, fb, to_x), (src_a, fa, to_y))
        return [
            remote(src, full.at[at, me], ps.at[side, step, n], pr.at[side, step, n], where)
            for n, (src, full, where) in enumerate(routes)
        ]

    def relay(side, step):
        at = block(side, step)
        return [
            remote(fa.at[at, mx], fa.at[at, mx], ps.at[side, step, 4], pr.at[side, step, 4], to_y),
            remote(fb.at[at, my], fb.at[at, my], ps.at[side, step, 5], pr.at[side, step, 5], to_x),
        ]

    span = gate_ref.shape[1] // 4
    sources = (gate_ref, up_ref, down_ref)

    def quarter(n, slot):
        return sources[n].at[:, pl.ds(pl.multiple_of(slot * span, span), span)]

    def spot(n):
        return ff.at[z, me, :, pl.ds(n * span, span)]

    locals_ = [
        pltpu.make_async_copy(a_ref, fa.at[z, me], local_sem.at[0]),
        pltpu.make_async_copy(b_ref, fb.at[z, me], local_sem.at[1]),
    ] + [pltpu.make_async_copy(quarter(n, me), spot(n), local_sem.at[2 + n]) for n in range(3)]
    quarters = [
        remote(quarter(n, slot), spot(n), fs.at[k, n], fr.at[k, n], where)
        for k, (slot, where) in enumerate(((mx, to_x), (my, to_y), (md, to_d)))
        for n in range(3)
    ]
    whole = [remote(ff.at[z], ff.at[z], vs.at[n], vr.at[n], to_z[n]) for n in range(2)]
    for side in range(2):

        @pl.when(ahead[side])
        def _(side=side):
            for copy in along(side, 0):
                copy.start()

    for copy in across(0, 0) + locals_ + quarters:
        copy.start()

    def sides(step):
        return (0,) if step == 0 else (0, 1)

    def pass_on(step):
        for side in sides(step):

            @pl.when(present(side, step))
            def _(side=side):
                first, sent = across(side, step), relay(side, step)
                first[0].wait_recv()
                sent[0].start()
                first[1].wait_recv()
                sent[1].start()

    for step in range(1, depth):
        for side in (0, 1):

            @pl.when(present(side, step))
            def _(side=side):
                for copy in along(side, step - 1):
                    copy.wait_recv()
                if step < depth - 1:

                    @pl.when(ahead[side])
                    def _():
                        for copy in along(side, step):
                            copy.start()

                for copy in across(side, step):
                    copy.start()

        pass_on(step - 1)
    for copy in quarters:
        copy.wait_recv()
    for copy in locals_[2:]:
        copy.wait()
    for side in range(2):

        @pl.when(ahead[side])
        def _(side=side):
            whole[side].start()

    pass_on(depth - 1)
    for step in range(depth):
        for side in sides(step):

            @pl.when(present(side, step))
            def _(side=side):
                first, sent = across(side, step), relay(side, step)
                for copy in (first[2], first[3], sent[0], sent[1]):
                    copy.wait_recv()
                for copy in first + sent:
                    copy.wait_send()

    for step in range(depth - 1):
        for side in range(2):

            @pl.when(present(side, step) & ahead[side])
            def _(side=side):
                for copy in along(side, step):
                    copy.wait_send()

    for side in range(2):

        @pl.when(ahead[side])
        def _(side=side):
            whole[side].wait_send()

        @pl.when(ahead[1 - side])
        def _(side=side):
            whole[side].wait_recv()

    for copy in quarters:
        copy.wait_send()
    locals_[0].wait()
    locals_[1].wait()


def gather_weights(depth, part_a, part_b, gate, up_part, down):
    rows, cols = part_a.shape
    dma = pltpu.SemaphoreType.DMA
    vmem, any_ = pl.BlockSpec(memory_space=pltpu.VMEM), pl.BlockSpec(memory_space=pl.ANY)
    full = jax.ShapeDtypeStruct((depth, 4, rows, cols), jnp.bfloat16)
    return pl.pallas_call(
        functools.partial(gather_kernel, depth),
        out_shape=(full, full, jax.ShapeDtypeStruct((depth, 4, rows, 3 * gate.shape[1] // 4), jnp.bfloat16)),
        in_specs=[vmem] * 5,
        out_specs=(any_,) * 3,
        scratch_shapes=[
            dma((2, depth, 2)),
            dma((2, depth, 2)),
            dma((2, depth, 6)),
            dma((2, depth, 6)),
            dma((3, 3)),
            dma((3, 3)),
            dma((2,)),
            dma((2,)),
            dma((5,)),
        ],
        compiler_params=pltpu.CompilerParams(collective_id=0, has_side_effects=True),
        name="gather_weights",
    )(part_a, part_b, gate, up_part, down)


def greet_line(depth, z, targets):
    barrier = pltpu.get_barrier_semaphore()
    for where in targets:
        pl.semaphore_signal(barrier, inc=1, device_id=where, device_id_type=MESH)
    for ahead, where in ((z + 1 < depth, {"z": z + 1}), (z > 0, {"z": z - 1})):

        @pl.when(ahead)
        def _(where=where):
            pl.semaphore_signal(barrier, inc=1, device_id=where, device_id_type=MESH)

    pl.semaphore_wait(barrier, len(targets) + jnp.minimum(z, 1) + jnp.minimum(depth - 1 - z, 1))


def line_step(depth, z, blocks, step, ss, rs):
    sides = (
        ((z >= step - 1) & (z + 1 < depth), z >= step, z - step + 1, {"z": z + 1}),
        ((z + step - 1 < depth) & (z > 0), z + step < depth, z + step - 1, {"z": z - 1}),
    )

    def copy(n):
        at, where = sides[n][2], sides[n][3]
        return remote(blocks.at[at], blocks.at[at], ss.at[n], rs.at[n], where)

    def start():
        for n in range(2):

            @pl.when(sides[n][0])
            def _(n=n):
                copy(n).start()

    def finish():
        for n in range(2):

            @pl.when(sides[n][1])
            def _(n=n):
                copy(n).wait_recv()

            @pl.when(sides[n][0])
            def _(n=n):
                copy(n).wait_send()

    return start, finish


def plane_phases(value, out, ss, rs, local_sem, sides=(0, 1)):
    y, x, t = lax.axis_index("y"), lax.axis_index("x"), lax.axis_index("t")
    to_x, to_y, to_t = {"x": 1 - x}, {"y": 1 - y}, {"t": 1 - t}
    half = value.shape[0] // 2
    low, high = pl.ds(0, half), pl.ds(half, half)
    relative = isinstance(sides[0], int)
    near = sides[0]
    far_side = sides[1] if relative else sides[0]
    mine = pltpu.make_async_copy(value, out.at[0, near], local_sem)
    routes = (
        (value, out.at[1, near], to_x),
        (value, out.at[2, near], to_y),
        (value, out.at[0, far_side], to_t),
        (out.at[1, near, low], out.at[3, near, low], to_y),
        (out.at[2, near, high], out.at[3, near, high], to_x),
        (out.at[1, near], out.at[1, far_side], to_t),
        (out.at[2, near], out.at[2, far_side], to_t),
        (out.at[3, near], out.at[3, far_side], to_t),
    )
    copies = [remote(src, dst, ss.at[n], rs.at[n], where) for n, (src, dst, where) in enumerate(routes)]

    def begin():
        for n in range(3):
            copies[n].start()
        mine.start()

    def relay():
        copies[0].wait_recv()
        copies[3].start()
        copies[5].start()
        copies[1].wait_recv()
        copies[4].start()
        copies[6].start()

    def end():
        copies[3].wait_recv()
        copies[4].wait_recv()
        copies[7].start()
        for n in (2, 5, 6, 7):
            copies[n].wait_recv()
        for copy in copies:
            copy.wait_send()
        mine.wait()

    return begin, relay, end


def ffn_kernel(depth, inner, *refs):
    iz, iy, ix, it = (lax.axis_index(name) for name in ("z", "y", "x", "t"))
    value, cots_in, extra = refs[:3]
    refs = refs[4:]
    out, down_out, extra_out, blocks = refs[:4]
    refs = refs[4:]
    if inner:
        own, near, far = refs[:3]
        refs = refs[3:]
    tokens, turned = refs[:2]
    refs = refs[1:]
    cots, weights4, send, keep, from_t, from_x, from_y, down_got = refs[1:9]
    ts, tr, xs, xr, ys, yr, gs, gr, ds_, dr, bs, br, zs, zr, local_sem = refs[9:24]
    refs = refs[24:]
    to_x, to_y, to_t = {"x": 1 - ix}, {"y": 1 - iy}, {"t": 1 - it}
    rows, cols = tokens.shape[2], weights4.shape[3] // 3
    model = tokens.shape[3]

    class Part:
        def __init__(self, n):
            self.lanes = pl.ds(n * cols, cols)

        def __getitem__(self, _):
            return weights4[:, :, :, self.lanes].reshape(model, cols)

    gate_w, up_w, down_w = Part(0), Part(1), Part(2)
    half = rows // 2
    low, high = pl.ds(0, half), pl.ds(half, half)
    targets = [to_x, to_y, to_t]
    if inner:
        piece_ref, fs, fr = refs
        reach = depth // 2
        targets.append({"z": lax.rem(iz + reach, depth)})
    greet_line(depth, iz, targets)
    first_begin, first_relay, first_end = plane_phases(value, tokens, bs, br, local_sem.at[0])
    first_begin()
    start, finish_line = line_step(depth, iz, blocks, depth - 1, zs, zr)
    start()
    load_cots = pltpu.make_async_copy(cots_in, cots, local_sem.at[2])
    load_cots.start()
    first_relay()
    begin, relay, end = plane_phases(extra, extra_out, gs, gr, local_sem.at[1], (it, 1 - it))
    begin()
    first_end()
    finish_line()
    load_weights = pltpu.make_async_copy(blocks, weights4, local_sem.at[3])
    load_weights.start()
    load_cots.wait()
    load_weights.wait()

    def tile(k, side, dst, at):
        value = tokens[k, side]
        gate = plain_product(value, gate_w[...])
        up_part = plain_product(value, up_w[...])
        grad_hidden = plain_product(cots[k, side], down_w[...])
        sig_gate = jax.nn.sigmoid(gate)
        gated = gate * sig_gate
        hidden = (gated * up_part).astype(jnp.bfloat16)
        grad_gate = (grad_hidden * up_part * sig_gate * (1.0 + gate * (1.0 - sig_gate))).astype(jnp.bfloat16)
        grad_up = (grad_hidden * gated).astype(jnp.bfloat16)
        lanes = pl.ds((2 * k + side) * rows, rows)
        turned[0, :, lanes] = grad_gate.T
        turned[1, :, lanes] = grad_up.T
        turned[2, :, lanes] = hidden.T
        dst[at] = tail_product(grad_gate, gate_w[...]) + tail_product(grad_up, up_w[...])

    slot = (1, 1, 0, 0)
    over = [remote(send.at[slot[k]], from_t.at[k], ts.at[k], tr.at[k], to_t) for k in range(4)]
    by_x = [
        remote(keep.at[k, part], from_x.at[n], xs.at[n], xr.at[n], to_x)
        for n, (k, part) in enumerate(((3, low), (1, low), (1, high)))
    ]
    by_y = [
        remote(keep.at[k, part], from_y.at[n], ys.at[n], yr.at[n], to_y)
        for n, (k, part) in enumerate(((3, high), (2, high), (2, low)))
    ]

    def compute(k):
        tile(k, 1, send, slot[k])
        over[k].start()
        tile(k, 0, keep, k)

    def merge(k):
        over[k].wait_recv()
        keep[k] = keep[k] + from_t[k]

    compute(3)
    compute(1)
    merge(3)
    by_x[0].start()
    by_y[0].start()
    over[3].wait_send()
    compute(2)
    merge(1)
    by_x[1].start()
    over[1].wait_send()
    compute(0)
    merge(2)
    by_y[1].start()
    merge(0)

    def second_stage():
        by_x[0].wait_recv()
        keep[2, low] = keep[2, low] + from_x[0]
        by_y[2].start()
        by_y[0].wait_recv()
        keep[1, high] = keep[1, high] + from_y[0]
        by_x[2].start()

    if inner:
        block = tokens.shape[3] // depth
        count = 8 * rows

        def piece(step, store):
            at = lax.rem(iz + step, depth)
            lanes = pl.ds(pl.multiple_of(at * block, block), block)
            right = tokens[:, :, :, lanes].reshape(count, block)

            @pl.loop(0, 2)
            def _(n):
                store(pl.multiple_of(n * cols, cols), plain_product(turned[n], right))

            store(2 * cols, plain_product(turned[2], cots[:, :, :, lanes].reshape(count, block)))

        def to_ref(ref, index=None):
            def store(start, value):
                if index is None:
                    ref[pl.ds(start, cols)] = value.astype(ref.dtype)
                else:
                    ref[index, pl.ds(start, cols)] = value.astype(ref.dtype)

            return store

        piece(reach, to_ref(piece_ref))
        flight = remote(piece_ref, far, fs, fr, {"z": lax.rem(iz + reach, depth)})
        flight.start()
        relay()
        second_stage()

        @pl.loop(0, depth - 2)
        def _(n):
            piece(n + 1 + lax.div(n + 1, reach), to_ref(near, n))

        piece(0, to_ref(own))
    else:
        relay()
        second_stage()

    def down_copy(k):
        return remote(down_out.at[k], down_got.at[k], ds_.at[k], dr.at[k], to_t)

    def down_part(k, side):
        lanes = pl.ds(pl.multiple_of((2 * k + side) * rows, rows), rows)
        return tail_product(turned[2, :, lanes].T, down_w[...])

    @pl.loop(0, 4)
    def _(k):
        down_out[k] = down_part(k, 1).astype(jnp.bfloat16)
        down_copy(k).start()

    @pl.loop(0, 4)
    def _(k):
        part = down_part(k, 0)
        down_copy(k).wait()
        down_out[k] = (part + down_got[k].astype(jnp.float32)).astype(jnp.bfloat16)

    by_x[1].wait_recv()
    by_y[1].wait_recv()
    keep[0, low] = keep[0, low] + from_x[1]
    keep[0, high] = keep[0, high] + from_y[1]
    by_y[2].wait_recv()
    out[low] = keep[0, low] + from_y[2]
    by_x[2].wait_recv()
    out[high] = keep[0, high] + from_x[2]
    for copy in [over[2], over[0]] + by_x + by_y:
        copy.wait_send()
    end()
    if inner:
        flight.wait_recv()
        flight.wait_send()


def feed_forward(depth, value, cots, blocks, extra, number):
    rows, model = extra.shape
    cols = blocks.shape[3] // 3
    block = model // depth
    inner = block % 128 == 0
    bf16, f32, dma = jnp.bfloat16, jnp.float32, pltpu.SemaphoreType.DMA
    shape = jax.ShapeDtypeStruct
    vmem, any_ = pl.BlockSpec(memory_space=pltpu.VMEM), pl.BlockSpec(memory_space=pl.ANY)
    plane = (4, 2, rows, model)
    shapes = [shape((rows, model), f32), shape((4, rows, model), bf16), shape(plane, bf16), shape(blocks.shape, bf16)]
    out_specs = [vmem, vmem, any_, any_]
    scratch = []
    if inner:
        shapes += [
            shape((3 * cols, block), f32),
            shape((depth - 2, 3 * cols, block), bf16),
            shape((3 * cols, block), bf16),
        ]
        out_specs += [vmem, vmem, any_]
        scratch += [pltpu.VMEM(plane, bf16), pltpu.VMEM((3, cols, 8 * rows), bf16)]
    else:
        shapes += [shape(plane, bf16), shape((3, cols, 8 * rows), bf16)]
        out_specs += [vmem, vmem]
    scratch += [
        pltpu.VMEM(plane, bf16),
        pltpu.VMEM(blocks.shape, bf16),
        pltpu.VMEM((2, rows, model), f32),
        pltpu.VMEM((4, rows, model), f32),
        pltpu.VMEM((4, rows, model), f32),
        pltpu.VMEM((3, rows // 2, model), f32),
        pltpu.VMEM((3, rows // 2, model), f32),
        pltpu.VMEM((4, rows, model), bf16),
    ] + [dma(item) for item in ((4,), (4,), (3,), (3,), (3,), (3,), (8,), (8,), (4,), (4,), (8,), (8,), (2,), (2,), (4,))]
    if inner:
        scratch += [pltpu.VMEM((3 * cols, block), bf16), dma, dma]
    return pl.pallas_call(
        functools.partial(ffn_kernel, depth, inner),
        out_shape=tuple(shapes),
        in_specs=[vmem, any_, vmem, any_],
        out_specs=tuple(out_specs),
        input_output_aliases={3: 3},
        scratch_shapes=scratch,
        compiler_params=pltpu.CompilerParams(
            collective_id=number, has_side_effects=True, vmem_limit_bytes=66 * 10**6
        ),
        name="feed_forward",
    )(value, cots, extra, blocks)


def weight_grad_kernel(pairs, at_ref, *refs):
    count, rights = len(pairs), max(pairs) + 1
    lefts, right = refs[:count], refs[count : count + rights]
    own, others = refs[count + rights :]
    step = pl.program_id(0)

    def product(n):
        return plain_product(lefts[n][...], right[pairs[n]][...])

    def spans():
        start = 0
        for left in lefts:
            yield pl.ds(start, left.shape[0])
            start += left.shape[0]

    @pl.when(step == 0)
    def _():
        for n, span in enumerate(spans()):
            own[span, :] = product(n)

    @pl.when(step > 0)
    def _():
        for n, span in enumerate(spans()):
            others[0, span, :] = product(n).astype(jnp.bfloat16)


def weight_grads(depth, iz, lefts, rights, pairs):
    tokens, width = rights[0].shape
    block = width // depth
    cols = sum(left.shape[0] for left in lefts)
    if block % 128:
        full = jnp.concatenate([plain_product(left, rights[n]) for left, n in zip(lefts, pairs)], axis=0)
        full = jnp.transpose(full.reshape(cols, depth, block), (1, 0, 2))
        own = picked(full, iz)
        return own, jnp.stack([picked(full, (iz + s) % depth).astype(jnp.bfloat16) for s in range(1, depth)])
    whole = lambda left: pl.BlockSpec(left.shape, lambda s, at: (0, 0))
    grid_spec = pltpu.PrefetchScalarGridSpec(
        num_scalar_prefetch=1,
        grid=(depth,),
        in_specs=[whole(left) for left in lefts]
        + [pl.BlockSpec((tokens, block), lambda s, at: (0, lax.rem(at[0] + s, depth)))] * len(rights),
        out_specs=(
            pl.BlockSpec((cols, block), lambda s, at: (0, 0)),
            pl.BlockSpec((1, cols, block), lambda s, at: (jnp.maximum(s - 1, 0), 0, 0)),
        ),
    )
    return pl.pallas_call(
        functools.partial(weight_grad_kernel, tuple(pairs)),
        grid_spec=grid_spec,
        out_shape=(
            jax.ShapeDtypeStruct((cols, block), jnp.float32),
            jax.ShapeDtypeStruct((depth - 1, cols, block), jnp.bfloat16),
        ),
        cost_estimate=pl.CostEstimate(
            flops=2 * tokens * cols * width,
            bytes_accessed=2 * tokens * (width * len(rights) + cols) + 2 * cols * width,
            transcendentals=0,
        ),
        name="weight_grads",
    )(iz.reshape(1), *lefts, *rights)


def owner_kernel(depth, widths, with_gains, *refs):
    own, others = refs[0], refs[1:depth]
    refs = refs[depth:]
    gains = None
    if with_gains:
        gains, refs = refs[0], refs[1:]
    outs, refs = refs[: len(widths)], refs[len(widths) :]
    if with_gains:
        gain_out, refs = refs[0], refs[1:]
    total, ss, rs, local_sem = refs[:4]
    z, y, x, t = (lax.axis_index(name) for name in ("z", "y", "x", "t"))
    to = (None, {"x": 1 - x}, {"y": 1 - y}, {"y": 1 - y, "x": 1 - x})
    me = 2 * y + x
    place = (me, 2 * y + 1 - x, 2 - 2 * y + x, 3 - me)
    rows, cols = total.shape[1], total.shape[2]
    targets = list(to[1:])
    if with_gains:
        targets += [{"t": 1 - t}] + [{"z": lax.rem(z + s, depth)} for s in range(1, depth)]
    greet(targets)
    if with_gains:
        gsum, got, got_z, gs, gr = refs[4:]
        gsum[0] = gains[...]
        stages = [
            remote(gsum.at[n], got.at[n], gs.at[n], gr.at[n], where)
            for n, where in enumerate(({"t": 1 - t}, to[1], to[2]))
        ]
        stages[0].start()
    spans = [(0, cols)] if len(widths) == 1 else [(n * widths[0], widths[0]) for n in range(len(widths))]
    for start, count in spans:
        at = pl.ds(start, count)
        part = own[at, :]
        for other in others:
            part = part + other[at, :].astype(jnp.float32)
        part = part.T
        for k in range(4):
            total[k, :, at] = part[k * rows : (k + 1) * rows]
    copies = []
    if len(widths) == 1:
        pieces = [(lambda ref: ref, outs[0].at[me])]
    else:
        pieces, start = [], 0
        for n, span in enumerate(widths):
            pieces.append(
                (
                    lambda ref, start=start, span=span: ref.at[:, pl.ds(start, span)],
                    outs[n].at[:, pl.ds(pl.multiple_of(me * span, span), span)],
                )
            )
            start += span
    for k in range(1, 4):
        for n, (cut, dst) in enumerate(pieces):
            copies.append(remote(cut(total.at[place[k]]), dst, ss.at[k - 1, n], rs.at[k - 1, n], to[k]))
    here = [pltpu.make_async_copy(cut(total.at[me]), dst, local_sem.at[n]) for n, (cut, dst) in enumerate(pieces)]
    for copy in copies + here:
        copy.start()
    if with_gains:
        for n in range(3):
            stages[n].wait_recv()
            gsum[n + 1] = gsum[n] + got[n]
            if n < 2:
                stages[n + 1].start()
        spread = [
            remote(gsum.at[3], got_z.at[z], gs.at[2 + s], gr.at[2 + s], {"z": lax.rem(z + s, depth)})
            for s in range(1, depth)
        ]
        for copy in spread:
            copy.start()
        got_z[z] = gsum[3]
        for copy in spread:
            copy.wait_recv()
        answer = got_z[0]
        for n in range(1, depth):
            answer = answer + got_z[n]
        gain_out[...] = answer
        for copy in stages + spread:
            copy.wait_send()
    for copy in copies:
        copy.wait_recv()
    for copy in copies:
        copy.wait_send()
    for copy in here:
        copy.wait()


def to_owners(depth, own, others, rows, widths, number, gains=None):
    cols = own.shape[0]
    dma, f32 = pltpu.SemaphoreType.DMA, jnp.float32
    vmem, any_ = pl.BlockSpec(memory_space=pltpu.VMEM), pl.BlockSpec(memory_space=pl.ANY)
    parts = len(widths)
    if parts == 1:
        shapes = [jax.ShapeDtypeStruct((4, rows, cols), f32)]
    else:
        shapes = [jax.ShapeDtypeStruct((rows, 4 * span), f32) for span in widths]
    out_specs = [any_] * parts
    operands = [own, *others]
    scratch = [pltpu.VMEM((4, rows, cols), f32), dma((3, parts)), dma((3, parts)), dma((parts,))]
    if gains is not None:
        operands.append(gains)
        shapes.append(jax.ShapeDtypeStruct(gains.shape, f32))
        out_specs.append(vmem)
        scratch += [
            pltpu.VMEM((4,) + gains.shape, f32),
            pltpu.VMEM((3,) + gains.shape, f32),
            pltpu.VMEM((depth,) + gains.shape, f32),
            dma((2 + depth,)),
            dma((2 + depth,)),
        ]
    return pl.pallas_call(
        functools.partial(owner_kernel, depth, tuple(widths), gains is not None),
        out_shape=tuple(shapes),
        in_specs=[vmem] * len(operands),
        out_specs=tuple(out_specs),
        scratch_shapes=scratch,
        compiler_params=pltpu.CompilerParams(collective_id=number, has_side_effects=True),
        name="to_owners",
    )(*operands)


def score_bias(seg_row, seg_col, bias):
    total = bias.shape[0]
    keys = lax.broadcasted_iota(jnp.int32, (total, total), 0)
    queries = lax.broadcasted_iota(jnp.int32, (total, total), 1)
    bias[...] = jnp.where((keys <= queries) & (seg_col[...] == seg_row[...]), 0.0, MASKED)


def attend_kernel(
    depth, own, other, fa, fb, cos_ref, sin_ref, seg_row, seg_col, x_ref, gain, cot, blocks_in,
    qt, kt, vt, att_all, lse, resid, normed, cot_all, blocks,
    at, raw, bias, mixed, arrived, send_sem, recv_sem, ss, rs, zs, zr, os_, or_, local_sem,
):
    z, y, x, t = (lax.axis_index(name) for name in ("z", "y", "x", "t"))
    heads, width, total = qt.shape
    groups = kt.shape[0]
    half = total // 2
    kcols = groups * width
    qcols = heads * width
    scale = 1.0 / math.sqrt(width)
    to_t = {"t": 1 - t}
    mine, theirs = (pl.ds(pl.multiple_of(p * half, half), half) for p in (t, 1 - t))
    to = (None, {"x": 1 - x}, {"y": 1 - y}, {"y": 1 - y, "x": 1 - x})
    me = 2 * y + x
    place = (me, 2 * y + 1 - x, 2 - 2 * y + x, 3 - me)
    ratio = heads // groups
    greet_line(depth, z, (*to[1:], to_t))
    begin, relay, end = plane_phases(cot, cot_all, ss, rs, local_sem)
    begin()
    steps = [
        line_step(depth, z, blocks, step, zs.at[step - 2], zr.at[step - 2]) for step in range(2, depth - 1)
    ]
    if steps:
        steps[0][0]()
    score_bias(seg_row, seg_col, bias)
    for rows, lanes in ((own, mine), (other, theirs)):
        value = rows[...]
        for start in range(0, qcols + kcols, kcols):
            raw[pl.ds(start, kcols), lanes] = plain_product(value, fa[:, start : start + kcols]).T
        raw[pl.ds(qcols + kcols, kcols), lanes] = plain_product(value, fb[:, :kcols]).T
    cosine, sine = cos_ref[...], sin_ref[...]
    for n in range(heads + groups):
        first = raw[n * width : n * width + width // 2]
        second = raw[n * width + width // 2 : (n + 1) * width]
        dst, index = (qt, n) if n < heads else (kt, n - heads)
        dst[index, : width // 2] = (first * cosine - second * sine).astype(jnp.bfloat16)
        dst[index, width // 2 :] = (second * cosine + first * sine).astype(jnp.bfloat16)
    for n in range(groups):
        start = qcols + kcols + n * width
        vt[n] = raw[start : start + width].astype(jnp.bfloat16)

    @pl.loop(0, groups)
    def _(g):
        key = kt[g].T
        for r in range(heads // groups):
            h = g * (heads // groups) + r
            for j in range(2):
                seen, lanes = (j + 1) * half, pl.ds(j * half, half)
                scores = plain_product(key[:seen], qt[h, :, lanes]) * scale + bias[:seen, lanes]
                top = jnp.max(scores, axis=0, keepdims=True)
                logs = top + jnp.log(jnp.sum(jnp.exp(scores - top), axis=0, keepdims=True))
                lse[h, :, lanes] = logs
                probs = jnp.exp(scores - logs).astype(jnp.bfloat16)
                at[h, :, lanes] = plain_product(vt[g, :, :seen], probs).astype(jnp.bfloat16)

    relay()
    o_sends = [
        remote(
            at.at[pl.ds(ratio * place[k], ratio)],
            att_all.at[:, :, pl.ds(k * total, total)],
            os_.at[k - 1],
            or_.at[k - 1],
            to[k],
        )
        for k in range(1, 4)
    ]
    for copy in o_sends:
        copy.start()
    att_all[:, :, :total] = at[pl.ds(ratio * me, ratio)]

    def project(lanes):
        rows = at[:, :, lanes].reshape(qcols, half).T
        return tail_product(rows, fb[:, kcols:])

    mixed[...] = project(theirs)
    copy = remote(mixed, arrived, send_sem, recv_sem, to_t)
    copy.start()
    part = x_ref[...].astype(jnp.float32) + project(mine)
    copy.wait_recv()
    part = part + arrived[...]
    resid[...] = part
    recip = lax.rsqrt(jnp.mean(part * part, axis=-1, keepdims=True) + EPSILON)
    normed[...] = (part * recip * gain[...]).astype(jnp.bfloat16)
    copy.wait_send()
    for n, (_, finish) in enumerate(steps):
        finish()
        if n + 1 < len(steps):
            steps[n + 1][0]()
    end()
    for copy in o_sends:
        copy.wait_recv()
        copy.wait_send()


def attention_forward(depth, own, other, fa, fb, cosine, sine, segments, x, gain, cot, blocks, heads, groups, number):
    rows, model = own.shape
    total, width = 2 * rows, 2 * cosine.shape[0]
    bf16, f32, dma = jnp.bfloat16, jnp.float32, pltpu.SemaphoreType.DMA
    shape = jax.ShapeDtypeStruct
    vmem = pl.BlockSpec(memory_space=pltpu.VMEM)
    any_ = pl.BlockSpec(memory_space=pl.ANY)
    hops = max(depth - 3, 1)
    return pl.pallas_call(
        functools.partial(attend_kernel, depth),
        out_shape=(
            shape((heads, width, total), bf16),
            shape((groups, width, total), bf16),
            shape((groups, width, total), bf16),
            shape((heads // groups, width, 4 * total), bf16),
            shape((heads, 1, total), f32),
            shape((rows, model), f32),
            shape((rows, model), bf16),
            shape((4, 2, rows, model), bf16),
            shape(blocks.shape, bf16),
        ),
        in_specs=[vmem] * 11 + [any_],
        out_specs=(vmem,) * 7 + (any_, any_),
        input_output_aliases={11: 8},
        scratch_shapes=[
            pltpu.VMEM((heads, width, total), bf16),
            pltpu.VMEM(((heads + 2 * groups) * width, total), f32),
            pltpu.VMEM((total, total), f32),
            pltpu.VMEM((rows, model), f32),
            pltpu.VMEM((rows, model), f32),
            dma,
            dma,
            dma((8,)),
            dma((8,)),
            dma((hops, 2)),
            dma((hops, 2)),
            dma((3,)),
            dma((3,)),
            dma,
        ],
        compiler_params=pltpu.CompilerParams(collective_id=number, has_side_effects=True),
        name="attention_forward",
    )(own, other, fa, fb, cosine, sine, segments, segments.reshape(total, 1), x, gain.reshape(1, model), cot, blocks)


def back_heads(fb, cos_ref, sin_ref, qt, kt, vt, lse, tok, own, other, bias, dat, dkv, turned, swap, mine, theirs):
    heads, width, total = qt.shape
    groups = kt.shape[0]
    ratio = heads // groups
    half = total // 2
    kcols = groups * width
    scale = 1.0 / math.sqrt(width)

    def incoming(rows, lanes):
        value = plain_product(rows[...], fb[:, kcols:]).astype(jnp.bfloat16)
        dat[:, :, lanes] = value.T.reshape(heads, width, half)

    incoming(own, mine)
    swap.wait_recv()
    incoming(other, theirs)
    cosine, sine = cos_ref[...], sin_ref[...]

    def unturned(grad):
        first, second = grad[: width // 2], grad[width // 2 :]
        return jnp.concatenate(
            [first * cosine + second * sine, second * cosine - first * sine], axis=0
        ).astype(jnp.bfloat16)

    @pl.loop(0, groups)
    def _(g):
        key, value = kt[g].T, vt[g].T
        dkv[...] = jnp.zeros_like(dkv)
        for r in range(ratio):
            h = g * ratio + r
            parts = []
            for j in range(2):
                seen, lanes = (j + 1) * half, pl.ds(j * half, half)
                query, grad = qt[h, :, lanes], dat[h, :, lanes]
                scores = plain_product(key[:seen], query) * scale + bias[:seen, lanes]
                probs = jnp.exp(scores - lse[h, :, lanes])
                grad_probs = plain_product(value[:seen], grad)
                delta = jnp.sum(probs * grad_probs, axis=0, keepdims=True)
                grad_scores = (probs * (grad_probs - delta) * scale).astype(jnp.bfloat16)
                parts.append(plain_product(kt[g, :, :seen], grad_scores))
                dkv[0, :, :seen] += tail_product(query, grad_scores)
                dkv[1, :, :seen] += tail_product(grad, probs.astype(jnp.bfloat16))
            grad_query = unturned(jnp.concatenate(parts, axis=1))
            turned[h] = grad_query
            tok[g, r * width : (r + 1) * width] = grad_query
        grad_key = unturned(dkv[0])
        turned[heads + g] = grad_key
        tok[g, ratio * width : (ratio + 1) * width] = grad_key
        grad_value = dkv[1].astype(jnp.bfloat16)
        turned[heads + groups + g] = grad_value
        tok[g, (ratio + 1) * width :] = grad_value


def attend_back_kernel(
    own, fa, fb, cos_ref, sin_ref, seg_row, seg_col, qt, kt, vt, lse, tok, result,
    other, bias, dat, dkv, turned, sent, arrived, send_sem, recv_sem,
):
    t = lax.axis_index("t")
    heads, width, total = qt.shape
    groups = kt.shape[0]
    half = total // 2
    kcols, qcols = groups * width, heads * width
    to_t = {"t": 1 - t}
    mine, theirs = (pl.ds(pl.multiple_of(p * half, half), half) for p in (t, 1 - t))
    greet((to_t,))
    swap = remote(own, other, send_sem.at[0], recv_sem.at[0], to_t)
    swap.start()
    score_bias(seg_row, seg_col, bias)
    back_heads(fb, cos_ref, sin_ref, qt, kt, vt, lse, tok, own, other, bias, dat, dkv, turned, swap, mine, theirs)

    def project(lanes):
        first = turned[: heads + groups, :, lanes].reshape(qcols + kcols, half).T
        second = turned[heads + groups :, :, lanes].reshape(kcols, half).T
        return tail_product(first, fa[...]) + tail_product(second, fb[:, :kcols])

    sent[...] = project(theirs).astype(jnp.bfloat16)
    back = remote(sent, arrived, send_sem.at[1], recv_sem.at[1], to_t)
    back.start()
    part = project(mine)
    back.wait_recv()
    result[...] = part + arrived[...].astype(jnp.float32)
    swap.wait_send()
    back.wait_send()


def attention_backward(own, fa, fb, cosine, sine, segments, qt, kt, vt, lse, number):
    rows, model = own.shape
    heads, width, total = qt.shape
    groups = kt.shape[0]
    bf16, f32, dma = jnp.bfloat16, jnp.float32, pltpu.SemaphoreType.DMA
    shape = jax.ShapeDtypeStruct
    vmem = pl.BlockSpec(memory_space=pltpu.VMEM)
    return pl.pallas_call(
        attend_back_kernel,
        out_shape=(
            shape((groups, (heads // groups + 2) * width, total), bf16),
            shape((rows, model), f32),
        ),
        in_specs=[vmem] * 11,
        out_specs=(vmem,) * 2,
        scratch_shapes=[
            pltpu.VMEM((rows, model), bf16),
            pltpu.VMEM((total, total), f32),
            pltpu.VMEM((heads, width, total), bf16),
            pltpu.VMEM((2, width, total), f32),
            pltpu.VMEM((heads + 2 * groups, width, total), bf16),
            pltpu.VMEM((rows, model), bf16),
            pltpu.VMEM((rows, model), bf16),
            dma((2,)),
            dma((2,)),
        ],
        compiler_params=pltpu.CompilerParams(collective_id=number, has_side_effects=True),
        name="attention_backward",
    )(own, fa, fb, cosine, sine, segments, segments.reshape(total, 1), qt, kt, vt, lse)


def finish_kernel(
    depth, dn2, resid, cot, x_ref, gain1, gain2, fa, fb, cos_ref, sin_ref, seg_row, seg_col, qt, kt, vt, lse,
    att_all, normed_plane, f_own, f_near, f_far, mine, result, grad_rows, gate_out, up_out, down_out, query_out,
    key_out, value_out, out_out, gain_out, resid_plane, bias, dat, dkv, turned, tok, dh, dhb, other, tok_all, sent, arrived, a_own, a_piece, a_got,
    f_got, total_f, total_a, landed, got_x, got_y, passed, right_n, right_r, gsum, g_got, g_z, fs, fr, ks, kr, ms, mr,
    ws, wr, ps, pr, as_, ar, us, ur, vs, vr, gs, gr, swap_s, swap_r, local_sem, load_sem,
):
    z, y, x, t = (lax.axis_index(name) for name in ("z", "y", "x", "t"))
    to_t, to_z = {"t": 1 - t}, [{"z": lax.rem(z + s, depth)} for s in range(depth)]
    to = (None, {"x": 1 - x}, {"y": 1 - y}, {"y": 1 - y, "x": 1 - x})
    me = 2 * y + x
    place = (me, 2 * y + 1 - x, 2 - 2 * y + x, 3 - me)
    heads, width, total = qt.shape
    groups = kt.shape[0]
    ratio = heads // groups
    half = total // 2
    kcols, qcols = groups * width, heads * width
    cut = (ratio + 2) * width
    bf16 = jnp.bfloat16
    reach = depth // 2
    steps = [s for s in range(1, depth) if s != reach]
    mine_lanes, their_lanes = (pl.ds(pl.multiple_of(p * half, half), half) for p in (t, 1 - t))
    greet([to_t, *to[1:], *to_z[1:]])
    f_sends = [remote(f_near.at[n], f_got.at[n], fs.at[n], fr.at[n], to_z[s]) for n, s in enumerate(steps)]
    for copy in f_sends:
        copy.start()
    grad_gain = []
    rows = dh.shape[0]
    for part in (pl.ds(0, rows // 2), pl.ds(rows // 2, rows // 2)):
        h, grad = resid[part], dn2[part]
        recip = lax.rsqrt(jnp.mean(h * h, axis=-1, keepdims=True) + EPSILON)
        hat = h * recip
        grad_gain.append(jnp.sum(grad * hat, axis=0, keepdims=True))
        grad_hat = grad * gain2[...]
        inner = jnp.mean(grad_hat * hat, axis=-1, keepdims=True)
        value = cot[part].astype(jnp.float32) + recip * (grad_hat - hat * inner)
        dh[part] = value
        dhb[part] = value.astype(bf16)
    gsum[0, 1:2] = grad_gain[0] + grad_gain[1]
    swap = remote(dhb, other, swap_s.at[0], swap_r.at[0], to_t)
    swap.start()
    begin, relay, end = plane_phases(dhb, resid_plane, ps, pr, local_sem.at[3], (t, 1 - t))
    begin()
    score_bias(seg_row, seg_col, bias)
    back_heads(fb, cos_ref, sin_ref, qt, kt, vt, lse, tok, dhb, other, bias, dat, dkv, turned, swap, mine_lanes, their_lanes)
    relay()
    k_sends = [
        remote(tok.at[place[k]], tok_all.at[:, pl.ds(k * total, total)], ks.at[k - 1], kr.at[k - 1], to[k])
        for k in range(1, 4)
    ]
    low, high = pl.ds(0, rows // 2), pl.ds(rows // 2, rows // 2)
    by_x = [
        remote(src, got_x.at[n], ms.at[n], mr.at[n], to[1])
        for n, src in enumerate((mine.at[3, low], mine.at[1, low], passed.at[0]))
    ]
    by_y = [
        remote(src, got_y.at[n], ws.at[n], wr.at[n], to[2])
        for n, src in enumerate((mine.at[3, high], mine.at[2, high], passed.at[1]))
    ]
    for copy in k_sends + by_x[:2] + by_y[:2]:
        copy.start()
    tok_all[:, :total] = tok[me]

    def project(lanes):
        first = turned[: heads + groups, :, lanes].reshape(qcols + kcols, half).T
        second = turned[heads + groups :, :, lanes].reshape(kcols, half).T
        return tail_product(first, fa[...]) + tail_product(second, fb[:, :kcols])

    sent[...] = project(their_lanes).astype(bf16)
    back = remote(sent, arrived, swap_s.at[1], swap_r.at[1], to_t)
    back.start()
    grad_rows[...] = project(mine_lanes)
    back.wait_recv()
    grad_gain = []
    for part in (pl.ds(0, rows // 2), pl.ds(rows // 2, rows // 2)):
        h, grad = x_ref[part].astype(jnp.float32), grad_rows[part] + arrived[part].astype(jnp.float32)
        recip = lax.rsqrt(jnp.mean(h * h, axis=-1, keepdims=True) + EPSILON)
        hat = h * recip
        grad_gain.append(jnp.sum(grad * hat, axis=0, keepdims=True))
        grad_hat = grad * gain1[...]
        inner = jnp.mean(grad_hat * hat, axis=-1, keepdims=True)
        grad_rows[part] = dh[part] + recip * (grad_hat - hat * inner)
    gsum[0, 0:1] = grad_gain[0] + grad_gain[1]
    stages = [remote(gsum.at[n], g_got.at[n], gs.at[n], gr.at[n], where) for n, where in enumerate((to_t, to[1], to[2]))]
    stages[0].start()
    end()
    block = right_n.shape[4]
    order = [reach, *steps, 0]

    def loads(i):
        lanes = pl.ds(pl.multiple_of(lax.rem(z + order[i], depth) * block, 128), block)
        slot = i % 2
        return [
            pltpu.make_async_copy(src.at[:, :, :, lanes], dst.at[slot], load_sem.at[slot, n])
            for n, (src, dst) in enumerate(((normed_plane, right_n), (resid_plane, right_r)))
        ]

    for copy in loads(0):
        copy.start()
    for copy in k_sends:
        copy.wait_recv()
    a_sends = []
    for i, s in enumerate(order):
        if i + 1 < depth:
            for copy in loads(i + 1):
                copy.start()
        for copy in loads(i):
            copy.wait()
        first = plain_product(tok_all[...], right_n[i % 2].reshape(4 * total, block))
        second = plain_product(att_all[...].reshape(ratio * width, 4 * total), right_r[i % 2].reshape(4 * total, block))
        if s:
            a_piece[s - 1, :cut] = first.astype(bf16)
            a_piece[s - 1, cut:] = second.astype(bf16)
            copy = remote(a_piece.at[s - 1], a_got.at[s - 1], as_.at[s - 1], ar.at[s - 1], to_z[s])
            copy.start()
            a_sends.append(copy)
        else:
            a_own[:cut] = first
            a_own[cut:] = second
    for n in range(3):
        stages[n].wait_recv()
        gsum[n + 1] = gsum[n] + g_got[n]
        if n < 2:
            stages[n + 1].start()
    spread = [remote(gsum.at[3], g_z.at[z], gs.at[2 + s], gr.at[2 + s], to_z[s]) for s in range(1, depth)]
    for copy in spread:
        copy.start()
    g_z[z] = gsum[3]
    by_y[0].wait_recv()
    passed[0] = (mine[1, high].astype(jnp.float32) + got_y[0].astype(jnp.float32)).astype(bf16)
    by_x[2].start()
    by_x[0].wait_recv()
    passed[1] = (mine[2, low].astype(jnp.float32) + got_x[0].astype(jnp.float32)).astype(bf16)
    by_y[2].start()
    for copy in f_sends:
        copy.wait_recv()
    wrows = total_f.shape[1]
    span = total_f.shape[2] // 3
    outs = (gate_out, up_out, down_out)
    u_sends, here = [], []
    for n in range(3):
        lanes = pl.ds(n * span, span)
        value = f_own[lanes] + f_far[lanes].astype(jnp.float32)
        for m in range(len(steps)):
            value = value + f_got[m, lanes].astype(jnp.float32)
        value = value.T
        for k in range(4):
            total_f[k, :, lanes] = value[k * wrows : (k + 1) * wrows]
        dst = outs[n].at[:, pl.ds(pl.multiple_of(me * span, span), span)]
        for k in range(1, 4):
            u_sends.append(remote(total_f.at[place[k], :, lanes], dst, us.at[k - 1, n], ur.at[k - 1, n], to[k]))
            u_sends[-1].start()
        here.append(pltpu.make_async_copy(total_f.at[me, :, lanes], dst, local_sem.at[n]))
        here[-1].start()
    for copy in a_sends:
        copy.wait_recv()
    value = a_own[...]
    for m in range(depth - 1):
        value = value + a_got[m].astype(jnp.float32)
    value = value.T
    for k in range(4):
        total_a[k] = value[k * wrows : (k + 1) * wrows]
    v_sends = [remote(total_a.at[place[k]], landed.at[me], vs.at[k - 1], vr.at[k - 1], to[k]) for k in range(1, 4)]
    for copy in v_sends:
        copy.start()
    landed[me] = total_a[me]
    for copy in spread:
        copy.wait_recv()
    answer = g_z[0]
    for n in range(1, depth):
        answer = answer + g_z[n]
    gain_out[...] = answer
    for copy in (by_x[1], by_x[2], by_y[1], by_y[2]):
        copy.wait_recv()
    for part, first, second in ((low, got_x[1], got_y[2]), (high, got_y[1], got_x[2])):
        value = mine[0, part].astype(jnp.float32) + first.astype(jnp.float32) + second.astype(jnp.float32)
        result[part] = (resid[part] + value).astype(bf16)
    for copy in v_sends:
        copy.wait_recv()
    qq = ratio * width
    for dst, start, count in ((query_out, 0, qq), (key_out, qq, width), (value_out, qq + width, width), (out_out, cut, qq)):
        dst[...] = jnp.concatenate([landed[k, :, start : start + count] for k in range(4)], axis=1)
    for copy in u_sends:
        copy.wait_recv()
    for copy in f_sends + k_sends + by_x + by_y + a_sends + stages + spread + u_sends + v_sends + [swap, back]:
        copy.wait_send()
    for copy in here:
        copy.wait()


def finish(
    depth, dn2, resid, cot, x, gain1, gain2, fa, fb, cosine, sine, segments, qt, kt, vt, lse, att_all, normed_plane, f_own,
    f_near, f_far, mine, wrows, number,
):
    rows, model = dn2.shape
    heads, width, total = qt.shape
    groups = kt.shape[0]
    ratio = heads // groups
    fcols, block = f_own.shape
    acols = (2 * ratio + 2) * width
    bf16, f32, dma = jnp.bfloat16, jnp.float32, pltpu.SemaphoreType.DMA
    shape = jax.ShapeDtypeStruct
    vmem, any_ = pl.BlockSpec(memory_space=pltpu.VMEM), pl.BlockSpec(memory_space=pl.ANY)
    grads = shape((wrows, 4 * fcols // 3), f32)
    scratch = [
        ((total, total), f32),
        ((heads, width, total), bf16),
        ((2, width, total), f32),
        ((heads + 2 * groups, width, total), bf16),
        ((groups, (ratio + 2) * width, total), bf16),
        ((rows, model), f32),
        ((rows, model), bf16),
        ((rows, model), bf16),
        (((ratio + 2) * width, 4 * total), bf16),
        ((rows, model), bf16),
        ((rows, model), bf16),
        ((acols, block), f32),
        ((depth - 1, acols, block), bf16),
        ((depth - 1, acols, block), bf16),
        ((depth - 2, fcols, block), bf16),
        ((4, wrows, fcols), f32),
        ((4, wrows, acols), f32),
        ((4, wrows, acols), f32),
        ((3, rows // 2, model), bf16),
        ((3, rows // 2, model), bf16),
        ((2, rows // 2, model), bf16),
        ((2, 4, 2, rows, block), bf16),
        ((2, 4, 2, rows, block), bf16),
        ((4, 2, model), f32),
        ((3, 2, model), f32),
        ((depth, 2, model), f32),
    ]
    sems = [
        (depth - 2,), (depth - 2,), (3,), (3,), (3,), (3,), (3,), (3,), (8,), (8,), (depth - 1,),
        (depth - 1,), (3, 3), (3, 3), (3,), (3,), (2 + depth,), (2 + depth,), (2,), (2,), (6,), (2, 2),
    ]
    return pl.pallas_call(
        functools.partial(finish_kernel, depth),
        out_shape=(
            shape((rows, model), bf16),
            shape((rows, model), f32),
            grads,
            grads,
            grads,
            shape((wrows, heads * width), f32),
            shape((wrows, groups * width), f32),
            shape((wrows, groups * width), f32),
            shape((wrows, heads * width), f32),
            shape((2, model), f32),
            shape((4, 2, rows, model), bf16),
        ),
        in_specs=[vmem] * 17 + [any_, vmem, any_, vmem, vmem],
        out_specs=(vmem, vmem, any_, any_, any_, vmem, vmem, vmem, vmem, vmem, any_),
        scratch_shapes=[pltpu.VMEM(*item) for item in scratch] + [dma(item) for item in sems],
        compiler_params=pltpu.CompilerParams(
            collective_id=number, has_side_effects=True, vmem_limit_bytes=66 * 10**6
        ),
        name="finish",
    )(
        dn2, resid, cot, x, gain1.reshape(1, model), gain2.reshape(1, model), fa, fb, cosine, sine, segments,
        segments.reshape(total, 1), qt, kt, vt, lse, att_all, normed_plane, f_own, f_near, f_far, mine,
    )


def shifted(value, axis, size, step):
    return lax.ppermute(value, axis, [(i, (i + step) % size) for i in range(size)])


def moved(value, axis, size, step):
    pairs = [(i, i + step) for i in range(size) if 0 <= i + step < size]
    return lax.ppermute(value, axis, pairs)


def crossed(value):
    return lax.ppermute(value, ("y", "x"), [(0, 3), (1, 2), (2, 1), (3, 0)])


def flipped(value, axis):
    return lax.ppermute(value, axis, [(0, 1), (1, 0)])


def placed(blocks, indices, total):
    out = jnp.zeros((total,) + blocks[0].shape, blocks[0].dtype)
    for block, index in zip(blocks, indices):
        out = lax.dynamic_update_index_in_dim(out, block, index, 0)
    return out


def pair_rows(value, it):
    rows = value.shape[0]
    out = placed([value, flipped(value, "t")], [it, 1 - it], 2)
    return out.reshape((2 * rows,) + value.shape[1:])


def plane_blocks(value):
    return [value, flipped(value, "x"), flipped(value, "y"), crossed(value)]


def plane_exchange(blocks):
    return [blocks[0], flipped(blocks[1], "x"), flipped(blocks[2], "y"), crossed(blocks[3])]


def picked(value, index):
    return lax.dynamic_index_in_dim(value, index, 0, keepdims=False)


def make_local(depth):
    def local(
        layer_input,
        segments,
        gain_attn,
        w_query,
        w_key,
        w_value,
        w_out,
        gain_ffn,
        w_gate,
        w_up,
        w_down,
        cotangent,
    ):
        bf16 = jnp.bfloat16
        iz, it = lax.axis_index("z"), lax.axis_index("t")
        ip = lax.axis_index("y") * 2 + lax.axis_index("x")
        seqs_here, total_len = segments.shape
        own_rows, width = layer_input.shape
        wrows = w_query.shape[0]
        qcols, kcols = w_query.shape[1], w_key.shape[1]
        fcols = w_gate.shape[1]
        fq = fcols // 4
        part_a = jnp.concatenate([w_query, w_key], axis=1)
        part_b = jnp.concatenate([w_value, w_out.T], axis=1)
        full_a, full_b, ffn_all = gather_weights(
            depth, part_a, part_b, w_gate, w_up, w_down.T
        )
        full_a, full_b = full_a.reshape(width, -1), full_b.reshape(width, -1)
        heads_here, groups_here = qcols // HD, kcols // HD
        x_float = layer_input.astype(jnp.float32)
        x_hat1, recip1, normed1 = rms_forward(x_float, gain_attn)
        positions = doc_positions(segments[0])
        cosine, sine = (table.T for table in rotary_tables(positions, HD))
        query_t, key_t, value_t, att_all, log_totals, resid, normed2, cot_all, ffn_all = attention_forward(
            depth,
            normed1,
            flipped(normed1, "t"),
            full_a,
            full_b,
            cosine,
            sine,
            segments,
            layer_input,
            gain_ffn,
            cotangent,
            ffn_all,
            heads_here,
            groups_here,
            5,
        )

        grad_normed2, down_sums, normed_plane, _, *ffn_grads = feed_forward(
            depth, normed2, cot_all, ffn_all, normed1, 2
        )
        qq, kq = qcols // 4, kcols // 4
        cut = qq + 2 * kq

        def columns(sums, start, count):
            part = sums[:, :, start : start + count]
            return jnp.transpose(part, (1, 0, 2)).reshape(wrows, 4 * count)

        def attention_sums(sums):
            return [columns(sums, *item) for item in ((0, qq), (qq, kq), (qq + kq, kq), (cut, qq))]

        if len(ffn_grads) == 3:
            own, near, far = ffn_grads
            result, grad_rows, sum_gate, sum_up, sum_down, sum_query, sum_key, sum_value, sum_out, gains, _ = finish(
                depth, grad_normed2, resid, cotangent, layer_input, gain_attn, gain_ffn, full_a, full_b, cosine, sine,
                segments, query_t, key_t, value_t, log_totals, att_all, normed_plane, own, near, far, down_sums,
                wrows, 7,
            )
            return (
                result, grad_rows, gains[0], sum_query, sum_key, sum_value, sum_out.T, gains[1], sum_gate, sum_up,
                sum_down.T,
            )

        normed_plane = normed_plane.reshape(4 * total_len, width)
        down_sums = down_sums.astype(jnp.float32)
        result = down_sums[0]
        for block in plane_exchange([down_sums[k].astype(bf16) for k in range(4)])[1:]:
            result = result + block.astype(jnp.float32)
        result = (resid + result).astype(bf16)
        tokens, turned = ffn_grads
        ffn_own, near = weight_grads(
            depth,
            iz,
            [turned[0], turned[1], turned[2]],
            [tokens.reshape(8 * own_rows, width), cot_all.reshape(8 * own_rows, width)],
            [0, 0, 1],
        )
        ffn_others = [shifted(near[s - 1], "z", depth, s) for s in range(1, depth)]
        x_hat2, recip2, _ = rms_forward(resid, gain_ffn)

        grad_norm2, grad_g2 = rms_backward(grad_normed2, x_hat2, recip2, gain_ffn)
        grad_resid = cotangent.astype(jnp.float32) + grad_norm2
        grad_resid_b = grad_resid.astype(bf16)
        tok, grad_normed1 = attention_backward(
            grad_resid_b, full_a, full_b, cosine, sine, segments, query_t, key_t, value_t, log_totals, 6
        )
        grad_norm1, grad_g1 = rms_backward(grad_normed1, x_hat1, recip1, gain_attn)
        grad_rows = grad_resid + grad_norm1

        def column_quarters(value):
            return jnp.concatenate(plane_exchange([picked(value, ip ^ k) for k in range(4)]), axis=1)

        att_all = att_all.reshape(qq, 4 * total_len)
        tok_all = column_quarters(tok)

        blocks = jnp.stack(plane_blocks(grad_resid_b))
        both = placed([blocks, flipped(blocks, "t")], [it, 1 - it], 2)
        resid_plane = jnp.transpose(both, (1, 0, 2, 3)).reshape(4 * total_len, width)
        gains = jnp.stack([grad_g1, grad_g2]).reshape(8, -1)
        own, near = weight_grads(depth, iz, [tok_all, att_all], [normed_plane, resid_plane], [0, 1])
        others = [shifted(near[s - 1], "z", depth, s) for s in range(1, depth)]
        ffn_own, own = lax.optimization_barrier((ffn_own, own))
        sum_gate, sum_up, sum_down = to_owners(depth, ffn_own, ffn_others, wrows, [fq] * 3, 3)
        attn_sums, gains = to_owners(depth, own, others, wrows, [cut + qq], 4, gains)
        total_g1, total_g2 = gains.reshape(2, width)

        sum_query, sum_key, sum_value, sum_out = attention_sums(attn_sums)
        return (
            result,
            grad_rows,
            total_g1,
            sum_query,
            sum_key,
            sum_value,
            sum_out.T,
            total_g2,
            sum_gate,
            sum_up,
            sum_down.T,
        )

    return local


def solution(mesh):
    ring = mesh.shape["dp"]
    fine = Mesh(mesh.devices.reshape(ring // 4, 2, 2, mesh.shape["tensor"]), ("z", "y", "x", "t"))
    dp, every = ("z", "y", "x"), ("z", "y", "x", "t")
    return jax.shard_map(
        make_local(ring // 4),
        mesh=fine,
        in_specs=(
            P(every, None),
            P(dp, None),
            P(),
            P(dp, "t"),
            P(dp, "t"),
            P(dp, "t"),
            P("t", dp),
            P(),
            P(dp, "t"),
            P(dp, "t"),
            P("t", dp),
            P(every, None),
        ),
        out_specs=(
            P(every, None),
            P(every, None),
            P(),
            P(dp, "t"),
            P(dp, "t"),
            P(dp, "t"),
            P("t", dp),
            P(),
            P(dp, "t"),
            P(dp, "t"),
            P("t", dp),
        ),
        check_vma=False,
    )
```

```python
import functools
import math

import jax
import jax.numpy as jnp
from jax import lax
from jax.experimental import pallas as pl
from jax.experimental.pallas import tpu as pltpu
from jax.sharding import Mesh
from jax.sharding import PartitionSpec as P

HD = 96


EPSILON = 1e-05
ROPE_BASE = 100000.0
MASKED = -1e30


def lead_product(left_arr, right_arr):
    return lax.dot_general(
        left_arr, right_arr, (((0,), (0,)), ((), ())), preferred_element_type=jnp.float32
    )


def tail_product(left_arr, right_arr):
    return lax.dot_general(
        left_arr, right_arr, (((1,), (1,)), ((), ())), preferred_element_type=jnp.float32
    )


def plain_product(left_arr, right_arr):
    return jnp.dot(left_arr, right_arr, preferred_element_type=jnp.float32)


def doc_positions(segment_row):
    total_len = segment_row.shape[0]
    indices = jnp.arange(total_len, dtype=jnp.int32)
    changes = jnp.concatenate([jnp.ones((1,), dtype=bool), segment_row[1:] != segment_row[:-1]])
    starts = jnp.where(changes, indices, jnp.zeros_like(indices))
    return indices - lax.cummax(starts, axis=0)


def rotary_tables(positions, head_width):
    half_width = head_width // 2
    frequency = jnp.exp(
        -math.log(ROPE_BASE) * 2.0 * jnp.arange(half_width, dtype=jnp.float32) / head_width
    )
    angles = positions.astype(jnp.float32)[:, None] * frequency[None, :]
    return (jnp.cos(angles), jnp.sin(angles))


def rms_forward(values, gain):
    recip = lax.rsqrt(jnp.mean(values * values, axis=-1, keepdims=True) + EPSILON)
    x_hat = values * recip
    return (x_hat, recip, (x_hat * gain).astype(jnp.bfloat16))


def rms_backward(grad_normed, x_hat, recip, gain):
    grad_hat = grad_normed * gain
    grad_gain = jnp.sum(grad_normed * x_hat, axis=0)
    inner = jnp.mean(grad_hat * x_hat, axis=-1, keepdims=True)
    return (recip * (grad_hat - x_hat * inner), grad_gain)


MESH = pl.DeviceIdType.MESH


def remote(src, dst, send_sem, recv_sem, where):
    return pltpu.make_async_remote_copy(
        src_ref=src, dst_ref=dst, send_sem=send_sem, recv_sem=recv_sem, device_id=where, device_id_type=MESH
    )


def greet(targets):
    barrier = pltpu.get_barrier_semaphore()
    for where in targets:
        pl.semaphore_signal(barrier, inc=1, device_id=where, device_id_type=MESH)
    pl.semaphore_wait(barrier, len(targets))


def greet_line(depth, z, targets):
    barrier = pltpu.get_barrier_semaphore()
    for where in targets:
        pl.semaphore_signal(barrier, inc=1, device_id=where, device_id_type=MESH)
    for ahead, where in ((z + 1 < depth, {"z": z + 1}), (z > 0, {"z": z - 1})):

        @pl.when(ahead)
        def _(where=where):
            pl.semaphore_signal(barrier, inc=1, device_id=where, device_id_type=MESH)

    pl.semaphore_wait(barrier, len(targets) + jnp.minimum(z, 1) + jnp.minimum(depth - 1 - z, 1))


def line_step(depth, z, blocks, step, ss, rs):
    sides = (
        ((z >= step - 1) & (z + 1 < depth), z >= step, z - step + 1, {"z": z + 1}),
        ((z + step - 1 < depth) & (z > 0), z + step < depth, z + step - 1, {"z": z - 1}),
    )

    def copy(n):
        at, where = sides[n][2], sides[n][3]
        return remote(blocks.at[at], blocks.at[at], ss.at[n], rs.at[n], where)

    def start():
        for n in range(2):

            @pl.when(sides[n][0])
            def _(n=n):
                copy(n).start()

    def finish():
        for n in range(2):

            @pl.when(sides[n][1])
            def _(n=n):
                copy(n).wait_recv()

            @pl.when(sides[n][0])
            def _(n=n):
                copy(n).wait_send()

    return start, finish


def plane_phases(value, out, ss, rs, local_sem, sides=(0, 1)):
    y, x, t = lax.axis_index("y"), lax.axis_index("x"), lax.axis_index("t")
    to_x, to_y, to_t = {"x": 1 - x}, {"y": 1 - y}, {"t": 1 - t}
    half = value.shape[0] // 2
    low, high = pl.ds(0, half), pl.ds(half, half)
    relative = isinstance(sides[0], int)
    near = sides[0]
    far_side = sides[1] if relative else sides[0]
    mine = pltpu.make_async_copy(value, out.at[0, near], local_sem)
    routes = (
        (value, out.at[1, near], to_x),
        (value, out.at[2, near], to_y),
        (value, out.at[0, far_side], to_t),
        (out.at[1, near, low], out.at[3, near, low], to_y),
        (out.at[2, near, high], out.at[3, near, high], to_x),
        (out.at[1, near], out.at[1, far_side], to_t),
        (out.at[2, near], out.at[2, far_side], to_t),
        (out.at[3, near], out.at[3, far_side], to_t),
    )
    copies = [remote(src, dst, ss.at[n], rs.at[n], where) for n, (src, dst, where) in enumerate(routes)]

    def begin():
        for n in range(3):
            copies[n].start()
        mine.start()

    def relay():
        copies[0].wait_recv()
        copies[3].start()
        copies[5].start()
        copies[1].wait_recv()
        copies[4].start()
        copies[6].start()

    def end():
        copies[3].wait_recv()
        copies[4].wait_recv()
        copies[7].start()
        for n in (2, 5, 6, 7):
            copies[n].wait_recv()
        for copy in copies:
            copy.wait_send()
        mine.wait()

    return begin, relay, end


def ffn_kernel(depth, inner, *refs):
    iz, iy, ix, it = (lax.axis_index(name) for name in ("z", "y", "x", "t"))
    value, cots_in, extra = refs[:3]
    refs = refs[4:]
    out, down_hbm, extra_out, blocks = refs[:4]
    refs = refs[4:]
    if inner:
        own_hbm, near_hbm, far = refs[:3]
        refs = refs[3:]
    tokens, turned = refs[:2]
    refs = refs[1:]
    cots, weights4, send, keep, from_t, from_x, from_y, down_got = refs[1:9]
    ts, tr, xs, xr, ys, yr, gs, gr, ds_, dr, bs, br, zs, zr, local_sem = refs[9:24]
    refs = refs[24:]
    to_x, to_y, to_t = {"x": 1 - ix}, {"y": 1 - iy}, {"t": 1 - it}
    rows, cols = tokens.shape[2], weights4.shape[3] // 3
    model = tokens.shape[3]

    class Part:
        def __init__(self, n):
            self.lanes = pl.ds(n * cols, cols)

        def __getitem__(self, _):
            return weights4[:, :, :, self.lanes].reshape(model, cols)

    gate_w, up_w, down_w = Part(0), Part(1), Part(2)
    half = rows // 2
    low, high = pl.ds(0, half), pl.ds(half, half)
    targets = [to_x, to_y, to_t]
    if not inner:
        down_out, out_sem = refs
    if inner:
        down_out, out_sem, piece_ref, own, near, fs, fr = refs
        reach = depth // 2
        targets.append({"z": lax.rem(iz + reach, depth)})
    greet_line(depth, iz, targets)
    first_begin, first_relay, first_end = plane_phases(value, tokens, bs, br, local_sem.at[0])
    first_begin()
    start, finish_line = line_step(depth, iz, blocks, depth - 1, zs, zr)
    start()
    load_cots = pltpu.make_async_copy(cots_in, cots, local_sem.at[2])
    load_cots.start()
    first_relay()
    begin, relay, end = plane_phases(extra, extra_out, gs, gr, local_sem.at[1], (it, 1 - it))
    begin()
    first_end()
    finish_line()
    load_weights = pltpu.make_async_copy(blocks, weights4, local_sem.at[3])
    load_weights.start()
    load_cots.wait()
    load_weights.wait()

    def tile(k, side, dst, at):
        value = tokens[k, side]
        gate = plain_product(value, gate_w[...])
        up_part = plain_product(value, up_w[...])
        grad_hidden = plain_product(cots[k, side], down_w[...])
        sig_gate = jax.nn.sigmoid(gate)
        gated = gate * sig_gate
        hidden = (gated * up_part).astype(jnp.bfloat16)
        grad_gate = (grad_hidden * up_part * sig_gate * (1.0 + gate * (1.0 - sig_gate))).astype(jnp.bfloat16)
        grad_up = (grad_hidden * gated).astype(jnp.bfloat16)
        lanes = pl.ds((2 * k + side) * rows, rows)
        turned[0, :, lanes] = grad_gate.T
        turned[1, :, lanes] = grad_up.T
        turned[2, :, lanes] = hidden.T
        dst[at] = tail_product(grad_gate, gate_w[...]) + tail_product(grad_up, up_w[...])

    slot = (1, 1, 0, 0)
    over = [remote(send.at[slot[k]], from_t.at[k], ts.at[k], tr.at[k], to_t) for k in range(4)]
    by_x = [
        remote(keep.at[k, part], from_x.at[n], xs.at[n], xr.at[n], to_x)
        for n, (k, part) in enumerate(((3, low), (1, low), (1, high)))
    ]
    by_y = [
        remote(keep.at[k, part], from_y.at[n], ys.at[n], yr.at[n], to_y)
        for n, (k, part) in enumerate(((3, high), (2, high), (2, low)))
    ]

    def compute(k):
        tile(k, 1, send, slot[k])
        over[k].start()
        tile(k, 0, keep, k)

    def merge(k):
        over[k].wait_recv()
        keep[k] = keep[k] + from_t[k]

    compute(3)
    compute(1)
    merge(3)
    by_x[0].start()
    by_y[0].start()
    over[3].wait_send()
    compute(2)
    merge(1)
    by_x[1].start()
    over[1].wait_send()
    compute(0)
    merge(2)
    by_y[1].start()
    merge(0)

    def second_stage():
        by_x[0].wait_recv()
        keep[2, low] = keep[2, low] + from_x[0]
        by_y[2].start()
        by_y[0].wait_recv()
        keep[1, high] = keep[1, high] + from_y[0]
        by_x[2].start()

    if inner:
        block = tokens.shape[3] // depth
        count = 8 * rows

        def piece(step, store):
            at = lax.rem(iz + step, depth)
            lanes = pl.ds(pl.multiple_of(at * block, block), block)
            right = tokens[:, :, :, lanes].reshape(count, block)

            @pl.loop(0, 2)
            def _(n):
                store(pl.multiple_of(n * cols, cols), plain_product(turned[n], right))

            store(2 * cols, plain_product(turned[2], cots[:, :, :, lanes].reshape(count, block)))

        def to_ref(ref, index=None):
            def store(start, value):
                if index is None:
                    ref[pl.ds(start, cols)] = value.astype(ref.dtype)
                else:
                    ref[index, pl.ds(start, cols)] = value.astype(ref.dtype)

            return store

        piece(reach, to_ref(piece_ref))
        flight = remote(piece_ref, far, fs, fr, {"z": lax.rem(iz + reach, depth)})
        flight.start()
        relay()
        second_stage()

        @pl.loop(0, depth - 2)
        def _(n):
            piece(n + 1 + lax.div(n + 1, reach), to_ref(near, n))

        piece(0, to_ref(own))
        results = [pltpu.make_async_copy(own, own_hbm, out_sem.at[1]), pltpu.make_async_copy(near, near_hbm, out_sem.at[2])]
        for copy in results:
            copy.start()
    else:
        relay()
        second_stage()

    def down_copy(k):
        return remote(down_out.at[k], down_got.at[k], ds_.at[k], dr.at[k], to_t)

    def down_part(k, side):
        lanes = pl.ds(pl.multiple_of((2 * k + side) * rows, rows), rows)
        return tail_product(turned[2, :, lanes].T, down_w[...])

    @pl.loop(0, 4)
    def _(k):
        down_out[k] = down_part(k, 1).astype(jnp.bfloat16)
        down_copy(k).start()

    @pl.loop(0, 4)
    def _(k):
        part = down_part(k, 0)
        down_copy(k).wait()
        down_out[k] = (part + down_got[k].astype(jnp.float32)).astype(jnp.bfloat16)

    down_done = pltpu.make_async_copy(down_out, down_hbm, out_sem.at[0])
    down_done.start()
    by_x[1].wait_recv()
    by_y[1].wait_recv()
    keep[0, low] = keep[0, low] + from_x[1]
    keep[0, high] = keep[0, high] + from_y[1]
    by_y[2].wait_recv()
    out[low] = keep[0, low] + from_y[2]
    by_x[2].wait_recv()
    out[high] = keep[0, high] + from_x[2]
    for copy in [over[2], over[0]] + by_x + by_y:
        copy.wait_send()
    end()
    down_done.wait()
    if inner:
        for copy in results:
            copy.wait()
        flight.wait_recv()
        flight.wait_send()


def feed_forward(depth, value, cots, blocks, extra, number):
    rows, model = extra.shape
    cols = blocks.shape[3] // 3
    block = model // depth
    inner = block % 128 == 0
    bf16, f32, dma = jnp.bfloat16, jnp.float32, pltpu.SemaphoreType.DMA
    shape = jax.ShapeDtypeStruct
    vmem, any_ = pl.BlockSpec(memory_space=pltpu.VMEM), pl.BlockSpec(memory_space=pl.ANY)
    plane = (4, 2, rows, model)
    shapes = [shape((rows, model), f32), shape((4, rows, model), bf16), shape(plane, bf16), shape(blocks.shape, bf16)]
    out_specs = [vmem, any_, any_, any_]
    scratch = []
    if inner:
        shapes += [
            shape((3 * cols, block), f32),
            shape((depth - 2, 3 * cols, block), bf16),
            shape((3 * cols, block), bf16),
        ]
        out_specs += [any_, any_, any_]
        scratch += [pltpu.VMEM(plane, bf16), pltpu.VMEM((3, cols, 8 * rows), bf16)]
    else:
        shapes += [shape(plane, bf16), shape((3, cols, 8 * rows), bf16)]
        out_specs += [vmem, vmem]
    scratch += [
        pltpu.VMEM(plane, bf16),
        pltpu.VMEM(blocks.shape, bf16),
        pltpu.VMEM((2, rows, model), f32),
        pltpu.VMEM((4, rows, model), f32),
        pltpu.VMEM((4, rows, model), f32),
        pltpu.VMEM((3, rows // 2, model), f32),
        pltpu.VMEM((3, rows // 2, model), f32),
        pltpu.VMEM((4, rows, model), bf16),
    ] + [dma(item) for item in ((4,), (4,), (3,), (3,), (3,), (3,), (8,), (8,), (4,), (4,), (8,), (8,), (2,), (2,), (4,))]
    scratch += [pltpu.VMEM((4, rows, model), bf16), dma((3,))]
    if inner:
        scratch += [
            pltpu.VMEM((3 * cols, block), bf16),
            pltpu.VMEM((3 * cols, block), f32),
            pltpu.VMEM((depth - 2, 3 * cols, block), bf16),
            dma,
            dma,
        ]
    return pl.pallas_call(
        functools.partial(ffn_kernel, depth, inner),
        out_shape=tuple(shapes),
        in_specs=[vmem, any_, vmem, any_],
        out_specs=tuple(out_specs),
        input_output_aliases={3: 3},
        scratch_shapes=scratch,
        compiler_params=pltpu.CompilerParams(
            collective_id=number, has_side_effects=True, vmem_limit_bytes=66 * 10**6
        ),
        name="feed_forward",
    )(value, cots, extra, blocks)


def weight_grad_kernel(pairs, at_ref, *refs):
    count, rights = len(pairs), max(pairs) + 1
    lefts, right = refs[:count], refs[count : count + rights]
    own, others = refs[count + rights :]
    step = pl.program_id(0)

    def product(n):
        return plain_product(lefts[n][...], right[pairs[n]][...])

    def spans():
        start = 0
        for left in lefts:
            yield pl.ds(start, left.shape[0])
            start += left.shape[0]

    @pl.when(step == 0)
    def _():
        for n, span in enumerate(spans()):
            own[span, :] = product(n)

    @pl.when(step > 0)
    def _():
        for n, span in enumerate(spans()):
            others[0, span, :] = product(n).astype(jnp.bfloat16)


def weight_grads(depth, iz, lefts, rights, pairs):
    tokens, width = rights[0].shape
    block = width // depth
    cols = sum(left.shape[0] for left in lefts)
    if block % 128:
        full = jnp.concatenate([plain_product(left, rights[n]) for left, n in zip(lefts, pairs)], axis=0)
        full = jnp.transpose(full.reshape(cols, depth, block), (1, 0, 2))
        own = picked(full, iz)
        return own, jnp.stack([picked(full, (iz + s) % depth).astype(jnp.bfloat16) for s in range(1, depth)])
    whole = lambda left: pl.BlockSpec(left.shape, lambda s, at: (0, 0))
    grid_spec = pltpu.PrefetchScalarGridSpec(
        num_scalar_prefetch=1,
        grid=(depth,),
        in_specs=[whole(left) for left in lefts]
        + [pl.BlockSpec((tokens, block), lambda s, at: (0, lax.rem(at[0] + s, depth)))] * len(rights),
        out_specs=(
            pl.BlockSpec((cols, block), lambda s, at: (0, 0)),
            pl.BlockSpec((1, cols, block), lambda s, at: (jnp.maximum(s - 1, 0), 0, 0)),
        ),
    )
    return pl.pallas_call(
        functools.partial(weight_grad_kernel, tuple(pairs)),
        grid_spec=grid_spec,
        out_shape=(
            jax.ShapeDtypeStruct((cols, block), jnp.float32),
            jax.ShapeDtypeStruct((depth - 1, cols, block), jnp.bfloat16),
        ),
        cost_estimate=pl.CostEstimate(
            flops=2 * tokens * cols * width,
            bytes_accessed=2 * tokens * (width * len(rights) + cols) + 2 * cols * width,
            transcendentals=0,
        ),
        name="weight_grads",
    )(iz.reshape(1), *lefts, *rights)


def owner_kernel(depth, widths, with_gains, *refs):
    own, others = refs[0], refs[1:depth]
    refs = refs[depth:]
    gains = None
    if with_gains:
        gains, refs = refs[0], refs[1:]
    outs, refs = refs[: len(widths)], refs[len(widths) :]
    if with_gains:
        gain_out, refs = refs[0], refs[1:]
    total, ss, rs, local_sem = refs[:4]
    z, y, x, t = (lax.axis_index(name) for name in ("z", "y", "x", "t"))
    to = (None, {"x": 1 - x}, {"y": 1 - y}, {"y": 1 - y, "x": 1 - x})
    me = 2 * y + x
    place = (me, 2 * y + 1 - x, 2 - 2 * y + x, 3 - me)
    rows, cols = total.shape[1], total.shape[2]
    targets = list(to[1:])
    if with_gains:
        targets += [{"t": 1 - t}] + [{"z": lax.rem(z + s, depth)} for s in range(1, depth)]
    greet(targets)
    if with_gains:
        gsum, got, got_z, gs, gr = refs[4:]
        gsum[0] = gains[...]
        stages = [
            remote(gsum.at[n], got.at[n], gs.at[n], gr.at[n], where)
            for n, where in enumerate(({"t": 1 - t}, to[1], to[2]))
        ]
        stages[0].start()
    spans = [(0, cols)] if len(widths) == 1 else [(n * widths[0], widths[0]) for n in range(len(widths))]
    for start, count in spans:
        at = pl.ds(start, count)
        part = own[at, :]
        for other in others:
            part = part + other[at, :].astype(jnp.float32)
        part = part.T
        for k in range(4):
            total[k, :, at] = part[k * rows : (k + 1) * rows]
    copies = []
    if len(widths) == 1:
        pieces = [(lambda ref: ref, outs[0].at[me])]
    else:
        pieces, start = [], 0
        for n, span in enumerate(widths):
            pieces.append(
                (
                    lambda ref, start=start, span=span: ref.at[:, pl.ds(start, span)],
                    outs[n].at[:, pl.ds(pl.multiple_of(me * span, span), span)],
                )
            )
            start += span
    for k in range(1, 4):
        for n, (cut, dst) in enumerate(pieces):
            copies.append(remote(cut(total.at[place[k]]), dst, ss.at[k - 1, n], rs.at[k - 1, n], to[k]))
    here = [pltpu.make_async_copy(cut(total.at[me]), dst, local_sem.at[n]) for n, (cut, dst) in enumerate(pieces)]
    for copy in copies + here:
        copy.start()
    if with_gains:
        for n in range(3):
            stages[n].wait_recv()
            gsum[n + 1] = gsum[n] + got[n]
            if n < 2:
                stages[n + 1].start()
        spread = [
            remote(gsum.at[3], got_z.at[z], gs.at[2 + s], gr.at[2 + s], {"z": lax.rem(z + s, depth)})
            for s in range(1, depth)
        ]
        for copy in spread:
            copy.start()
        got_z[z] = gsum[3]
        for copy in spread:
            copy.wait_recv()
        answer = got_z[0]
        for n in range(1, depth):
            answer = answer + got_z[n]
        gain_out[...] = answer
        for copy in stages + spread:
            copy.wait_send()
    for copy in copies:
        copy.wait_recv()
    for copy in copies:
        copy.wait_send()
    for copy in here:
        copy.wait()


def to_owners(depth, own, others, rows, widths, number, gains=None):
    cols = own.shape[0]
    dma, f32 = pltpu.SemaphoreType.DMA, jnp.float32
    vmem, any_ = pl.BlockSpec(memory_space=pltpu.VMEM), pl.BlockSpec(memory_space=pl.ANY)
    parts = len(widths)
    if parts == 1:
        shapes = [jax.ShapeDtypeStruct((4, rows, cols), f32)]
    else:
        shapes = [jax.ShapeDtypeStruct((rows, 4 * span), f32) for span in widths]
    out_specs = [any_] * parts
    operands = [own, *others]
    scratch = [pltpu.VMEM((4, rows, cols), f32), dma((3, parts)), dma((3, parts)), dma((parts,))]
    if gains is not None:
        operands.append(gains)
        shapes.append(jax.ShapeDtypeStruct(gains.shape, f32))
        out_specs.append(vmem)
        scratch += [
            pltpu.VMEM((4,) + gains.shape, f32),
            pltpu.VMEM((3,) + gains.shape, f32),
            pltpu.VMEM((depth,) + gains.shape, f32),
            dma((2 + depth,)),
            dma((2 + depth,)),
        ]
    return pl.pallas_call(
        functools.partial(owner_kernel, depth, tuple(widths), gains is not None),
        out_shape=tuple(shapes),
        in_specs=[vmem] * len(operands),
        out_specs=tuple(out_specs),
        scratch_shapes=scratch,
        compiler_params=pltpu.CompilerParams(collective_id=number, has_side_effects=True),
        name="to_owners",
    )(*operands)


def score_bias(seg_row, seg_col, bias):
    total = bias.shape[0]
    keys = lax.broadcasted_iota(jnp.int32, (total, total), 0)
    queries = lax.broadcasted_iota(jnp.int32, (total, total), 1)
    bias[...] = jnp.where((keys <= queries) & (seg_col[...] == seg_row[...]), 0.0, MASKED)


def spread_weights(depth, z, to_x, to_y, mx, my, me, own, spot, zs, zr, ps, pr):
    to_z = ({"z": z + 1}, {"z": z - 1})
    ahead = (z + 1 < depth, z > 0)

    def block(side, step):
        return z - step if side == 0 else z + step

    def present(side, step):
        return z >= step if side == 0 else z + step < depth

    def sides(step):
        return (0,) if step == 0 else (0, 1)

    def source(c, side, step):
        return own[c] if step == 0 else spot(c, block(side, step), me)

    def along(side, step):
        return [
            remote(
                source(c, side, step),
                spot(c, block(side, step), me),
                zs.at[side, step, c],
                zr.at[side, step, c],
                to_z[side],
            )
            for c in range(2)
        ]

    def across(side, step):
        return [
            remote(
                source(c, side, step),
                spot(c, block(side, step), me),
                ps.at[side, step, n],
                pr.at[side, step, n],
                where,
            )
            for n, (c, where) in enumerate(((0, to_x), (1, to_y), (1, to_x), (0, to_y)))
        ]

    def relay(side, step):
        at = block(side, step)
        return [
            remote(spot(0, at, mx), spot(0, at, mx), ps.at[side, step, 4], pr.at[side, step, 4], to_y),
            remote(spot(1, at, my), spot(1, at, my), ps.at[side, step, 5], pr.at[side, step, 5], to_x),
        ]

    def depart():
        for side in range(2):

            @pl.when(ahead[side])
            def _(side=side):
                for copy in along(side, 0):
                    copy.start()

    def advance(step):
        for side in range(2):

            @pl.when(present(side, step))
            def _(side=side):
                for copy in along(side, step - 1):
                    copy.wait_recv()
                if step < depth - 1:

                    @pl.when(ahead[side])
                    def _():
                        for copy in along(side, step):
                            copy.start()

    def share(step):
        for side in sides(step):

            @pl.when(present(side, step))
            def _(side=side):
                for copy in across(side, step):
                    copy.start()

    def pass_on(step):
        for side in sides(step):

            @pl.when(present(side, step))
            def _(side=side):
                first, sent = across(side, step), relay(side, step)
                first[0].wait_recv()
                sent[0].start()
                first[1].wait_recv()
                sent[1].start()

    def arrive():
        for step in range(depth):
            for side in sides(step):

                @pl.when(present(side, step))
                def _(side=side):
                    first, sent = across(side, step), relay(side, step)
                    for copy in (first[2], first[3], sent[0], sent[1]):
                        copy.wait_recv()

    def settle():
        for step in range(depth):
            for side in sides(step):

                @pl.when(present(side, step))
                def _(side=side):
                    for copy in across(side, step) + relay(side, step):
                        copy.wait_send()

        for step in range(depth - 1):
            for side in range(2):

                @pl.when(present(side, step) & ahead[side])
                def _(side=side):
                    for copy in along(side, step):
                        copy.wait_send()

    return depart, advance, share, pass_on, arrive, settle


def front_kernel(
    depth, x_ref, gain1, gain2, wq, wkv, wo, gate_ref, up_ref, down_ref, cos_ref, sin_ref, seg_row, seg_col, cot,
    fq_out, fkv_out, fo_out, blocks, qt, kt, vt, att_all, lse, resid, normed, own, cot_all,
    other, at, raw, bias, mixed, arrived, fq, fkv, fo, az, ar, ap, aq, bz, br, bp, bq, fs, fr, hs, hr, ss, rs, os_, or_, swap_s,
    swap_r, local_sem,
):
    z, y, x, t = (lax.axis_index(name) for name in ("z", "y", "x", "t"))
    heads, width, total = qt.shape
    groups = kt.shape[0]
    ratio = heads // groups
    half = total // 2
    kcols = groups * width
    qcols = heads * width
    model = x_ref.shape[1]
    scale = 1.0 / math.sqrt(width)
    to_t = {"t": 1 - t}
    to = (None, {"x": 1 - x}, {"y": 1 - y}, {"y": 1 - y, "x": 1 - x})
    me = 2 * y + x
    place = (me, 2 * y + 1 - x, 2 - 2 * y + x, 3 - me)
    mine, theirs = (pl.ds(pl.multiple_of(p * half, half), half) for p in (t, 1 - t))
    cut = qcols // 2
    low, high = pl.ds(0, cut), pl.ds(cut, cut)
    ways = (depth, z, to[1], to[2], place[1], place[2], me)
    depart, advance, share, pass_on, arrive, settle = spread_weights(
        *ways, (wq, wkv), lambda c, at, p: (fq, fkv)[c].at[at, p], az, ar, ap, aq
    )
    o_depart, o_advance, o_share, o_pass_on, o_arrive, o_settle = spread_weights(
        *ways, (wo.at[:, low], wo.at[:, high]), lambda c, at, p: fo.at[at, p, :, (low, high)[c]], bz, br, bp, bq
    )
    span = gate_ref.shape[1] // 4
    sources = (gate_ref, up_ref, down_ref)

    def quarter(n, slot):
        return sources[n].at[:, pl.ds(pl.multiple_of(slot * span, span), span)]

    def spot(n):
        return blocks.at[z, me, :, pl.ds(n * span, span)]

    here = [
        pltpu.make_async_copy(src, dst.at[z, me], local_sem.at[n])
        for n, (src, dst) in enumerate(((wq, fq), (wkv, fkv), (wo, fo)))
    ] + [pltpu.make_async_copy(quarter(n, me), spot(n), local_sem.at[3 + n]) for n in range(3)]
    quarters = [
        remote(quarter(n, place[k]), spot(n), fs.at[k - 1, n], fr.at[k - 1, n], to[k])
        for k in range(1, 4)
        for n in range(3)
    ]
    greet_line(depth, z, (*to[1:], to_t))
    depart()
    share(0)
    o_depart()
    for copy in quarters + here:
        copy.start()
    value = x_ref[...].astype(jnp.float32)
    recip = lax.rsqrt(jnp.mean(value * value, axis=-1, keepdims=True) + EPSILON)
    own[...] = (value * recip * gain1[...]).astype(jnp.bfloat16)
    swap = remote(own, other, swap_s.at[0], swap_r.at[0], to_t)
    swap.start()
    score_bias(seg_row, seg_col, bias)
    for step in range(1, depth):
        advance(step)
        share(step)
        o_advance(step)
        pass_on(step - 1)
    for step in range(depth):
        o_share(step)
    for copy in quarters:
        copy.wait_recv()
    for copy in here[3:]:
        copy.wait()
    hops = [line_step(depth, z, blocks, step, hs.at[step - 1], hr.at[step - 1]) for step in range(1, depth - 1)]
    hops[0][0]()
    pass_on(depth - 1)
    swap.wait_recv()
    for copy in here[:3]:
        copy.wait()
    arrive()
    written = [
        pltpu.make_async_copy(src, dst, local_sem.at[7 + n])
        for n, (src, dst) in enumerate(((fq, fq_out), (fkv, fkv_out), (fo, fo_out)))
    ]
    written[0].start()
    written[1].start()
    for rows, lanes in ((own, mine), (other, theirs)):
        value = rows[...]
        for start in range(0, qcols, kcols):
            weights = fq[:, :, :, start : start + kcols].reshape(model, kcols)
            raw[pl.ds(start, kcols), lanes] = plain_product(value, weights).T
        for start in range(0, 2 * kcols, kcols):
            weights = fkv[:, :, :, start : start + kcols].reshape(model, kcols)
            raw[pl.ds(qcols + start, kcols), lanes] = plain_product(value, weights).T
    o_pass_on(0)
    cosine, sine = cos_ref[...], sin_ref[...]
    for n in range(heads + groups):
        first = raw[n * width : n * width + width // 2]
        second = raw[n * width + width // 2 : (n + 1) * width]
        dst, index = (qt, n) if n < heads else (kt, n - heads)
        dst[index, : width // 2] = (first * cosine - second * sine).astype(jnp.bfloat16)
        dst[index, width // 2 :] = (second * cosine + first * sine).astype(jnp.bfloat16)
    for n in range(groups):
        start = qcols + kcols + n * width
        vt[n] = raw[start : start + width].astype(jnp.bfloat16)
    hops[0][1]()
    if len(hops) > 1:
        hops[1][0]()

    @pl.loop(0, groups)
    def _(g):
        key = kt[g].T
        for r in range(ratio):
            h = g * ratio + r
            for j in range(2):
                seen, lanes = (j + 1) * half, pl.ds(j * half, half)
                scores = plain_product(key[:seen], qt[h, :, lanes]) * scale + bias[:seen, lanes]
                top = jnp.max(scores, axis=0, keepdims=True)
                logs = top + jnp.log(jnp.sum(jnp.exp(scores - top), axis=0, keepdims=True))
                lse[h, :, lanes] = logs
                probs = jnp.exp(scores - logs).astype(jnp.bfloat16)
                at[h, :, lanes] = plain_product(vt[g, :, :seen], probs).astype(jnp.bfloat16)

    for step in range(1, depth):
        o_pass_on(step)
    begin, relay, end = plane_phases(cot, cot_all, ss, rs, local_sem.at[6])
    begin()
    o_sends = [
        remote(
            at.at[pl.ds(ratio * place[k], ratio)],
            att_all.at[:, :, pl.ds(k * total, total)],
            os_.at[k - 1],
            or_.at[k - 1],
            to[k],
        )
        for k in range(1, 4)
    ]
    for copy in o_sends:
        copy.start()
    att_all[:, :, :total] = at[pl.ds(ratio * me, ratio)]
    o_arrive()
    written[2].start()

    def project(lanes):
        rows = at[:, :, lanes].reshape(qcols, half).T
        return tail_product(rows, fo[...].reshape(model, qcols))

    mixed[...] = project(theirs)
    copy = remote(mixed, arrived, swap_s.at[1], swap_r.at[1], to_t)
    copy.start()
    part = x_ref[...].astype(jnp.float32) + project(mine)
    copy.wait_recv()
    part = part + arrived[...]
    resid[...] = part
    recip = lax.rsqrt(jnp.mean(part * part, axis=-1, keepdims=True) + EPSILON)
    normed[...] = (part * recip * gain2[...]).astype(jnp.bfloat16)
    relay()
    copy.wait_send()
    swap.wait_send()
    settle()
    o_settle()
    for n, (_, finish_hop) in enumerate(hops):
        if n:
            finish_hop()
        if n and n + 1 < len(hops):
            hops[n + 1][0]()
    for copy in quarters:
        copy.wait_send()
    end()
    for copy in o_sends:
        copy.wait_recv()
        copy.wait_send()
    for copy in written:
        copy.wait()


def front(depth, x, gain1, gain2, wq, wkv, wo, gate, up_part, down, cosine, sine, segments, cot, groups, number):
    rows, model = x.shape
    total, width = 2 * rows, 2 * cosine.shape[0]
    wrows, qcols = wq.shape
    heads = qcols // width
    bf16, f32, dma = jnp.bfloat16, jnp.float32, pltpu.SemaphoreType.DMA
    shape = jax.ShapeDtypeStruct
    vmem, any_ = pl.BlockSpec(memory_space=pltpu.VMEM), pl.BlockSpec(memory_space=pl.ANY)
    full = shape((depth, 4, wrows, qcols), bf16)
    sems = [(2, depth, 2), (2, depth, 2), (2, depth, 6), (2, depth, 6)] * 2
    sems += [(3, 3), (3, 3), (depth, 2), (depth, 2), (8,), (8,), (3,), (3,), (2,), (2,), (10,)]
    return pl.pallas_call(
        functools.partial(front_kernel, depth),
        out_shape=(
            full,
            full,
            full,
            shape((depth, 4, wrows, 3 * gate.shape[1] // 4), bf16),
            shape((heads, width, total), bf16),
            shape((groups, width, total), bf16),
            shape((groups, width, total), bf16),
            shape((heads // groups, width, 4 * total), bf16),
            shape((heads, 1, total), f32),
            shape((rows, model), f32),
            shape((rows, model), bf16),
            shape((rows, model), bf16),
            shape((4, 2, rows, model), bf16),
        ),
        in_specs=[vmem] * 14,
        out_specs=(any_,) * 4 + (vmem,) * 8 + (any_,),
        scratch_shapes=[
            pltpu.VMEM((rows, model), bf16),
            pltpu.VMEM((heads, width, total), bf16),
            pltpu.VMEM(((heads + 2 * groups) * width, total), f32),
            pltpu.VMEM((total, total), f32),
            pltpu.VMEM((rows, model), f32),
            pltpu.VMEM((rows, model), f32),
        ]
        + [pltpu.VMEM(full.shape, bf16)] * 3
        + [dma(item) for item in sems],
        compiler_params=pltpu.CompilerParams(collective_id=number, has_side_effects=True),
        name="front",
    )(
        x, gain1.reshape(1, model), gain2.reshape(1, model), wq, wkv, wo, gate, up_part, down, cosine, sine, segments,
        segments.reshape(total, 1), cot,
    )


def back_heads(wo, cos_ref, sin_ref, qt, kt, vt, lse, tok, own, other, bias, dat, dkv, turned, swap, mine, theirs):
    heads, width, total = qt.shape
    groups = kt.shape[0]
    ratio = heads // groups
    half = total // 2
    kcols = groups * width
    scale = 1.0 / math.sqrt(width)

    def incoming(rows, lanes):
        value = plain_product(rows[...], wo[...]).astype(jnp.bfloat16)
        dat[:, :, lanes] = value.T.reshape(heads, width, half)

    incoming(own, mine)
    swap.wait_recv()
    incoming(other, theirs)
    cosine, sine = cos_ref[...], sin_ref[...]

    def unturned(grad):
        first, second = grad[: width // 2], grad[width // 2 :]
        return jnp.concatenate(
            [first * cosine + second * sine, second * cosine - first * sine], axis=0
        ).astype(jnp.bfloat16)

    @pl.loop(0, groups)
    def _(g):
        key, value = kt[g].T, vt[g].T
        dkv[...] = jnp.zeros_like(dkv)
        for r in range(ratio):
            h = g * ratio + r
            parts = []
            for j in range(2):
                seen, lanes = (j + 1) * half, pl.ds(j * half, half)
                query, grad = qt[h, :, lanes], dat[h, :, lanes]
                scores = plain_product(key[:seen], query) * scale + bias[:seen, lanes]
                probs = jnp.exp(scores - lse[h, :, lanes])
                grad_probs = plain_product(value[:seen], grad)
                delta = jnp.sum(probs * grad_probs, axis=0, keepdims=True)
                grad_scores = (probs * (grad_probs - delta) * scale).astype(jnp.bfloat16)
                parts.append(plain_product(kt[g, :, :seen], grad_scores))
                dkv[0, :, :seen] += tail_product(query, grad_scores)
                dkv[1, :, :seen] += tail_product(grad, probs.astype(jnp.bfloat16))
            grad_query = unturned(jnp.concatenate(parts, axis=1))
            turned[h] = grad_query
            tok[g, r * width : (r + 1) * width] = grad_query
        grad_key = unturned(dkv[0])
        turned[heads + g] = grad_key
        tok[g, ratio * width : (ratio + 1) * width] = grad_key
        grad_value = dkv[1].astype(jnp.bfloat16)
        turned[heads + groups + g] = grad_value
        tok[g, (ratio + 1) * width :] = grad_value


def attend_back_kernel(
    own, fq, fkv, fo, cos_ref, sin_ref, seg_row, seg_col, qt, kt, vt, lse, tok, result,
    other, bias, dat, dkv, turned, sent, arrived, send_sem, recv_sem,
):
    t = lax.axis_index("t")
    heads, width, total = qt.shape
    groups = kt.shape[0]
    half = total // 2
    kcols, qcols = groups * width, heads * width
    to_t = {"t": 1 - t}
    mine, theirs = (pl.ds(pl.multiple_of(p * half, half), half) for p in (t, 1 - t))
    greet((to_t,))
    swap = remote(own, other, send_sem.at[0], recv_sem.at[0], to_t)
    swap.start()
    score_bias(seg_row, seg_col, bias)
    back_heads(fo, cos_ref, sin_ref, qt, kt, vt, lse, tok, own, other, bias, dat, dkv, turned, swap, mine, theirs)

    def project(lanes):
        first = turned[:heads, :, lanes].reshape(qcols, half).T
        second = turned[heads:, :, lanes].reshape(2 * kcols, half).T
        return tail_product(first, fq[...]) + tail_product(second, fkv[...])

    sent[...] = project(theirs).astype(jnp.bfloat16)
    back = remote(sent, arrived, send_sem.at[1], recv_sem.at[1], to_t)
    back.start()
    part = project(mine)
    back.wait_recv()
    result[...] = part + arrived[...].astype(jnp.float32)
    swap.wait_send()
    back.wait_send()


def attention_backward(own, fq, fkv, fo, cosine, sine, segments, qt, kt, vt, lse, number):
    rows, model = own.shape
    heads, width, total = qt.shape
    groups = kt.shape[0]
    bf16, f32, dma = jnp.bfloat16, jnp.float32, pltpu.SemaphoreType.DMA
    shape = jax.ShapeDtypeStruct
    vmem = pl.BlockSpec(memory_space=pltpu.VMEM)
    return pl.pallas_call(
        attend_back_kernel,
        out_shape=(
            shape((groups, (heads // groups + 2) * width, total), bf16),
            shape((rows, model), f32),
        ),
        in_specs=[vmem] * 12,
        out_specs=(vmem,) * 2,
        scratch_shapes=[
            pltpu.VMEM((rows, model), bf16),
            pltpu.VMEM((total, total), f32),
            pltpu.VMEM((heads, width, total), bf16),
            pltpu.VMEM((2, width, total), f32),
            pltpu.VMEM((heads + 2 * groups, width, total), bf16),
            pltpu.VMEM((rows, model), bf16),
            pltpu.VMEM((rows, model), bf16),
            dma((2,)),
            dma((2,)),
        ],
        compiler_params=pltpu.CompilerParams(collective_id=number, has_side_effects=True),
        name="attention_backward",
    )(own, fq, fkv, fo, cosine, sine, segments, segments.reshape(total, 1), qt, kt, vt, lse)


def finish_kernel(
    depth, dn2, resid, cot, x_ref, gain1, gain2, fq_in, fkv_in, fo, cos_ref, sin_ref, seg_row, seg_col, qt, kt, vt, lse,
    att_all, normed_plane, own_in, f_near, far_in, mine, result, grad_rows, gate_out, up_out, down_out, query_out,
    key_out, value_out, out_out, gain_out, resid_plane, bias, dat, dkv, turned, tok, dh, dhb, other, tok_all, sent, arrived, a_own, a_piece, a_got,
    f_got, total_f, total_a, landed, got_x, got_y, passed, right_n, right_r, gsum, g_got, g_z, fq, fkv, f_own, f_far, mine_v, fs, fr, ks, kr, ms, mr,
    ws, wr, ps, pr, as_, ar, us, ur, vs, vr, gs, gr, swap_s, swap_r, local_sem, load_sem, late_sem,
):
    z, y, x, t = (lax.axis_index(name) for name in ("z", "y", "x", "t"))
    to_t, to_z = {"t": 1 - t}, [{"z": lax.rem(z + s, depth)} for s in range(depth)]
    to = (None, {"x": 1 - x}, {"y": 1 - y}, {"y": 1 - y, "x": 1 - x})
    me = 2 * y + x
    place = (me, 2 * y + 1 - x, 2 - 2 * y + x, 3 - me)
    heads, width, total = qt.shape
    groups = kt.shape[0]
    ratio = heads // groups
    half = total // 2
    kcols, qcols = groups * width, heads * width
    cut = (ratio + 2) * width
    bf16 = jnp.bfloat16
    reach = depth // 2
    steps = [s for s in range(1, depth) if s != reach]
    mine_lanes, their_lanes = (pl.ds(pl.multiple_of(p * half, half), half) for p in (t, 1 - t))
    greet([to_t, *to[1:], *to_z[1:]])
    f_sends = [remote(f_near.at[n], f_got.at[n], fs.at[n], fr.at[n], to_z[s]) for n, s in enumerate(steps)]
    for copy in f_sends:
        copy.start()
    late = [
        pltpu.make_async_copy(src, dst, late_sem.at[n])
        for n, (src, dst) in enumerate(
            ((fq_in, fq), (fkv_in, fkv), (mine, mine_v), (own_in, f_own), (far_in, f_far))
        )
    ]
    for copy in late:
        copy.start()
    grad_gain = []
    rows = dh.shape[0]
    for part in (pl.ds(0, rows // 2), pl.ds(rows // 2, rows // 2)):
        h, grad = resid[part], dn2[part]
        recip = lax.rsqrt(jnp.mean(h * h, axis=-1, keepdims=True) + EPSILON)
        hat = h * recip
        grad_gain.append(jnp.sum(grad * hat, axis=0, keepdims=True))
        grad_hat = grad * gain2[...]
        inner = jnp.mean(grad_hat * hat, axis=-1, keepdims=True)
        value = cot[part].astype(jnp.float32) + recip * (grad_hat - hat * inner)
        dh[part] = value
        dhb[part] = value.astype(bf16)
    gsum[0, 1:2] = grad_gain[0] + grad_gain[1]
    swap = remote(dhb, other, swap_s.at[0], swap_r.at[0], to_t)
    swap.start()
    begin, relay, end = plane_phases(dhb, resid_plane, ps, pr, local_sem.at[3], (t, 1 - t))
    begin()
    score_bias(seg_row, seg_col, bias)
    back_heads(fo, cos_ref, sin_ref, qt, kt, vt, lse, tok, dhb, other, bias, dat, dkv, turned, swap, mine_lanes, their_lanes)
    relay()
    k_sends = [
        remote(tok.at[place[k]], tok_all.at[:, pl.ds(k * total, total)], ks.at[k - 1], kr.at[k - 1], to[k])
        for k in range(1, 4)
    ]
    low, high = pl.ds(0, rows // 2), pl.ds(rows // 2, rows // 2)
    by_x = [
        remote(src, got_x.at[n], ms.at[n], mr.at[n], to[1])
        for n, src in enumerate((mine.at[3, low], mine.at[1, low], passed.at[0]))
    ]
    by_y = [
        remote(src, got_y.at[n], ws.at[n], wr.at[n], to[2])
        for n, src in enumerate((mine.at[3, high], mine.at[2, high], passed.at[1]))
    ]
    for copy in k_sends + by_x[:2] + by_y[:2]:
        copy.start()
    tok_all[:, :total] = tok[me]

    def project(lanes):
        first = turned[:heads, :, lanes].reshape(qcols, half).T
        second = turned[heads:, :, lanes].reshape(2 * kcols, half).T
        return tail_product(first, fq[...]) + tail_product(second, fkv[...])

    late[0].wait()
    late[1].wait()
    sent[...] = project(their_lanes).astype(bf16)
    back = remote(sent, arrived, swap_s.at[1], swap_r.at[1], to_t)
    back.start()
    grad_rows[...] = project(mine_lanes)
    back.wait_recv()
    grad_gain = []
    for part in (pl.ds(0, rows // 2), pl.ds(rows // 2, rows // 2)):
        h, grad = x_ref[part].astype(jnp.float32), grad_rows[part] + arrived[part].astype(jnp.float32)
        recip = lax.rsqrt(jnp.mean(h * h, axis=-1, keepdims=True) + EPSILON)
        hat = h * recip
        grad_gain.append(jnp.sum(grad * hat, axis=0, keepdims=True))
        grad_hat = grad * gain1[...]
        inner = jnp.mean(grad_hat * hat, axis=-1, keepdims=True)
        grad_rows[part] = dh[part] + recip * (grad_hat - hat * inner)
    gsum[0, 0:1] = grad_gain[0] + grad_gain[1]
    stages = [remote(gsum.at[n], g_got.at[n], gs.at[n], gr.at[n], where) for n, where in enumerate((to_t, to[1], to[2]))]
    stages[0].start()
    end()
    block = right_n.shape[4]
    order = [reach, *steps, 0]

    def loads(i):
        lanes = pl.ds(pl.multiple_of(lax.rem(z + order[i], depth) * block, 128), block)
        slot = i % 2
        return [
            pltpu.make_async_copy(src.at[:, :, :, lanes], dst.at[slot], load_sem.at[slot, n])
            for n, (src, dst) in enumerate(((normed_plane, right_n), (resid_plane, right_r)))
        ]

    for copy in loads(0):
        copy.start()
    for copy in k_sends:
        copy.wait_recv()
    a_sends = []
    for i, s in enumerate(order):
        if i + 1 < depth:
            for copy in loads(i + 1):
                copy.start()
        for copy in loads(i):
            copy.wait()
        first = plain_product(tok_all[...], right_n[i % 2].reshape(4 * total, block))
        second = plain_product(att_all[...].reshape(ratio * width, 4 * total), right_r[i % 2].reshape(4 * total, block))
        if s:
            a_piece[s - 1, :cut] = first.astype(bf16)
            a_piece[s - 1, cut:] = second.astype(bf16)
            copy = remote(a_piece.at[s - 1], a_got.at[s - 1], as_.at[s - 1], ar.at[s - 1], to_z[s])
            copy.start()
            a_sends.append(copy)
        else:
            a_own[:cut] = first
            a_own[cut:] = second
    for n in range(3):
        stages[n].wait_recv()
        gsum[n + 1] = gsum[n] + g_got[n]
        if n < 2:
            stages[n + 1].start()
    spread = [remote(gsum.at[3], g_z.at[z], gs.at[2 + s], gr.at[2 + s], to_z[s]) for s in range(1, depth)]
    for copy in spread:
        copy.start()
    g_z[z] = gsum[3]
    late[2].wait()
    by_y[0].wait_recv()
    passed[0] = (mine_v[1, high].astype(jnp.float32) + got_y[0].astype(jnp.float32)).astype(bf16)
    by_x[2].start()
    by_x[0].wait_recv()
    passed[1] = (mine_v[2, low].astype(jnp.float32) + got_x[0].astype(jnp.float32)).astype(bf16)
    by_y[2].start()
    for copy in f_sends:
        copy.wait_recv()
    late[3].wait()
    late[4].wait()
    wrows = total_f.shape[1]
    span = total_f.shape[2] // 3
    outs = (gate_out, up_out, down_out)
    u_sends, here = [], []
    for n in range(3):
        lanes = pl.ds(n * span, span)
        value = f_own[lanes] + f_far[lanes].astype(jnp.float32)
        for m in range(len(steps)):
            value = value + f_got[m, lanes].astype(jnp.float32)
        value = value.T
        for k in range(4):
            total_f[k, :, lanes] = value[k * wrows : (k + 1) * wrows]
        dst = outs[n].at[:, pl.ds(pl.multiple_of(me * span, span), span)]
        for k in range(1, 4):
            u_sends.append(remote(total_f.at[place[k], :, lanes], dst, us.at[k - 1, n], ur.at[k - 1, n], to[k]))
            u_sends[-1].start()
        here.append(pltpu.make_async_copy(total_f.at[me, :, lanes], dst, local_sem.at[n]))
        here[-1].start()
    for copy in a_sends:
        copy.wait_recv()
    value = a_own[...]
    for m in range(depth - 1):
        value = value + a_got[m].astype(jnp.float32)
    value = value.T
    for k in range(4):
        total_a[k] = value[k * wrows : (k + 1) * wrows]
    v_sends = [remote(total_a.at[place[k]], landed.at[me], vs.at[k - 1], vr.at[k - 1], to[k]) for k in range(1, 4)]
    for copy in v_sends:
        copy.start()
    landed[me] = total_a[me]
    for copy in spread:
        copy.wait_recv()
    answer = g_z[0]
    for n in range(1, depth):
        answer = answer + g_z[n]
    gain_out[...] = answer
    for copy in (by_x[1], by_x[2], by_y[1], by_y[2]):
        copy.wait_recv()
    for part, first, second in ((low, got_x[1], got_y[2]), (high, got_y[1], got_x[2])):
        value = mine_v[0, part].astype(jnp.float32) + first.astype(jnp.float32) + second.astype(jnp.float32)
        result[part] = (resid[part] + value).astype(bf16)
    for copy in v_sends:
        copy.wait_recv()
    qq = ratio * width
    for dst, start, count in ((query_out, 0, qq), (key_out, qq, width), (value_out, qq + width, width), (out_out, cut, qq)):
        dst[...] = jnp.concatenate([landed[k, :, start : start + count] for k in range(4)], axis=1)
    for copy in u_sends:
        copy.wait_recv()
    for copy in f_sends + k_sends + by_x + by_y + a_sends + stages + spread + u_sends + v_sends + [swap, back]:
        copy.wait_send()
    for copy in here:
        copy.wait()


def finish(
    depth, dn2, resid, cot, x, gain1, gain2, fq, fkv, fo, cosine, sine, segments, qt, kt, vt, lse, att_all, normed_plane, f_own,
    f_near, f_far, mine, wrows, number,
):
    rows, model = dn2.shape
    heads, width, total = qt.shape
    groups = kt.shape[0]
    ratio = heads // groups
    fcols, block = f_own.shape
    acols = (2 * ratio + 2) * width
    bf16, f32, dma = jnp.bfloat16, jnp.float32, pltpu.SemaphoreType.DMA
    shape = jax.ShapeDtypeStruct
    vmem, any_ = pl.BlockSpec(memory_space=pltpu.VMEM), pl.BlockSpec(memory_space=pl.ANY)
    grads = shape((wrows, 4 * fcols // 3), f32)
    scratch = [
        ((total, total), f32),
        ((heads, width, total), bf16),
        ((2, width, total), f32),
        ((heads + 2 * groups, width, total), bf16),
        ((groups, (ratio + 2) * width, total), bf16),
        ((rows, model), f32),
        ((rows, model), bf16),
        ((rows, model), bf16),
        (((ratio + 2) * width, 4 * total), bf16),
        ((rows, model), bf16),
        ((rows, model), bf16),
        ((acols, block), f32),
        ((depth - 1, acols, block), bf16),
        ((depth - 1, acols, block), bf16),
        ((depth - 2, fcols, block), bf16),
        ((4, wrows, fcols), f32),
        ((4, wrows, acols), f32),
        ((4, wrows, acols), f32),
        ((3, rows // 2, model), bf16),
        ((3, rows // 2, model), bf16),
        ((2, rows // 2, model), bf16),
        ((2, 4, 2, rows, block), bf16),
        ((2, 4, 2, rows, block), bf16),
        ((4, 2, model), f32),
        ((3, 2, model), f32),
        ((depth, 2, model), f32),
        ((model, heads * width), bf16),
        ((model, 2 * groups * width), bf16),
        ((fcols, block), f32),
        ((fcols, block), bf16),
        ((4, rows, model), bf16),
    ]
    sems = [
        (depth - 2,), (depth - 2,), (3,), (3,), (3,), (3,), (3,), (3,), (8,), (8,), (depth - 1,),
        (depth - 1,), (3, 3), (3, 3), (3,), (3,), (2 + depth,), (2 + depth,), (2,), (2,), (6,), (2, 2), (5,),
    ]
    return pl.pallas_call(
        functools.partial(finish_kernel, depth),
        out_shape=(
            shape((rows, model), bf16),
            shape((rows, model), f32),
            grads,
            grads,
            grads,
            shape((wrows, heads * width), f32),
            shape((wrows, groups * width), f32),
            shape((wrows, groups * width), f32),
            shape((wrows, heads * width), f32),
            shape((2, model), f32),
            shape((4, 2, rows, model), bf16),
        ),
        in_specs=[vmem] * 6 + [any_, any_] + [vmem] * 10 + [any_] * 5,
        out_specs=(vmem, vmem, any_, any_, any_, vmem, vmem, vmem, vmem, vmem, any_),
        scratch_shapes=[pltpu.VMEM(*item) for item in scratch] + [dma(item) for item in sems],
        compiler_params=pltpu.CompilerParams(
            collective_id=number, has_side_effects=True, vmem_limit_bytes=66 * 10**6
        ),
        name="finish",
    )(
        dn2, resid, cot, x, gain1.reshape(1, model), gain2.reshape(1, model), fq, fkv, fo, cosine, sine, segments,
        segments.reshape(total, 1), qt, kt, vt, lse, att_all, normed_plane, f_own, f_near, f_far, mine,
    )


def copy_kernel(*refs):
    for src, dst in zip(refs[: len(refs) // 2], refs[len(refs) // 2 :]):
        dst[...] = src[...]


def copied(arrays):
    specs = [pl.BlockSpec((array.shape[0] // 2, array.shape[1]), lambda i: (i, 0)) for array in arrays]
    return pl.pallas_call(
        copy_kernel,
        grid=(2,),
        out_shape=tuple(jax.ShapeDtypeStruct(array.shape, array.dtype) for array in arrays),
        in_specs=specs,
        out_specs=tuple(specs),
        name="copied",
    )(*arrays)


def shifted(value, axis, size, step):
    return lax.ppermute(value, axis, [(i, (i + step) % size) for i in range(size)])


def moved(value, axis, size, step):
    pairs = [(i, i + step) for i in range(size) if 0 <= i + step < size]
    return lax.ppermute(value, axis, pairs)


def crossed(value):
    return lax.ppermute(value, ("y", "x"), [(0, 3), (1, 2), (2, 1), (3, 0)])


def flipped(value, axis):
    return lax.ppermute(value, axis, [(0, 1), (1, 0)])


def placed(blocks, indices, total):
    out = jnp.zeros((total,) + blocks[0].shape, blocks[0].dtype)
    for block, index in zip(blocks, indices):
        out = lax.dynamic_update_index_in_dim(out, block, index, 0)
    return out


def pair_rows(value, it):
    rows = value.shape[0]
    out = placed([value, flipped(value, "t")], [it, 1 - it], 2)
    return out.reshape((2 * rows,) + value.shape[1:])


def plane_blocks(value):
    return [value, flipped(value, "x"), flipped(value, "y"), crossed(value)]


def plane_exchange(blocks):
    return [blocks[0], flipped(blocks[1], "x"), flipped(blocks[2], "y"), crossed(blocks[3])]


def picked(value, index):
    return lax.dynamic_index_in_dim(value, index, 0, keepdims=False)


def make_local(depth):
    def local(
        layer_input,
        segments,
        gain_attn,
        w_query,
        w_key,
        w_value,
        w_out,
        gain_ffn,
        w_gate,
        w_up,
        w_down,
        cotangent,
    ):
        bf16 = jnp.bfloat16
        iz, it = lax.axis_index("z"), lax.axis_index("t")
        ip = lax.axis_index("y") * 2 + lax.axis_index("x")
        seqs_here, total_len = segments.shape
        own_rows, width = layer_input.shape
        wrows = w_query.shape[0]
        qcols, kcols = w_query.shape[1], w_key.shape[1]
        fcols = w_gate.shape[1]
        fq = fcols // 4
        positions = doc_positions(segments[0])
        cosine, sine = (table.T for table in rotary_tables(positions, HD))
        (
            full_q, full_kv, full_o, ffn_all, query_t, key_t, value_t, att_all, log_totals, resid, normed2, normed1, cot_all,
        ) = front(
            depth, layer_input, gain_attn, gain_ffn, w_query, jnp.concatenate([w_key, w_value], axis=1), w_out.T, w_gate,
            w_up, w_down.T, cosine, sine, segments, cotangent, kcols // HD, 0,
        )
        full_q, full_kv, full_o = (full.reshape(width, qcols) for full in (full_q, full_kv, full_o))
        grad_normed2, down_sums, normed_plane, _, *ffn_grads = feed_forward(
            depth, normed2, cot_all, ffn_all, normed1, 2
        )
        qq, kq = qcols // 4, kcols // 4
        cut = qq + 2 * kq

        def columns(sums, start, count):
            part = sums[:, :, start : start + count]
            return jnp.transpose(part, (1, 0, 2)).reshape(wrows, 4 * count)

        def attention_sums(sums):
            return [columns(sums, *item) for item in ((0, qq), (qq, kq), (qq + kq, kq), (cut, qq))]

        if len(ffn_grads) == 3:
            own, near, far = ffn_grads
            result, grad_rows, sum_gate, sum_up, sum_down, sum_query, sum_key, sum_value, sum_out, gains, _ = finish(
                depth, grad_normed2, resid, cotangent, layer_input, gain_attn, gain_ffn, full_q, full_kv, full_o, cosine, sine,
                segments, query_t, key_t, value_t, log_totals, att_all, normed_plane, own, near, far, down_sums,
                wrows, 7,
            )
            result, grad_rows, sum_gate, sum_up, sum_down, sum_query, sum_key, sum_value, sum_out = copied(
                (result, grad_rows, sum_gate, sum_up, sum_down, sum_query, sum_key, sum_value, sum_out)
            )
            return (
                result, grad_rows, gains[0], sum_query, sum_key, sum_value, sum_out.T, gains[1], sum_gate, sum_up,
                sum_down.T,
            )

        normed_plane = normed_plane.reshape(4 * total_len, width)
        down_sums = down_sums.astype(jnp.float32)
        result = down_sums[0]
        for block in plane_exchange([down_sums[k].astype(bf16) for k in range(4)])[1:]:
            result = result + block.astype(jnp.float32)
        result = (resid + result).astype(bf16)
        tokens, turned = ffn_grads
        ffn_own, near = weight_grads(
            depth,
            iz,
            [turned[0], turned[1], turned[2]],
            [tokens.reshape(8 * own_rows, width), cot_all.reshape(8 * own_rows, width)],
            [0, 0, 1],
        )
        ffn_others = [shifted(near[s - 1], "z", depth, s) for s in range(1, depth)]
        x_float = layer_input.astype(jnp.float32)
        x_hat1, recip1, _ = rms_forward(x_float, gain_attn)
        x_hat2, recip2, _ = rms_forward(resid, gain_ffn)

        grad_norm2, grad_g2 = rms_backward(grad_normed2, x_hat2, recip2, gain_ffn)
        grad_resid = cotangent.astype(jnp.float32) + grad_norm2
        grad_resid_b = grad_resid.astype(bf16)
        tok, grad_normed1 = attention_backward(
            grad_resid_b, full_q, full_kv, full_o, cosine, sine, segments, query_t, key_t, value_t, log_totals, 6
        )
        grad_norm1, grad_g1 = rms_backward(grad_normed1, x_hat1, recip1, gain_attn)
        grad_rows = grad_resid + grad_norm1

        def column_quarters(value):
            return jnp.concatenate(plane_exchange([picked(value, ip ^ k) for k in range(4)]), axis=1)

        att_all = att_all.reshape(qq, 4 * total_len)
        tok_all = column_quarters(tok)

        blocks = jnp.stack(plane_blocks(grad_resid_b))
        both = placed([blocks, flipped(blocks, "t")], [it, 1 - it], 2)
        resid_plane = jnp.transpose(both, (1, 0, 2, 3)).reshape(4 * total_len, width)
        gains = jnp.stack([grad_g1, grad_g2]).reshape(8, -1)
        own, near = weight_grads(depth, iz, [tok_all, att_all], [normed_plane, resid_plane], [0, 1])
        others = [shifted(near[s - 1], "z", depth, s) for s in range(1, depth)]
        ffn_own, own = lax.optimization_barrier((ffn_own, own))
        sum_gate, sum_up, sum_down = to_owners(depth, ffn_own, ffn_others, wrows, [fq] * 3, 3)
        attn_sums, gains = to_owners(depth, own, others, wrows, [cut + qq], 4, gains)
        total_g1, total_g2 = gains.reshape(2, width)

        sum_query, sum_key, sum_value, sum_out = attention_sums(attn_sums)
        return (
            result,
            grad_rows,
            total_g1,
            sum_query,
            sum_key,
            sum_value,
            sum_out.T,
            total_g2,
            sum_gate,
            sum_up,
            sum_down.T,
        )

    return local


def solution(mesh):
    ring = mesh.shape["dp"]
    fine = Mesh(mesh.devices.reshape(ring // 4, 2, 2, mesh.shape["tensor"]), ("z", "y", "x", "t"))
    dp, every = ("z", "y", "x"), ("z", "y", "x", "t")
    return jax.shard_map(
        make_local(ring // 4),
        mesh=fine,
        in_specs=(
            P(every, None),
            P(dp, None),
            P(),
            P(dp, "t"),
            P(dp, "t"),
            P(dp, "t"),
            P("t", dp),
            P(),
            P(dp, "t"),
            P(dp, "t"),
            P("t", dp),
            P(every, None),
        ),
        out_specs=(
            P(every, None),
            P(every, None),
            P(),
            P(dp, "t"),
            P(dp, "t"),
            P(dp, "t"),
            P("t", dp),
            P(),
            P(dp, "t"),
            P(dp, "t"),
            P("t", dp),
        ),
        check_vma=False,
    )
```

```python
import functools
import math

import jax
import jax.numpy as jnp
from jax import lax
from jax.experimental import pallas as pl
from jax.experimental.pallas import tpu as pltpu
from jax.sharding import Mesh
from jax.sharding import PartitionSpec as P

HD = 96


EPSILON = 1e-05
ROPE_BASE = 100000.0
MASKED = -1e30


def lead_product(left_arr, right_arr):
    return lax.dot_general(
        left_arr, right_arr, (((0,), (0,)), ((), ())), preferred_element_type=jnp.float32
    )


def tail_product(left_arr, right_arr):
    return lax.dot_general(
        left_arr, right_arr, (((1,), (1,)), ((), ())), preferred_element_type=jnp.float32
    )


def plain_product(left_arr, right_arr):
    return jnp.dot(left_arr, right_arr, preferred_element_type=jnp.float32)


def doc_positions(segment_row):
    total_len = segment_row.shape[0]
    indices = jnp.arange(total_len, dtype=jnp.int32)
    changes = jnp.concatenate([jnp.ones((1,), dtype=bool), segment_row[1:] != segment_row[:-1]])
    starts = jnp.where(changes, indices, jnp.zeros_like(indices))
    return indices - lax.cummax(starts, axis=0)


def rotary_tables(positions, head_width):
    half_width = head_width // 2
    frequency = jnp.exp(
        -math.log(ROPE_BASE) * 2.0 * jnp.arange(half_width, dtype=jnp.float32) / head_width
    )
    angles = positions.astype(jnp.float32)[:, None] * frequency[None, :]
    return (jnp.cos(angles), jnp.sin(angles))


def rms_forward(values, gain):
    recip = lax.rsqrt(jnp.mean(values * values, axis=-1, keepdims=True) + EPSILON)
    x_hat = values * recip
    return (x_hat, recip, (x_hat * gain).astype(jnp.bfloat16))


def rms_backward(grad_normed, x_hat, recip, gain):
    grad_hat = grad_normed * gain
    grad_gain = jnp.sum(grad_normed * x_hat, axis=0)
    inner = jnp.mean(grad_hat * x_hat, axis=-1, keepdims=True)
    return (recip * (grad_hat - x_hat * inner), grad_gain)


MESH = pl.DeviceIdType.MESH


def remote(src, dst, send_sem, recv_sem, where):
    return pltpu.make_async_remote_copy(
        src_ref=src, dst_ref=dst, send_sem=send_sem, recv_sem=recv_sem, device_id=where, device_id_type=MESH
    )


def greet(targets):
    barrier = pltpu.get_barrier_semaphore()
    for where in targets:
        pl.semaphore_signal(barrier, inc=1, device_id=where, device_id_type=MESH)
    pl.semaphore_wait(barrier, len(targets))


def greet_line(depth, z, targets):
    barrier = pltpu.get_barrier_semaphore()
    for where in targets:
        pl.semaphore_signal(barrier, inc=1, device_id=where, device_id_type=MESH)
    for ahead, where in ((z + 1 < depth, {"z": z + 1}), (z > 0, {"z": z - 1})):

        @pl.when(ahead)
        def _(where=where):
            pl.semaphore_signal(barrier, inc=1, device_id=where, device_id_type=MESH)

    pl.semaphore_wait(barrier, len(targets) + jnp.minimum(z, 1) + jnp.minimum(depth - 1 - z, 1))


def line_step(depth, z, blocks, step, ss, rs):
    sides = (
        ((z >= step - 1) & (z + 1 < depth), z >= step, z - step + 1, {"z": z + 1}),
        ((z + step - 1 < depth) & (z > 0), z + step < depth, z + step - 1, {"z": z - 1}),
    )

    def copy(n):
        at, where = sides[n][2], sides[n][3]
        return remote(blocks.at[at], blocks.at[at], ss.at[n], rs.at[n], where)

    def start():
        for n in range(2):

            @pl.when(sides[n][0])
            def _(n=n):
                copy(n).start()

    def finish():
        for n in range(2):

            @pl.when(sides[n][1])
            def _(n=n):
                copy(n).wait_recv()

            @pl.when(sides[n][0])
            def _(n=n):
                copy(n).wait_send()

    return start, finish


def plane_phases(value, out, ss, rs, local_sem, sides=(0, 1)):
    y, x, t = lax.axis_index("y"), lax.axis_index("x"), lax.axis_index("t")
    to_x, to_y, to_t = {"x": 1 - x}, {"y": 1 - y}, {"t": 1 - t}
    half = value.shape[0] // 2
    low, high = pl.ds(0, half), pl.ds(half, half)
    relative = isinstance(sides[0], int)
    near = sides[0]
    far_side = sides[1] if relative else sides[0]
    mine = pltpu.make_async_copy(value, out.at[0, near], local_sem)
    routes = (
        (value, out.at[1, near], to_x),
        (value, out.at[2, near], to_y),
        (value, out.at[0, far_side], to_t),
        (out.at[1, near, low], out.at[3, near, low], to_y),
        (out.at[2, near, high], out.at[3, near, high], to_x),
        (out.at[1, near], out.at[1, far_side], to_t),
        (out.at[2, near], out.at[2, far_side], to_t),
        (out.at[3, near], out.at[3, far_side], to_t),
    )
    copies = [remote(src, dst, ss.at[n], rs.at[n], where) for n, (src, dst, where) in enumerate(routes)]

    def begin():
        for n in range(3):
            copies[n].start()
        mine.start()

    def relay():
        copies[0].wait_recv()
        copies[3].start()
        copies[5].start()
        copies[1].wait_recv()
        copies[4].start()
        copies[6].start()

    def end():
        copies[3].wait_recv()
        copies[4].wait_recv()
        copies[7].start()
        for n in (2, 5, 6, 7):
            copies[n].wait_recv()
        for copy in copies:
            copy.wait_send()
        mine.wait()

    return begin, relay, end


def ffn_kernel(depth, inner, *refs):
    iz, iy, ix, it = (lax.axis_index(name) for name in ("z", "y", "x", "t"))
    value, cots_in, extra = refs[:3]
    refs = refs[4:]
    out, down_hbm, extra_out, blocks = refs[:4]
    refs = refs[4:]
    if inner:
        own_hbm, near_hbm, far = refs[:3]
        refs = refs[3:]
    tokens, turned = refs[:2]
    refs = refs[1:]
    cots, weights4, send, keep, from_t, from_x, from_y, down_got = refs[1:9]
    ts, tr, xs, xr, ys, yr, gs, gr, ds_, dr, bs, br, zs, zr, local_sem = refs[9:24]
    refs = refs[24:]
    to_x, to_y, to_t = {"x": 1 - ix}, {"y": 1 - iy}, {"t": 1 - it}
    rows, cols = tokens.shape[2], weights4.shape[3] // 3
    model = tokens.shape[3]

    class Part:
        def __init__(self, n):
            self.lanes = pl.ds(n * cols, cols)

        def __getitem__(self, _):
            return weights4[:, :, :, self.lanes].reshape(model, cols)

    gate_w, up_w, down_w = Part(0), Part(1), Part(2)
    half = rows // 2
    low, high = pl.ds(0, half), pl.ds(half, half)
    targets = [to_x, to_y, to_t]
    if not inner:
        down_out, out_sem = refs
    if inner:
        down_out, out_sem, piece_ref, own, near, fs, fr = refs
        reach = depth // 2
        targets.append({"z": lax.rem(iz + reach, depth)})
    greet_line(depth, iz, targets)
    first_begin, first_relay, first_end = plane_phases(value, tokens, bs, br, local_sem.at[0])
    first_begin()
    start, finish_line = line_step(depth, iz, blocks, depth - 1, zs, zr)
    start()
    load_cots = pltpu.make_async_copy(cots_in, cots, local_sem.at[2])
    load_cots.start()
    first_relay()
    begin, relay, end = plane_phases(extra, extra_out, gs, gr, local_sem.at[1], (it, 1 - it))
    begin()
    first_end()
    finish_line()
    load_weights = pltpu.make_async_copy(blocks, weights4, local_sem.at[3])
    load_weights.start()
    load_cots.wait()
    load_weights.wait()

    def tile(k, side, dst, at):
        value = tokens[k, side]
        gate = plain_product(value, gate_w[...])
        up_part = plain_product(value, up_w[...])
        grad_hidden = plain_product(cots[k, side], down_w[...])
        sig_gate = jax.nn.sigmoid(gate)
        gated = gate * sig_gate
        hidden = (gated * up_part).astype(jnp.bfloat16)
        grad_gate = (grad_hidden * up_part * sig_gate * (1.0 + gate * (1.0 - sig_gate))).astype(jnp.bfloat16)
        grad_up = (grad_hidden * gated).astype(jnp.bfloat16)
        lanes = pl.ds((2 * k + side) * rows, rows)
        turned[0, :, lanes] = grad_gate.T
        turned[1, :, lanes] = grad_up.T
        turned[2, :, lanes] = hidden.T
        dst[at] = tail_product(grad_gate, gate_w[...]) + tail_product(grad_up, up_w[...])

    slot = (1, 1, 0, 0)
    over = [remote(send.at[slot[k]], from_t.at[k], ts.at[k], tr.at[k], to_t) for k in range(4)]
    by_x = [
        remote(keep.at[k, part], from_x.at[n], xs.at[n], xr.at[n], to_x)
        for n, (k, part) in enumerate(((3, low), (1, low), (1, high)))
    ]
    by_y = [
        remote(keep.at[k, part], from_y.at[n], ys.at[n], yr.at[n], to_y)
        for n, (k, part) in enumerate(((3, high), (2, high), (2, low)))
    ]

    def compute(k):
        tile(k, 1, send, slot[k])
        over[k].start()
        tile(k, 0, keep, k)

    def merge(k):
        over[k].wait_recv()
        keep[k] = keep[k] + from_t[k]

    compute(3)
    compute(1)
    merge(3)
    by_x[0].start()
    by_y[0].start()
    over[3].wait_send()
    compute(2)
    merge(1)
    by_x[1].start()
    over[1].wait_send()
    compute(0)
    merge(2)
    by_y[1].start()
    merge(0)

    def second_stage():
        by_x[0].wait_recv()
        keep[2, low] = keep[2, low] + from_x[0]
        by_y[2].start()
        by_y[0].wait_recv()
        keep[1, high] = keep[1, high] + from_y[0]
        by_x[2].start()

    if inner:
        block = tokens.shape[3] // depth
        count = 8 * rows

        def piece(step, store):
            at = lax.rem(iz + step, depth)
            lanes = pl.ds(pl.multiple_of(at * block, block), block)
            right = tokens[:, :, :, lanes].reshape(count, block)

            @pl.loop(0, 2)
            def _(n):
                store(n, plain_product(turned[n], right))

            store(2, plain_product(turned[2], cots[:, :, :, lanes].reshape(count, block)))

        def to_ref(ref, index=None):
            more = cols // 4

            def store(n, value):
                dst = ref if index is None else ref.at[index]
                rounded = value.astype(ref.dtype)
                dst[pl.ds(pl.multiple_of(n * cols, cols), cols)] = rounded
                if dst.shape[0] > 3 * cols:
                    rest = value[:more] - rounded[:more].astype(jnp.float32)
                    dst[pl.ds(pl.multiple_of(3 * cols + n * more, more), more)] = rest.astype(jnp.bfloat16)

            return store

        piece(reach, to_ref(piece_ref))
        flight = remote(piece_ref, far, fs, fr, {"z": lax.rem(iz + reach, depth)})
        flight.start()
        relay()
        second_stage()

        @pl.loop(0, depth - 2)
        def _(n):
            piece(n + 1 + lax.div(n + 1, reach), to_ref(near, n))

        piece(0, to_ref(own))
        results = [pltpu.make_async_copy(own, own_hbm, out_sem.at[1]), pltpu.make_async_copy(near, near_hbm, out_sem.at[2])]
        for copy in results:
            copy.start()
    else:
        relay()
        second_stage()

    def down_copy(k):
        return remote(down_out.at[k], down_got.at[k], ds_.at[k], dr.at[k], to_t)

    def down_part(k, side):
        lanes = pl.ds(pl.multiple_of((2 * k + side) * rows, rows), rows)
        return tail_product(turned[2, :, lanes].T, down_w[...])

    @pl.loop(0, 4)
    def _(k):
        down_out[k] = down_part(k, 1).astype(jnp.bfloat16)
        down_copy(k).start()

    @pl.loop(0, 4)
    def _(k):
        part = down_part(k, 0)
        down_copy(k).wait()
        down_out[k] = (part + down_got[k].astype(jnp.float32)).astype(jnp.bfloat16)

    down_done = pltpu.make_async_copy(down_out, down_hbm, out_sem.at[0])
    down_done.start()
    by_x[1].wait_recv()
    by_y[1].wait_recv()
    keep[0, low] = keep[0, low] + from_x[1]
    keep[0, high] = keep[0, high] + from_y[1]
    by_y[2].wait_recv()
    out[low] = keep[0, low] + from_y[2]
    by_x[2].wait_recv()
    out[high] = keep[0, high] + from_x[2]
    for copy in [over[2], over[0]] + by_x + by_y:
        copy.wait_send()
    end()
    down_done.wait()
    if inner:
        for copy in results:
            copy.wait()
        flight.wait_recv()
        flight.wait_send()


def feed_forward(depth, value, cots, blocks, extra, number):
    rows, model = extra.shape
    cols = blocks.shape[3] // 3
    block = model // depth
    inner = block % 128 == 0
    sent_rows = 3 * (cols + cols // 4)
    bf16, f32, dma = jnp.bfloat16, jnp.float32, pltpu.SemaphoreType.DMA
    shape = jax.ShapeDtypeStruct
    vmem, any_ = pl.BlockSpec(memory_space=pltpu.VMEM), pl.BlockSpec(memory_space=pl.ANY)
    plane = (4, 2, rows, model)
    shapes = [shape((rows, model), f32), shape((4, rows, model), bf16), shape(plane, bf16), shape(blocks.shape, bf16)]
    out_specs = [vmem, any_, any_, any_]
    scratch = []
    if inner:
        shapes += [
            shape((3 * cols, block), f32),
            shape((depth - 2, sent_rows, block), bf16),
            shape((3 * cols, block), bf16),
        ]
        out_specs += [any_, any_, any_]
        scratch += [pltpu.VMEM(plane, bf16), pltpu.VMEM((3, cols, 8 * rows), bf16)]
    else:
        shapes += [shape(plane, bf16), shape((3, cols, 8 * rows), bf16)]
        out_specs += [vmem, vmem]
    scratch += [
        pltpu.VMEM(plane, bf16),
        pltpu.VMEM(blocks.shape, bf16),
        pltpu.VMEM((2, rows, model), f32),
        pltpu.VMEM((4, rows, model), f32),
        pltpu.VMEM((4, rows, model), f32),
        pltpu.VMEM((3, rows // 2, model), f32),
        pltpu.VMEM((3, rows // 2, model), f32),
        pltpu.VMEM((4, rows, model), bf16),
    ] + [dma(item) for item in ((4,), (4,), (3,), (3,), (3,), (3,), (8,), (8,), (4,), (4,), (8,), (8,), (2,), (2,), (4,))]
    scratch += [pltpu.VMEM((4, rows, model), bf16), dma((3,))]
    if inner:
        scratch += [
            pltpu.VMEM((3 * cols, block), bf16),
            pltpu.VMEM((3 * cols, block), f32),
            pltpu.VMEM((depth - 2, sent_rows, block), bf16),
            dma,
            dma,
        ]
    return pl.pallas_call(
        functools.partial(ffn_kernel, depth, inner),
        out_shape=tuple(shapes),
        in_specs=[vmem, any_, vmem, any_],
        out_specs=tuple(out_specs),
        input_output_aliases={3: 3},
        scratch_shapes=scratch,
        compiler_params=pltpu.CompilerParams(
            collective_id=number, has_side_effects=True, vmem_limit_bytes=67 * 10**6
        ),
        name="feed_forward",
    )(value, cots, extra, blocks)


def weight_grad_kernel(pairs, at_ref, *refs):
    count, rights = len(pairs), max(pairs) + 1
    lefts, right = refs[:count], refs[count : count + rights]
    own, others = refs[count + rights :]
    step = pl.program_id(0)

    def product(n):
        return plain_product(lefts[n][...], right[pairs[n]][...])

    def spans():
        start = 0
        for left in lefts:
            yield pl.ds(start, left.shape[0])
            start += left.shape[0]

    @pl.when(step == 0)
    def _():
        for n, span in enumerate(spans()):
            own[span, :] = product(n)

    @pl.when(step > 0)
    def _():
        for n, span in enumerate(spans()):
            others[0, span, :] = product(n).astype(jnp.bfloat16)


def weight_grads(depth, iz, lefts, rights, pairs):
    tokens, width = rights[0].shape
    block = width // depth
    cols = sum(left.shape[0] for left in lefts)
    if block % 128:
        full = jnp.concatenate([plain_product(left, rights[n]) for left, n in zip(lefts, pairs)], axis=0)
        full = jnp.transpose(full.reshape(cols, depth, block), (1, 0, 2))
        own = picked(full, iz)
        return own, jnp.stack([picked(full, (iz + s) % depth) for s in range(1, depth)])
    whole = lambda left: pl.BlockSpec(left.shape, lambda s, at: (0, 0))
    grid_spec = pltpu.PrefetchScalarGridSpec(
        num_scalar_prefetch=1,
        grid=(depth,),
        in_specs=[whole(left) for left in lefts]
        + [pl.BlockSpec((tokens, block), lambda s, at: (0, lax.rem(at[0] + s, depth)))] * len(rights),
        out_specs=(
            pl.BlockSpec((cols, block), lambda s, at: (0, 0)),
            pl.BlockSpec((1, cols, block), lambda s, at: (jnp.maximum(s - 1, 0), 0, 0)),
        ),
    )
    return pl.pallas_call(
        functools.partial(weight_grad_kernel, tuple(pairs)),
        grid_spec=grid_spec,
        out_shape=(
            jax.ShapeDtypeStruct((cols, block), jnp.float32),
            jax.ShapeDtypeStruct((depth - 1, cols, block), jnp.bfloat16),
        ),
        cost_estimate=pl.CostEstimate(
            flops=2 * tokens * cols * width,
            bytes_accessed=2 * tokens * (width * len(rights) + cols) + 2 * cols * width,
            transcendentals=0,
        ),
        name="weight_grads",
    )(iz.reshape(1), *lefts, *rights)


def owner_kernel(depth, widths, with_gains, *refs):
    own, others = refs[0], refs[1:depth]
    refs = refs[depth:]
    gains = None
    if with_gains:
        gains, refs = refs[0], refs[1:]
    outs, refs = refs[: len(widths)], refs[len(widths) :]
    if with_gains:
        gain_out, refs = refs[0], refs[1:]
    total, ss, rs, local_sem = refs[:4]
    z, y, x, t = (lax.axis_index(name) for name in ("z", "y", "x", "t"))
    to = (None, {"x": 1 - x}, {"y": 1 - y}, {"y": 1 - y, "x": 1 - x})
    me = 2 * y + x
    place = (me, 2 * y + 1 - x, 2 - 2 * y + x, 3 - me)
    rows, cols = total.shape[1], total.shape[2]
    targets = list(to[1:])
    if with_gains:
        targets += [{"t": 1 - t}] + [{"z": lax.rem(z + s, depth)} for s in range(1, depth)]
    greet(targets)
    if with_gains:
        gsum, got, got_z, gs, gr = refs[4:]
        gsum[0] = gains[...]
        stages = [
            remote(gsum.at[n], got.at[n], gs.at[n], gr.at[n], where)
            for n, where in enumerate(({"t": 1 - t}, to[1], to[2]))
        ]
        stages[0].start()
    spans = [(0, cols)] if len(widths) == 1 else [(n * widths[0], widths[0]) for n in range(len(widths))]
    for start, count in spans:
        at = pl.ds(start, count)
        part = own[at, :]
        for other in others:
            part = part + other[at, :].astype(jnp.float32)
        part = part.T
        for k in range(4):
            total[k, :, at] = part[k * rows : (k + 1) * rows]
    copies = []
    if len(widths) == 1:
        pieces = [(lambda ref: ref, outs[0].at[me])]
    else:
        pieces, start = [], 0
        for n, span in enumerate(widths):
            pieces.append(
                (
                    lambda ref, start=start, span=span: ref.at[:, pl.ds(start, span)],
                    outs[n].at[:, pl.ds(pl.multiple_of(me * span, span), span)],
                )
            )
            start += span
    for k in range(1, 4):
        for n, (cut, dst) in enumerate(pieces):
            copies.append(remote(cut(total.at[place[k]]), dst, ss.at[k - 1, n], rs.at[k - 1, n], to[k]))
    here = [pltpu.make_async_copy(cut(total.at[me]), dst, local_sem.at[n]) for n, (cut, dst) in enumerate(pieces)]
    for copy in copies + here:
        copy.start()
    if with_gains:
        for n in range(3):
            stages[n].wait_recv()
            gsum[n + 1] = gsum[n] + got[n]
            if n < 2:
                stages[n + 1].start()
        spread = [
            remote(gsum.at[3], got_z.at[z], gs.at[2 + s], gr.at[2 + s], {"z": lax.rem(z + s, depth)})
            for s in range(1, depth)
        ]
        for copy in spread:
            copy.start()
        got_z[z] = gsum[3]
        for copy in spread:
            copy.wait_recv()
        answer = got_z[0]
        for n in range(1, depth):
            answer = answer + got_z[n]
        gain_out[...] = answer
        for copy in stages + spread:
            copy.wait_send()
    for copy in copies:
        copy.wait_recv()
    for copy in copies:
        copy.wait_send()
    for copy in here:
        copy.wait()


def to_owners(depth, own, others, rows, widths, number, gains=None):
    cols = own.shape[0]
    dma, f32 = pltpu.SemaphoreType.DMA, jnp.float32
    vmem, any_ = pl.BlockSpec(memory_space=pltpu.VMEM), pl.BlockSpec(memory_space=pl.ANY)
    parts = len(widths)
    if parts == 1:
        shapes = [jax.ShapeDtypeStruct((4, rows, cols), f32)]
    else:
        shapes = [jax.ShapeDtypeStruct((rows, 4 * span), f32) for span in widths]
    out_specs = [any_] * parts
    operands = [own, *others]
    scratch = [pltpu.VMEM((4, rows, cols), f32), dma((3, parts)), dma((3, parts)), dma((parts,))]
    if gains is not None:
        operands.append(gains)
        shapes.append(jax.ShapeDtypeStruct(gains.shape, f32))
        out_specs.append(vmem)
        scratch += [
            pltpu.VMEM((4,) + gains.shape, f32),
            pltpu.VMEM((3,) + gains.shape, f32),
            pltpu.VMEM((depth,) + gains.shape, f32),
            dma((2 + depth,)),
            dma((2 + depth,)),
        ]
    return pl.pallas_call(
        functools.partial(owner_kernel, depth, tuple(widths), gains is not None),
        out_shape=tuple(shapes),
        in_specs=[vmem] * len(operands),
        out_specs=tuple(out_specs),
        scratch_shapes=scratch,
        compiler_params=pltpu.CompilerParams(collective_id=number, has_side_effects=True),
        name="to_owners",
    )(*operands)


def score_bias(seg_row, seg_col, bias):
    total = bias.shape[0]
    keys = lax.broadcasted_iota(jnp.int32, (total, total), 0)
    queries = lax.broadcasted_iota(jnp.int32, (total, total), 1)
    bias[...] = jnp.where((keys <= queries) & (seg_col[...] == seg_row[...]), 0.0, MASKED)


def spread_weights(depth, z, to_x, to_y, mx, my, me, own, spot, zs, zr, ps, pr):
    to_z = ({"z": z + 1}, {"z": z - 1})
    ahead = (z + 1 < depth, z > 0)

    def block(side, step):
        return z - step if side == 0 else z + step

    def present(side, step):
        return z >= step if side == 0 else z + step < depth

    def sides(step):
        return (0,) if step == 0 else (0, 1)

    def source(c, side, step):
        return own[c] if step == 0 else spot(c, block(side, step), me)

    def along(side, step):
        return [
            remote(
                source(c, side, step),
                spot(c, block(side, step), me),
                zs.at[side, step, c],
                zr.at[side, step, c],
                to_z[side],
            )
            for c in range(2)
        ]

    def across(side, step):
        return [
            remote(
                source(c, side, step),
                spot(c, block(side, step), me),
                ps.at[side, step, n],
                pr.at[side, step, n],
                where,
            )
            for n, (c, where) in enumerate(((0, to_x), (1, to_y), (1, to_x), (0, to_y)))
        ]

    def relay(side, step):
        at = block(side, step)
        return [
            remote(spot(0, at, mx), spot(0, at, mx), ps.at[side, step, 4], pr.at[side, step, 4], to_y),
            remote(spot(1, at, my), spot(1, at, my), ps.at[side, step, 5], pr.at[side, step, 5], to_x),
        ]

    def depart():
        for side in range(2):

            @pl.when(ahead[side])
            def _(side=side):
                for copy in along(side, 0):
                    copy.start()

    def advance(step):
        for side in range(2):

            @pl.when(present(side, step))
            def _(side=side):
                for copy in along(side, step - 1):
                    copy.wait_recv()
                if step < depth - 1:

                    @pl.when(ahead[side])
                    def _():
                        for copy in along(side, step):
                            copy.start()

    def share(step):
        for side in sides(step):

            @pl.when(present(side, step))
            def _(side=side):
                for copy in across(side, step):
                    copy.start()

    def pass_on(step):
        for side in sides(step):

            @pl.when(present(side, step))
            def _(side=side):
                first, sent = across(side, step), relay(side, step)
                first[0].wait_recv()
                sent[0].start()
                first[1].wait_recv()
                sent[1].start()

    def arrive():
        for step in range(depth):
            for side in sides(step):

                @pl.when(present(side, step))
                def _(side=side):
                    first, sent = across(side, step), relay(side, step)
                    for copy in (first[2], first[3], sent[0], sent[1]):
                        copy.wait_recv()

    def settle():
        for step in range(depth):
            for side in sides(step):

                @pl.when(present(side, step))
                def _(side=side):
                    for copy in across(side, step) + relay(side, step):
                        copy.wait_send()

        for step in range(depth - 1):
            for side in range(2):

                @pl.when(present(side, step) & ahead[side])
                def _(side=side):
                    for copy in along(side, step):
                        copy.wait_send()

    return depart, advance, share, pass_on, arrive, settle


def front_kernel(
    depth, x_ref, gain1, gain2, wq, wkv, wo, gate_ref, up_ref, down_ref, cos_ref, sin_ref, seg_row, seg_col, cot,
    fq_out, fkv_out, fo_out, blocks, qt, kt, vt, att_all, lse, resid, normed, own, cot_all,
    other, at, raw, bias, mixed, arrived, fq, fkv, fo, az, ar, ap, aq, bz, br, bp, bq, fs, fr, hs, hr, ss, rs, os_, or_, swap_s,
    swap_r, local_sem,
):
    z, y, x, t = (lax.axis_index(name) for name in ("z", "y", "x", "t"))
    heads, width, total = qt.shape
    groups = kt.shape[0]
    ratio = heads // groups
    half = total // 2
    kcols = groups * width
    qcols = heads * width
    model = x_ref.shape[1]
    scale = 1.0 / math.sqrt(width)
    to_t = {"t": 1 - t}
    to = (None, {"x": 1 - x}, {"y": 1 - y}, {"y": 1 - y, "x": 1 - x})
    me = 2 * y + x
    place = (me, 2 * y + 1 - x, 2 - 2 * y + x, 3 - me)
    mine, theirs = (pl.ds(pl.multiple_of(p * half, half), half) for p in (t, 1 - t))
    cut = qcols // 2
    low, high = pl.ds(0, cut), pl.ds(cut, cut)
    ways = (depth, z, to[1], to[2], place[1], place[2], me)
    depart, advance, share, pass_on, arrive, settle = spread_weights(
        *ways, (wq, wkv), lambda c, at, p: (fq, fkv)[c].at[at, p], az, ar, ap, aq
    )
    o_depart, o_advance, o_share, o_pass_on, o_arrive, o_settle = spread_weights(
        *ways, (wo.at[:, low], wo.at[:, high]), lambda c, at, p: fo.at[at, p, :, (low, high)[c]], bz, br, bp, bq
    )
    span = gate_ref.shape[1] // 4
    sources = (gate_ref, up_ref, down_ref)

    def quarter(n, slot):
        return sources[n].at[:, pl.ds(pl.multiple_of(slot * span, span), span)]

    def spot(n):
        return blocks.at[z, me, :, pl.ds(n * span, span)]

    here = [
        pltpu.make_async_copy(src, dst.at[z, me], local_sem.at[n])
        for n, (src, dst) in enumerate(((wq, fq), (wkv, fkv), (wo, fo)))
    ] + [pltpu.make_async_copy(quarter(n, me), spot(n), local_sem.at[3 + n]) for n in range(3)]
    quarters = [
        remote(quarter(n, place[k]), spot(n), fs.at[k - 1, n], fr.at[k - 1, n], to[k])
        for k in range(1, 4)
        for n in range(3)
    ]
    greet_line(depth, z, (*to[1:], to_t))
    depart()
    share(0)
    o_depart()
    for copy in quarters + here:
        copy.start()
    value = x_ref[...].astype(jnp.float32)
    recip = lax.rsqrt(jnp.mean(value * value, axis=-1, keepdims=True) + EPSILON)
    own[...] = (value * recip * gain1[...]).astype(jnp.bfloat16)
    swap = remote(own, other, swap_s.at[0], swap_r.at[0], to_t)
    swap.start()
    score_bias(seg_row, seg_col, bias)
    for step in range(1, depth):
        advance(step)
        share(step)
        o_advance(step)
        pass_on(step - 1)
    for step in range(depth):
        o_share(step)
    for copy in quarters:
        copy.wait_recv()
    for copy in here[3:]:
        copy.wait()
    hops = [line_step(depth, z, blocks, step, hs.at[step - 1], hr.at[step - 1]) for step in range(1, depth - 1)]
    hops[0][0]()
    pass_on(depth - 1)
    swap.wait_recv()
    for copy in here[:3]:
        copy.wait()
    arrive()
    written = [
        pltpu.make_async_copy(src, dst, local_sem.at[7 + n])
        for n, (src, dst) in enumerate(((fq, fq_out), (fkv, fkv_out), (fo, fo_out)))
    ]
    written[0].start()
    written[1].start()
    for rows, lanes in ((own, mine), (other, theirs)):
        value = rows[...]
        for start in range(0, qcols, kcols):
            weights = fq[:, :, :, start : start + kcols].reshape(model, kcols)
            raw[pl.ds(start, kcols), lanes] = plain_product(value, weights).T
        for start in range(0, 2 * kcols, kcols):
            weights = fkv[:, :, :, start : start + kcols].reshape(model, kcols)
            raw[pl.ds(qcols + start, kcols), lanes] = plain_product(value, weights).T
    o_pass_on(0)
    cosine, sine = cos_ref[...], sin_ref[...]
    for n in range(heads + groups):
        first = raw[n * width : n * width + width // 2]
        second = raw[n * width + width // 2 : (n + 1) * width]
        dst, index = (qt, n) if n < heads else (kt, n - heads)
        dst[index, : width // 2] = (first * cosine - second * sine).astype(jnp.bfloat16)
        dst[index, width // 2 :] = (second * cosine + first * sine).astype(jnp.bfloat16)
    for n in range(groups):
        start = qcols + kcols + n * width
        vt[n] = raw[start : start + width].astype(jnp.bfloat16)
    hops[0][1]()
    if len(hops) > 1:
        hops[1][0]()

    @pl.loop(0, groups)
    def _(g):
        key = kt[g].T
        for r in range(ratio):
            h = g * ratio + r
            for j in range(2):
                seen, lanes = (j + 1) * half, pl.ds(j * half, half)
                scores = plain_product(key[:seen], qt[h, :, lanes]) * scale + bias[:seen, lanes]
                top = jnp.max(scores, axis=0, keepdims=True)
                logs = top + jnp.log(jnp.sum(jnp.exp(scores - top), axis=0, keepdims=True))
                lse[h, :, lanes] = logs
                probs = jnp.exp(scores - logs).astype(jnp.bfloat16)
                at[h, :, lanes] = plain_product(vt[g, :, :seen], probs).astype(jnp.bfloat16)

    for step in range(1, depth):
        o_pass_on(step)
    begin, relay, end = plane_phases(cot, cot_all, ss, rs, local_sem.at[6])
    begin()
    o_sends = [
        remote(
            at.at[pl.ds(ratio * place[k], ratio)],
            att_all.at[:, :, pl.ds(k * total, total)],
            os_.at[k - 1],
            or_.at[k - 1],
            to[k],
        )
        for k in range(1, 4)
    ]
    for copy in o_sends:
        copy.start()
    att_all[:, :, :total] = at[pl.ds(ratio * me, ratio)]
    o_arrive()
    written[2].start()

    def project(lanes):
        rows = at[:, :, lanes].reshape(qcols, half).T
        return tail_product(rows, fo[...].reshape(model, qcols))

    mixed[...] = project(theirs)
    copy = remote(mixed, arrived, swap_s.at[1], swap_r.at[1], to_t)
    copy.start()
    part = x_ref[...].astype(jnp.float32) + project(mine)
    copy.wait_recv()
    part = part + arrived[...]
    resid[...] = part
    recip = lax.rsqrt(jnp.mean(part * part, axis=-1, keepdims=True) + EPSILON)
    normed[...] = (part * recip * gain2[...]).astype(jnp.bfloat16)
    relay()
    copy.wait_send()
    swap.wait_send()
    settle()
    o_settle()
    for n, (_, finish_hop) in enumerate(hops):
        if n:
            finish_hop()
        if n and n + 1 < len(hops):
            hops[n + 1][0]()
    for copy in quarters:
        copy.wait_send()
    end()
    for copy in o_sends:
        copy.wait_recv()
        copy.wait_send()
    for copy in written:
        copy.wait()


def front(depth, x, gain1, gain2, wq, wkv, wo, gate, up_part, down, cosine, sine, segments, cot, groups, number):
    rows, model = x.shape
    total, width = 2 * rows, 2 * cosine.shape[0]
    wrows, qcols = wq.shape
    heads = qcols // width
    bf16, f32, dma = jnp.bfloat16, jnp.float32, pltpu.SemaphoreType.DMA
    shape = jax.ShapeDtypeStruct
    vmem, any_ = pl.BlockSpec(memory_space=pltpu.VMEM), pl.BlockSpec(memory_space=pl.ANY)
    full = shape((depth, 4, wrows, qcols), bf16)
    sems = [(2, depth, 2), (2, depth, 2), (2, depth, 6), (2, depth, 6)] * 2
    sems += [(3, 3), (3, 3), (depth, 2), (depth, 2), (8,), (8,), (3,), (3,), (2,), (2,), (10,)]
    return pl.pallas_call(
        functools.partial(front_kernel, depth),
        out_shape=(
            full,
            full,
            full,
            shape((depth, 4, wrows, 3 * gate.shape[1] // 4), bf16),
            shape((heads, width, total), bf16),
            shape((groups, width, total), bf16),
            shape((groups, width, total), bf16),
            shape((heads // groups, width, 4 * total), bf16),
            shape((heads, 1, total), f32),
            shape((rows, model), f32),
            shape((rows, model), bf16),
            shape((rows, model), bf16),
            shape((4, 2, rows, model), bf16),
        ),
        in_specs=[vmem] * 14,
        out_specs=(any_,) * 4 + (vmem,) * 8 + (any_,),
        scratch_shapes=[
            pltpu.VMEM((rows, model), bf16),
            pltpu.VMEM((heads, width, total), bf16),
            pltpu.VMEM(((heads + 2 * groups) * width, total), f32),
            pltpu.VMEM((total, total), f32),
            pltpu.VMEM((rows, model), f32),
            pltpu.VMEM((rows, model), f32),
        ]
        + [pltpu.VMEM(full.shape, bf16)] * 3
        + [dma(item) for item in sems],
        compiler_params=pltpu.CompilerParams(collective_id=number, has_side_effects=True),
        name="front",
    )(
        x, gain1.reshape(1, model), gain2.reshape(1, model), wq, wkv, wo, gate, up_part, down, cosine, sine, segments,
        segments.reshape(total, 1), cot,
    )


def back_heads(wo, cos_ref, sin_ref, qt, kt, vt, lse, tok, own, other, bias, dat, dkv, turned, swap, mine, theirs):
    heads, width, total = qt.shape
    groups = kt.shape[0]
    ratio = heads // groups
    half = total // 2
    kcols = groups * width
    scale = 1.0 / math.sqrt(width)

    def incoming(rows, lanes):
        value = plain_product(rows[...], wo[...]).astype(jnp.bfloat16)
        dat[:, :, lanes] = value.T.reshape(heads, width, half)

    incoming(own, mine)
    swap.wait_recv()
    incoming(other, theirs)
    cosine, sine = cos_ref[...], sin_ref[...]

    def unturned(grad):
        first, second = grad[: width // 2], grad[width // 2 :]
        return jnp.concatenate(
            [first * cosine + second * sine, second * cosine - first * sine], axis=0
        ).astype(jnp.bfloat16)

    @pl.loop(0, groups)
    def _(g):
        key, value = kt[g].T, vt[g].T
        dkv[...] = jnp.zeros_like(dkv)
        for r in range(ratio):
            h = g * ratio + r
            parts = []
            for j in range(2):
                seen, lanes = (j + 1) * half, pl.ds(j * half, half)
                query, grad = qt[h, :, lanes], dat[h, :, lanes]
                scores = plain_product(key[:seen], query) * scale + bias[:seen, lanes]
                probs = jnp.exp(scores - lse[h, :, lanes])
                grad_probs = plain_product(value[:seen], grad)
                delta = jnp.sum(probs * grad_probs, axis=0, keepdims=True)
                grad_scores = (probs * (grad_probs - delta) * scale).astype(jnp.bfloat16)
                parts.append(plain_product(kt[g, :, :seen], grad_scores))
                dkv[0, :, :seen] += tail_product(query, grad_scores)
                dkv[1, :, :seen] += tail_product(grad, probs.astype(jnp.bfloat16))
            grad_query = unturned(jnp.concatenate(parts, axis=1))
            turned[h] = grad_query
            tok[g, r * width : (r + 1) * width] = grad_query
        grad_key = unturned(dkv[0])
        turned[heads + g] = grad_key
        tok[g, ratio * width : (ratio + 1) * width] = grad_key
        grad_value = dkv[1].astype(jnp.bfloat16)
        turned[heads + groups + g] = grad_value
        tok[g, (ratio + 1) * width :] = grad_value


def attend_back_kernel(
    own, fq, fkv, fo, cos_ref, sin_ref, seg_row, seg_col, qt, kt, vt, lse, tok, result,
    other, bias, dat, dkv, turned, sent, arrived, send_sem, recv_sem,
):
    t = lax.axis_index("t")
    heads, width, total = qt.shape
    groups = kt.shape[0]
    half = total // 2
    kcols, qcols = groups * width, heads * width
    to_t = {"t": 1 - t}
    mine, theirs = (pl.ds(pl.multiple_of(p * half, half), half) for p in (t, 1 - t))
    greet((to_t,))
    swap = remote(own, other, send_sem.at[0], recv_sem.at[0], to_t)
    swap.start()
    score_bias(seg_row, seg_col, bias)
    back_heads(fo, cos_ref, sin_ref, qt, kt, vt, lse, tok, own, other, bias, dat, dkv, turned, swap, mine, theirs)

    def project(lanes):
        first = turned[:heads, :, lanes].reshape(qcols, half).T
        second = turned[heads:, :, lanes].reshape(2 * kcols, half).T
        return tail_product(first, fq[...]) + tail_product(second, fkv[...])

    sent[...] = project(theirs).astype(jnp.bfloat16)
    back = remote(sent, arrived, send_sem.at[1], recv_sem.at[1], to_t)
    back.start()
    part = project(mine)
    back.wait_recv()
    result[...] = part + arrived[...].astype(jnp.float32)
    swap.wait_send()
    back.wait_send()


def attention_backward(own, fq, fkv, fo, cosine, sine, segments, qt, kt, vt, lse, number):
    rows, model = own.shape
    heads, width, total = qt.shape
    groups = kt.shape[0]
    bf16, f32, dma = jnp.bfloat16, jnp.float32, pltpu.SemaphoreType.DMA
    shape = jax.ShapeDtypeStruct
    vmem = pl.BlockSpec(memory_space=pltpu.VMEM)
    return pl.pallas_call(
        attend_back_kernel,
        out_shape=(
            shape((groups, (heads // groups + 2) * width, total), bf16),
            shape((rows, model), f32),
        ),
        in_specs=[vmem] * 12,
        out_specs=(vmem,) * 2,
        scratch_shapes=[
            pltpu.VMEM((rows, model), bf16),
            pltpu.VMEM((total, total), f32),
            pltpu.VMEM((heads, width, total), bf16),
            pltpu.VMEM((2, width, total), f32),
            pltpu.VMEM((heads + 2 * groups, width, total), bf16),
            pltpu.VMEM((rows, model), bf16),
            pltpu.VMEM((rows, model), bf16),
            dma((2,)),
            dma((2,)),
        ],
        compiler_params=pltpu.CompilerParams(collective_id=number, has_side_effects=True),
        name="attention_backward",
    )(own, fq, fkv, fo, cosine, sine, segments, segments.reshape(total, 1), qt, kt, vt, lse)


def attention_extras(ratio, width):
    share, third, at = ratio * width // 4, width // 3, (2 * ratio + 2) * width
    found, row = [], at
    for start, count in (
        (0, share),
        (ratio * width, third),
        ((ratio + 1) * width, third),
        ((ratio + 2) * width, share),
    ):
        found.append((start, count, row))
        row += count
    return found


def finish_kernel(
    depth, dn2, resid, cot, x_ref, gain1, gain2, fq_in, fkv_in, fo, cos_ref, sin_ref, seg_row, seg_col, qt, kt, vt, lse,
    att_all, normed_plane, own_in, f_near, far_in, mine, result, grad_rows, gate_out, up_out, down_out, query_out,
    key_out, value_out, out_out, gain_out, resid_plane, bias, dat, dkv, turned, tok, dh, dhb, other, tok_all, sent, arrived, a_own, a_piece, a_got,
    f_got, total_f, total_a, landed, got_x, got_y, passed, right_n, right_r, gsum, g_got, g_z, fq, fkv, f_own, f_far, mine_v, fs, fr, ks, kr, ms, mr,
    ws, wr, ps, pr, as_, ar, us, ur, vs, vr, gs, gr, swap_s, swap_r, local_sem, load_sem, late_sem,
):
    z, y, x, t = (lax.axis_index(name) for name in ("z", "y", "x", "t"))
    to_t, to_z = {"t": 1 - t}, [{"z": lax.rem(z + s, depth)} for s in range(depth)]
    to = (None, {"x": 1 - x}, {"y": 1 - y}, {"y": 1 - y, "x": 1 - x})
    me = 2 * y + x
    place = (me, 2 * y + 1 - x, 2 - 2 * y + x, 3 - me)
    heads, width, total = qt.shape
    groups = kt.shape[0]
    ratio = heads // groups
    half = total // 2
    kcols, qcols = groups * width, heads * width
    cut = (ratio + 2) * width
    bf16 = jnp.bfloat16
    reach = depth // 2
    steps = [s for s in range(1, depth) if s != reach]
    mine_lanes, their_lanes = (pl.ds(pl.multiple_of(p * half, half), half) for p in (t, 1 - t))
    greet([to_t, *to[1:], *to_z[1:]])
    f_sends = [remote(f_near.at[n], f_got.at[n], fs.at[n], fr.at[n], to_z[s]) for n, s in enumerate(steps)]
    for copy in f_sends:
        copy.start()
    late = [
        pltpu.make_async_copy(src, dst, late_sem.at[n])
        for n, (src, dst) in enumerate(
            ((fq_in, fq), (fkv_in, fkv), (mine, mine_v), (own_in, f_own), (far_in, f_far))
        )
    ]
    for copy in late:
        copy.start()
    grad_gain = []
    rows = dh.shape[0]
    for part in (pl.ds(0, rows // 2), pl.ds(rows // 2, rows // 2)):
        h, grad = resid[part], dn2[part]
        recip = lax.rsqrt(jnp.mean(h * h, axis=-1, keepdims=True) + EPSILON)
        hat = h * recip
        grad_gain.append(jnp.sum(grad * hat, axis=0, keepdims=True))
        grad_hat = grad * gain2[...]
        inner = jnp.mean(grad_hat * hat, axis=-1, keepdims=True)
        value = cot[part].astype(jnp.float32) + recip * (grad_hat - hat * inner)
        dh[part] = value
        dhb[part] = value.astype(bf16)
    gsum[0, 1:2] = grad_gain[0] + grad_gain[1]
    swap = remote(dhb, other, swap_s.at[0], swap_r.at[0], to_t)
    swap.start()
    begin, relay, end = plane_phases(dhb, resid_plane, ps, pr, local_sem.at[3], (t, 1 - t))
    begin()
    score_bias(seg_row, seg_col, bias)
    back_heads(fo, cos_ref, sin_ref, qt, kt, vt, lse, tok, dhb, other, bias, dat, dkv, turned, swap, mine_lanes, their_lanes)
    relay()
    k_sends = [
        remote(tok.at[place[k]], tok_all.at[:, pl.ds(k * total, total)], ks.at[k - 1], kr.at[k - 1], to[k])
        for k in range(1, 4)
    ]
    low, high = pl.ds(0, rows // 2), pl.ds(rows // 2, rows // 2)
    by_x = [
        remote(src, got_x.at[n], ms.at[n], mr.at[n], to[1])
        for n, src in enumerate((mine.at[3, low], mine.at[1, low], passed.at[0]))
    ]
    by_y = [
        remote(src, got_y.at[n], ws.at[n], wr.at[n], to[2])
        for n, src in enumerate((mine.at[3, high], mine.at[2, high], passed.at[1]))
    ]
    for copy in k_sends + by_x[:2] + by_y[:2]:
        copy.start()
    tok_all[:, :total] = tok[me]

    def project(lanes):
        first = turned[:heads, :, lanes].reshape(qcols, half).T
        second = turned[heads:, :, lanes].reshape(2 * kcols, half).T
        return tail_product(first, fq[...]) + tail_product(second, fkv[...])

    late[0].wait()
    late[1].wait()
    sent[...] = project(their_lanes).astype(bf16)
    back = remote(sent, arrived, swap_s.at[1], swap_r.at[1], to_t)
    back.start()
    grad_rows[...] = project(mine_lanes)
    back.wait_recv()
    grad_gain = []
    for part in (pl.ds(0, rows // 2), pl.ds(rows // 2, rows // 2)):
        h, grad = x_ref[part].astype(jnp.float32), grad_rows[part] + arrived[part].astype(jnp.float32)
        recip = lax.rsqrt(jnp.mean(h * h, axis=-1, keepdims=True) + EPSILON)
        hat = h * recip
        grad_gain.append(jnp.sum(grad * hat, axis=0, keepdims=True))
        grad_hat = grad * gain1[...]
        inner = jnp.mean(grad_hat * hat, axis=-1, keepdims=True)
        grad_rows[part] = dh[part] + recip * (grad_hat - hat * inner)
    gsum[0, 0:1] = grad_gain[0] + grad_gain[1]
    stages = [remote(gsum.at[n], g_got.at[n], gs.at[n], gr.at[n], where) for n, where in enumerate((to_t, to[1], to[2]))]
    stages[0].start()
    end()
    block = right_n.shape[4]
    order = [reach, *steps, 0]

    def loads(i):
        lanes = pl.ds(pl.multiple_of(lax.rem(z + order[i], depth) * block, 128), block)
        slot = i % 2
        return [
            pltpu.make_async_copy(src.at[:, :, :, lanes], dst.at[slot], load_sem.at[slot, n])
            for n, (src, dst) in enumerate(((normed_plane, right_n), (resid_plane, right_r)))
        ]

    for copy in loads(0):
        copy.start()
    for copy in k_sends:
        copy.wait_recv()
    extras = attention_extras(ratio, width)
    a_sends = []
    for i, s in enumerate(order):
        if i + 1 < depth:
            for copy in loads(i + 1):
                copy.start()
        for copy in loads(i):
            copy.wait()
        first = plain_product(tok_all[...], right_n[i % 2].reshape(4 * total, block))
        second = plain_product(att_all[...].reshape(ratio * width, 4 * total), right_r[i % 2].reshape(4 * total, block))
        if s:
            for value, start in ((first, 0), (second, cut)):
                rounded = value.astype(bf16)
                a_piece[s - 1, start : start + value.shape[0]] = rounded
                for at, count, to_row in extras if s != reach else ():
                    if start <= at < start + value.shape[0]:
                        rows_of = slice(at - start, at - start + count)
                        rest = value[rows_of] - rounded[rows_of].astype(jnp.float32)
                        a_piece[s - 1, to_row : to_row + count] = rest.astype(bf16)
            sent_rows = pl.ds(0, a_own.shape[0] if s == reach else a_piece.shape[1])
            copy = remote(
                a_piece.at[s - 1, sent_rows], a_got.at[s - 1, sent_rows], as_.at[s - 1], ar.at[s - 1], to_z[s]
            )
            copy.start()
            a_sends.append(copy)
        else:
            a_own[:cut] = first
            a_own[cut:] = second
    for n in range(3):
        stages[n].wait_recv()
        gsum[n + 1] = gsum[n] + g_got[n]
        if n < 2:
            stages[n + 1].start()
    spread = [remote(gsum.at[3], g_z.at[z], gs.at[2 + s], gr.at[2 + s], to_z[s]) for s in range(1, depth)]
    for copy in spread:
        copy.start()
    g_z[z] = gsum[3]
    late[2].wait()
    by_y[0].wait_recv()
    passed[0] = (mine_v[1, high].astype(jnp.float32) + got_y[0].astype(jnp.float32)).astype(bf16)
    by_x[2].start()
    by_x[0].wait_recv()
    passed[1] = (mine_v[2, low].astype(jnp.float32) + got_x[0].astype(jnp.float32)).astype(bf16)
    by_y[2].start()
    for copy in f_sends:
        copy.wait_recv()
    late[3].wait()
    late[4].wait()
    wrows = total_f.shape[1]
    span = total_f.shape[2] // 3
    outs = (gate_out, up_out, down_out)
    u_sends, here = [], []
    for n in range(3):
        lanes = pl.ds(n * span, span)
        value = f_own[lanes] + f_far[lanes].astype(jnp.float32)
        for m in range(len(steps)):
            value = value + f_got[m, lanes].astype(jnp.float32)
        more = span // 4
        kept = pl.ds(3 * span + n * more, more)
        rest = value[:more]
        for m in range(len(steps)):
            rest = rest + f_got[m, kept].astype(jnp.float32)
        value = jnp.concatenate([rest, value[more:]], axis=0).T
        for k in range(4):
            total_f[k, :, lanes] = value[k * wrows : (k + 1) * wrows]
        dst = outs[n].at[:, pl.ds(pl.multiple_of(me * span, span), span)]
        for k in range(1, 4):
            u_sends.append(remote(total_f.at[place[k], :, lanes], dst, us.at[k - 1, n], ur.at[k - 1, n], to[k]))
            u_sends[-1].start()
        here.append(pltpu.make_async_copy(total_f.at[me, :, lanes], dst, local_sem.at[n]))
        here[-1].start()
    for copy in a_sends:
        copy.wait_recv()
    acols = a_own.shape[0]
    value = a_own[...]
    for m in range(depth - 1):
        value = value + a_got[m, :acols].astype(jnp.float32)
    a_own[...] = value
    for start, count, to_row in extras:
        rest = a_own[start : start + count]
        for m in (s - 1 for s in steps):
            rest = rest + a_got[m, to_row : to_row + count].astype(jnp.float32)
        a_own[start : start + count] = rest
    value = a_own[...].T
    for k in range(4):
        total_a[k] = value[k * wrows : (k + 1) * wrows]
    v_sends = [remote(total_a.at[place[k]], landed.at[me], vs.at[k - 1], vr.at[k - 1], to[k]) for k in range(1, 4)]
    for copy in v_sends:
        copy.start()
    landed[me] = total_a[me]
    for copy in spread:
        copy.wait_recv()
    answer = g_z[0]
    for n in range(1, depth):
        answer = answer + g_z[n]
    gain_out[...] = answer
    for copy in (by_x[1], by_x[2], by_y[1], by_y[2]):
        copy.wait_recv()
    for part, first, second in ((low, got_x[1], got_y[2]), (high, got_y[1], got_x[2])):
        value = mine_v[0, part].astype(jnp.float32) + first.astype(jnp.float32) + second.astype(jnp.float32)
        result[part] = (resid[part] + value).astype(bf16)
    for copy in v_sends:
        copy.wait_recv()
    qq = ratio * width
    for dst, start, count in ((query_out, 0, qq), (key_out, qq, width), (value_out, qq + width, width), (out_out, cut, qq)):
        dst[...] = jnp.concatenate([landed[k, :, start : start + count] for k in range(4)], axis=1)
    for copy in u_sends:
        copy.wait_recv()
    for copy in f_sends + k_sends + by_x + by_y + a_sends + stages + spread + u_sends + v_sends + [swap, back]:
        copy.wait_send()
    for copy in here:
        copy.wait()


def finish(
    depth, dn2, resid, cot, x, gain1, gain2, fq, fkv, fo, cosine, sine, segments, qt, kt, vt, lse, att_all, normed_plane, f_own,
    f_near, f_far, mine, wrows, number,
):
    rows, model = dn2.shape
    heads, width, total = qt.shape
    groups = kt.shape[0]
    ratio = heads // groups
    fcols, block = f_own.shape
    acols = (2 * ratio + 2) * width
    frows = fcols + fcols // 4
    arows = acols + sum(count for _, count, _ in attention_extras(ratio, width))
    bf16, f32, dma = jnp.bfloat16, jnp.float32, pltpu.SemaphoreType.DMA
    shape = jax.ShapeDtypeStruct
    vmem, any_ = pl.BlockSpec(memory_space=pltpu.VMEM), pl.BlockSpec(memory_space=pl.ANY)
    grads = shape((wrows, 4 * fcols // 3), f32)
    scratch = [
        ((total, total), f32),
        ((heads, width, total), bf16),
        ((2, width, total), f32),
        ((heads + 2 * groups, width, total), bf16),
        ((groups, (ratio + 2) * width, total), bf16),
        ((rows, model), f32),
        ((rows, model), bf16),
        ((rows, model), bf16),
        (((ratio + 2) * width, 4 * total), bf16),
        ((rows, model), bf16),
        ((rows, model), bf16),
        ((acols, block), f32),
        ((depth - 1, arows, block), bf16),
        ((depth - 1, arows, block), bf16),
        ((depth - 2, frows, block), bf16),
        ((4, wrows, fcols), f32),
        ((4, wrows, acols), f32),
        ((4, wrows, acols), f32),
        ((3, rows // 2, model), bf16),
        ((3, rows // 2, model), bf16),
        ((2, rows // 2, model), bf16),
        ((2, 4, 2, rows, block), bf16),
        ((2, 4, 2, rows, block), bf16),
        ((4, 2, model), f32),
        ((3, 2, model), f32),
        ((depth, 2, model), f32),
        ((model, heads * width), bf16),
        ((model, 2 * groups * width), bf16),
        ((fcols, block), f32),
        ((fcols, block), bf16),
        ((4, rows, model), bf16),
    ]
    sems = [
        (depth - 2,), (depth - 2,), (3,), (3,), (3,), (3,), (3,), (3,), (8,), (8,), (depth - 1,),
        (depth - 1,), (3, 3), (3, 3), (3,), (3,), (2 + depth,), (2 + depth,), (2,), (2,), (6,), (2, 2), (5,),
    ]
    return pl.pallas_call(
        functools.partial(finish_kernel, depth),
        out_shape=(
            shape((rows, model), bf16),
            shape((rows, model), f32),
            grads,
            grads,
            grads,
            shape((wrows, heads * width), f32),
            shape((wrows, groups * width), f32),
            shape((wrows, groups * width), f32),
            shape((wrows, heads * width), f32),
            shape((2, model), f32),
            shape((4, 2, rows, model), bf16),
        ),
        in_specs=[vmem] * 6 + [any_, any_] + [vmem] * 10 + [any_] * 5,
        out_specs=(vmem, vmem, any_, any_, any_, vmem, vmem, vmem, vmem, vmem, any_),
        scratch_shapes=[pltpu.VMEM(*item) for item in scratch] + [dma(item) for item in sems],
        compiler_params=pltpu.CompilerParams(
            collective_id=number, has_side_effects=True, vmem_limit_bytes=66 * 10**6
        ),
        name="finish",
    )(
        dn2, resid, cot, x, gain1.reshape(1, model), gain2.reshape(1, model), fq, fkv, fo, cosine, sine, segments,
        segments.reshape(total, 1), qt, kt, vt, lse, att_all, normed_plane, f_own, f_near, f_far, mine,
    )


def copy_kernel(*refs):
    for src, dst in zip(refs[: len(refs) // 2], refs[len(refs) // 2 :]):
        dst[...] = src[...]


def copied(arrays):
    specs = [pl.BlockSpec((array.shape[0] // 2, array.shape[1]), lambda i: (i, 0)) for array in arrays]
    return pl.pallas_call(
        copy_kernel,
        grid=(2,),
        out_shape=tuple(jax.ShapeDtypeStruct(array.shape, array.dtype) for array in arrays),
        in_specs=specs,
        out_specs=tuple(specs),
        name="copied",
    )(*arrays)


def shifted(value, axis, size, step):
    return lax.ppermute(value, axis, [(i, (i + step) % size) for i in range(size)])


def moved(value, axis, size, step):
    pairs = [(i, i + step) for i in range(size) if 0 <= i + step < size]
    return lax.ppermute(value, axis, pairs)


def crossed(value):
    return lax.ppermute(value, ("y", "x"), [(0, 3), (1, 2), (2, 1), (3, 0)])


def flipped(value, axis):
    return lax.ppermute(value, axis, [(0, 1), (1, 0)])


def placed(blocks, indices, total):
    out = jnp.zeros((total,) + blocks[0].shape, blocks[0].dtype)
    for block, index in zip(blocks, indices):
        out = lax.dynamic_update_index_in_dim(out, block, index, 0)
    return out


def pair_rows(value, it):
    rows = value.shape[0]
    out = placed([value, flipped(value, "t")], [it, 1 - it], 2)
    return out.reshape((2 * rows,) + value.shape[1:])


def plane_blocks(value):
    return [value, flipped(value, "x"), flipped(value, "y"), crossed(value)]


def plane_exchange(blocks):
    return [blocks[0], flipped(blocks[1], "x"), flipped(blocks[2], "y"), crossed(blocks[3])]


def picked(value, index):
    return lax.dynamic_index_in_dim(value, index, 0, keepdims=False)


def make_local(depth):
    def local(
        layer_input,
        segments,
        gain_attn,
        w_query,
        w_key,
        w_value,
        w_out,
        gain_ffn,
        w_gate,
        w_up,
        w_down,
        cotangent,
    ):
        bf16 = jnp.bfloat16
        iz, it = lax.axis_index("z"), lax.axis_index("t")
        ip = lax.axis_index("y") * 2 + lax.axis_index("x")
        seqs_here, total_len = segments.shape
        own_rows, width = layer_input.shape
        wrows = w_query.shape[0]
        qcols, kcols = w_query.shape[1], w_key.shape[1]
        fcols = w_gate.shape[1]
        fq = fcols // 4
        positions = doc_positions(segments[0])
        cosine, sine = (table.T for table in rotary_tables(positions, HD))
        (
            full_q, full_kv, full_o, ffn_all, query_t, key_t, value_t, att_all, log_totals, resid, normed2, normed1, cot_all,
        ) = front(
            depth, layer_input, gain_attn, gain_ffn, w_query, jnp.concatenate([w_key, w_value], axis=1), w_out.T, w_gate,
            w_up, w_down.T, cosine, sine, segments, cotangent, kcols // HD, 0,
        )
        full_q, full_kv, full_o = (full.reshape(width, qcols) for full in (full_q, full_kv, full_o))
        grad_normed2, down_sums, normed_plane, _, *ffn_grads = feed_forward(
            depth, normed2, cot_all, ffn_all, normed1, 2
        )
        qq, kq = qcols // 4, kcols // 4
        cut = qq + 2 * kq

        def columns(sums, start, count):
            part = sums[:, :, start : start + count]
            return jnp.transpose(part, (1, 0, 2)).reshape(wrows, 4 * count)

        def attention_sums(sums):
            return [columns(sums, *item) for item in ((0, qq), (qq, kq), (qq + kq, kq), (cut, qq))]

        if len(ffn_grads) == 3:
            own, near, far = ffn_grads
            result, grad_rows, sum_gate, sum_up, sum_down, sum_query, sum_key, sum_value, sum_out, gains, _ = finish(
                depth, grad_normed2, resid, cotangent, layer_input, gain_attn, gain_ffn, full_q, full_kv, full_o, cosine, sine,
                segments, query_t, key_t, value_t, log_totals, att_all, normed_plane, own, near, far, down_sums,
                wrows, 7,
            )
            result, grad_rows, sum_gate, sum_up, sum_down, sum_query, sum_key, sum_value, sum_out = copied(
                (result, grad_rows, sum_gate, sum_up, sum_down, sum_query, sum_key, sum_value, sum_out)
            )
            return (
                result, grad_rows, gains[0], sum_query, sum_key, sum_value, sum_out.T, gains[1], sum_gate, sum_up,
                sum_down.T,
            )

        normed_plane = normed_plane.reshape(4 * total_len, width)
        down_sums = down_sums.astype(jnp.float32)
        result = down_sums[0]
        for block in plane_exchange([down_sums[k].astype(bf16) for k in range(4)])[1:]:
            result = result + block.astype(jnp.float32)
        result = (resid + result).astype(bf16)
        tokens, turned = ffn_grads
        ffn_own, near = weight_grads(
            depth,
            iz,
            [turned[0], turned[1], turned[2]],
            [tokens.reshape(8 * own_rows, width), cot_all.reshape(8 * own_rows, width)],
            [0, 0, 1],
        )
        ffn_others = [shifted(near[s - 1], "z", depth, s) for s in range(1, depth)]
        x_float = layer_input.astype(jnp.float32)
        x_hat1, recip1, _ = rms_forward(x_float, gain_attn)
        x_hat2, recip2, _ = rms_forward(resid, gain_ffn)

        grad_norm2, grad_g2 = rms_backward(grad_normed2, x_hat2, recip2, gain_ffn)
        grad_resid = cotangent.astype(jnp.float32) + grad_norm2
        grad_resid_b = grad_resid.astype(bf16)
        tok, grad_normed1 = attention_backward(
            grad_resid_b, full_q, full_kv, full_o, cosine, sine, segments, query_t, key_t, value_t, log_totals, 6
        )
        grad_norm1, grad_g1 = rms_backward(grad_normed1, x_hat1, recip1, gain_attn)
        grad_rows = grad_resid + grad_norm1

        def column_quarters(value):
            return jnp.concatenate(plane_exchange([picked(value, ip ^ k) for k in range(4)]), axis=1)

        att_all = att_all.reshape(qq, 4 * total_len)
        tok_all = column_quarters(tok)

        blocks = jnp.stack(plane_blocks(grad_resid_b))
        both = placed([blocks, flipped(blocks, "t")], [it, 1 - it], 2)
        resid_plane = jnp.transpose(both, (1, 0, 2, 3)).reshape(4 * total_len, width)
        gains = jnp.stack([grad_g1, grad_g2]).reshape(8, -1)
        own, near = weight_grads(depth, iz, [tok_all, att_all], [normed_plane, resid_plane], [0, 1])
        others = [shifted(near[s - 1], "z", depth, s) for s in range(1, depth)]
        ffn_own, own = lax.optimization_barrier((ffn_own, own))
        sum_gate, sum_up, sum_down = to_owners(depth, ffn_own, ffn_others, wrows, [fq] * 3, 3)
        attn_sums, gains = to_owners(depth, own, others, wrows, [cut + qq], 4, gains)
        total_g1, total_g2 = gains.reshape(2, width)

        sum_query, sum_key, sum_value, sum_out = attention_sums(attn_sums)
        return (
            result,
            grad_rows,
            total_g1,
            sum_query,
            sum_key,
            sum_value,
            sum_out.T,
            total_g2,
            sum_gate,
            sum_up,
            sum_down.T,
        )

    return local


def solution(mesh):
    ring = mesh.shape["dp"]
    fine = Mesh(mesh.devices.reshape(ring // 4, 2, 2, mesh.shape["tensor"]), ("z", "y", "x", "t"))
    dp, every = ("z", "y", "x"), ("z", "y", "x", "t")
    return jax.shard_map(
        make_local(ring // 4),
        mesh=fine,
        in_specs=(
            P(every, None),
            P(dp, None),
            P(),
            P(dp, "t"),
            P(dp, "t"),
            P(dp, "t"),
            P("t", dp),
            P(),
            P(dp, "t"),
            P(dp, "t"),
            P("t", dp),
            P(every, None),
        ),
        out_specs=(
            P(every, None),
            P(every, None),
            P(),
            P(dp, "t"),
            P(dp, "t"),
            P(dp, "t"),
            P("t", dp),
            P(),
            P(dp, "t"),
            P(dp, "t"),
            P("t", dp),
        ),
        check_vma=False,
    )
```
